32 devices in a mesh: dp: 16 (over z, y, x), tensor: 2 (over core).
Axes of the slice: x: 2, y: 2, z: 4, core: 2. Of those that a mesh axis runs over, the one named last changes fastest.
Arguments:
- residual_in: float32 [16, 2048, 640], P('dp'), may hold values from -6 to 6
- cotangent: float32 [16, 2048, 640], P('dp'), may hold values from -6 to 6
- segment_ids: int32 [16, 2048], P('dp'), may hold values from 0 to 15, never falling along the last dimension, each value on 1 to 512 neighbouring positions
- gain_attn_in: float32 [640], replicated, may hold values from 0.25 to 1.75
- w_query: bfloat16 [640, 1024], P(None, 'tensor'), may hold values from -0.25 to 0.25
- w_key: bfloat16 [640, 256], replicated, may hold values from -0.25 to 0.25
- w_value: bfloat16 [640, 256], replicated, may hold values from -0.25 to 0.25
- gain_query: float32 [256], replicated, may hold values from 0.5 to 4
- gain_key: float32 [256], replicated, may hold values from 0.5 to 4
- w_out: bfloat16 [1024, 640], P('tensor'), may hold values from -0.1875 to 0.1875
- gain_attn_out: float32 [640], replicated, may hold values from 0.25 to 1.75
- gain_ff_in: float32 [640], replicated, may hold values from 0.25 to 1.75
- w_gate: bfloat16 [640, 2048], P(None, 'tensor'), may hold values from -0.25 to 0.25
- w_up: bfloat16 [640, 2048], P(None, 'tensor'), may hold values from -0.25 to 0.25
- w_down: bfloat16 [2048, 640], P('tensor'), may hold values from -0.125 to 0.125
- gain_ff_out: float32 [640], replicated, may hold values from 0.25 to 1.75
Outputs:
- output: float32 [16, 2048, 640], P('dp', 'tensor')
- grad_input: float32 [16, 2048, 640], P('dp', 'tensor')
- grad_gain_attn_in: float32 [640], replicated
- grad_w_query: float32 [640, 1024], P(None, ('tensor', 'dp'))
- grad_w_key: float32 [640, 256], replicated
- grad_w_value: float32 [640, 256], replicated
- grad_gain_query: float32 [256], replicated
- grad_gain_key: float32 [256], replicated
- grad_w_out: float32 [1024, 640], P('tensor', 'dp')
- grad_gain_attn_out: float32 [640], replicated
- grad_gain_ff_in: float32 [640], replicated
- grad_w_gate: float32 [640, 2048], P(None, ('tensor', 'dp'))
- grad_w_up: float32 [640, 2048], P(None, ('tensor', 'dp'))
- grad_w_down: float32 [2048, 640], P('tensor', 'dp')
- grad_gain_ff_out: float32 [640], replicated
The draws below stay inside these ranges and needn't reach their ends.
Inputs may be any that keep to these rules, and one draw needn't show every extreme that they name: `segment_ids`: each row holds 16 sequences numbered from 0 upward in order without gaps; each has 1 to 512 tokens and some sequence of each row has exactly 512.
All inputs are finite; a program needn't handle non-finite values.
Results may differ from the reference program's by a relative error of at most 0.015.
The reference program's roundings to bfloat16 on the way count: a program that leaves them out, or rounds other values in their place, can miss the bound.
Values may be sent and summed in bfloat16 or wider, within the bound.
A program may use at most 256 MiB of HBM per device.

```python
import math
import jax
import jax.numpy as jnp
import numpy as np
from jax import lax

D = 640
H = 4
HEAD_WIDTH = 256
FF = 2048
TOK_DEV = 2048
BLOCK = 512
SEGS = 16
N_DP = 16
N_TENSOR = 2


def gain_law(key):
    return jnp.exp(jax.random.uniform(key, (HEAD_WIDTH,), jnp.float32, jnp.log(0.5), jnp.log(2.0)))


def draw_gain_query(key, part):
    return gain_law(jax.random.fold_in(key, 11))


def draw_gain_key(key, part):
    return gain_law(jax.random.fold_in(key, 23))


def steps_of(rng, shape, pieces, smallest, high):
    level, own = 1.0, jax.random.fold_in(rng, 6)
    for axis_at, shards_of in pieces:
        steps = jnp.exp(jax.random.uniform(jax.random.fold_in(own, axis_at), (shards_of,), jnp.float32, smallest / len(pieces), high / len(pieces)))
        level = level * jnp.repeat(steps, shape[axis_at] // shards_of).reshape([-1 if axis == axis_at else 1 for axis in range(len(shape))])
    return level


def profile(amount, total, reach, slope):
    portions = [(1 << 20) // math.isqrt(rank ** slope) + 1 for rank in range(2, amount + 1)]
    rest, counts = total - reach - (amount - 1), [1] * (amount - 1)
    while rest > 0:
        movable = [i for i in range(amount - 1) if counts[i] < reach]
        whole, remaining = sum([portions[i] for i in movable]), rest
        for i in movable:
            extra = min(reach - counts[i], max(1, remaining * portions[i] // whole), rest)
            counts[i] = counts[i] + extra
            rest = rest - extra
    return np.array([reach] + counts)


def ragged(key, count, total, limit, skew):
    if count == 2:
        one = jax.random.randint(key, (), max(1, total - limit), min(limit, total - 1) + 1)
        return jnp.stack([one, total - one])
    lengths = jnp.asarray(profile(count, total, limit, skew), jnp.int32)
    couples = (count - 1) // 2
    giver, sink = lengths[1:1 + 2 * couples:2], lengths[2:2 + 2 * couples:2]
    margin = jnp.minimum(giver - 1, limit - sink)
    shifted = jax.random.randint(jax.random.fold_in(key, 1), (couples,), 0, 1 << 20) % (margin + 1)
    lengths = lengths.at[1:1 + 2 * couples:2].set(giver - shifted).at[2:2 + 2 * couples:2].set(sink + shifted)
    return lengths[jax.random.permutation(jax.random.fold_in(key, 2), count)]


def bell_draw(stream_key, dims, width, most, split=(), held_as=jnp.bfloat16):
    result = width * jax.random.normal(stream_key, dims, jnp.float32)
    if split:
        result = result * steps_of(stream_key, dims, split, -0.22, 0.18)
    return jnp.clip(result, -most, most).astype(held_as)


def setup_inputs(seed: int = 0) -> dict:
    streams_of = jax.random.split(jax.random.key(seed), 17)
    residual_in = bell_draw(streams_of[0], (N_DP, TOK_DEV, D), 1.0, 6.0, ((0, 16),), jnp.float32)
    cotangent = bell_draw(streams_of[1], (N_DP, TOK_DEV, D), 1.0, 6.0, ((0, 16),), jnp.float32)
    segment_ids = jax.vmap(lambda own: jnp.searchsorted(jnp.cumsum(ragged(own, SEGS, TOK_DEV, BLOCK, 2)), jnp.arange(TOK_DEV), side="right"))(jax.random.split(streams_of[2], N_DP)).reshape((N_DP, TOK_DEV)).astype(jnp.int32)
    gain_attn_in = jnp.clip(1.0 + 0.15 * jax.random.normal(streams_of[3], (D,), jnp.float32), 0.25, 1.75)
    w_query = bell_draw(streams_of[4], (D, H * HEAD_WIDTH), D ** -0.5, 0.25, ((1, 2),))
    w_key = bell_draw(streams_of[5], (D, HEAD_WIDTH), D ** -0.5, 0.25)
    w_value = bell_draw(streams_of[6], (D, HEAD_WIDTH), D ** -0.5, 0.25)
    gain_query = draw_gain_query(jax.random.fold_in(streams_of[16], 71), 0)
    gain_key = draw_gain_key(jax.random.fold_in(streams_of[16], 71), 0)
    w_out = bell_draw(streams_of[9], (H * HEAD_WIDTH, D), (H * HEAD_WIDTH) ** -0.5, 0.1875, ((0, 2),))
    gain_attn_out = jnp.clip(1.0 + 0.15 * jax.random.normal(streams_of[10], (D,), jnp.float32), 0.25, 1.75)
    gain_ff_in = jnp.clip(1.0 + 0.15 * jax.random.normal(streams_of[11], (D,), jnp.float32), 0.25, 1.75)
    w_gate = bell_draw(streams_of[12], (D, FF), D ** -0.5, 0.25, ((1, 2),))
    w_up = bell_draw(streams_of[13], (D, FF), D ** -0.5, 0.25, ((1, 2),))
    w_down = bell_draw(streams_of[14], (FF, D), FF ** -0.5, 0.125, ((0, 2),))
    gain_ff_out = jnp.clip(1.0 + 0.15 * jax.random.normal(streams_of[15], (D,), jnp.float32), 0.25, 1.75)
    return dict(residual_in=residual_in, cotangent=cotangent, segment_ids=segment_ids, gain_attn_in=gain_attn_in, w_query=w_query, w_key=w_key, w_value=w_value, gain_query=gain_query, gain_key=gain_key, w_out=w_out, gain_attn_out=gain_attn_out, gain_ff_in=gain_ff_in, w_gate=w_gate, w_up=w_up, w_down=w_down, gain_ff_out=gain_ff_out)


EPS = 1e-06
THETA = 1000000.0
SCORE_SCALE = 0.0625
GELU_C = 0.7978845608028654
GELU_A = 0.044715

def to_bf16(values):
    return lax.optimization_barrier(values.astype(jnp.bfloat16))

def rms_forward(values, gain):
    inv_rms = lax.rsqrt(lax.optimization_barrier(jnp.mean(values * values, axis=-1, keepdims=True)) + EPS)
    normed = values * inv_rms
    return (normed * gain, normed, inv_rms)

def rms_backward(normed, inv_rms, gain, upstream):
    scaled = upstream * gain
    return inv_rms * (scaled - normed * lax.optimization_barrier(jnp.mean(scaled * normed, axis=-1, keepdims=True)))

def positions_of(segment_row):
    token_count = segment_row.shape[0]
    index_row = jnp.arange(token_count, dtype=jnp.int32)
    first_pos = jnp.concatenate([jnp.ones((1,), bool), segment_row[1:] != segment_row[:-1]])
    start_row = lax.cummax(jnp.where(first_pos, index_row, 0).astype(jnp.int32), axis=0)
    return index_row - start_row

def rope_tables(positions):
    freq_index = jnp.arange(HEAD_WIDTH // 2, dtype=jnp.float32)
    inv_freq = jnp.exp(freq_index * (-2.0 * jnp.log(THETA) / HEAD_WIDTH))
    angles = positions.astype(jnp.float32)[:, None] * inv_freq[None, :]
    return (jnp.cos(angles)[:, None, :], jnp.sin(angles)[:, None, :])

def rotate(values, cos_tab, sin_tab, direction):
    half_a = values[..., :HEAD_WIDTH // 2]
    half_b = values[..., HEAD_WIDTH // 2:]
    return jnp.concatenate([half_a * cos_tab - direction * half_b * sin_tab, half_b * cos_tab + direction * half_a * sin_tab], axis=-1)

def windows(values, fill_value):
    blocks = values.shape[0] // BLOCK
    padded = jnp.concatenate([jnp.full((BLOCK,) + values.shape[1:], fill_value, values.dtype), values], axis=0)
    padded = padded.reshape((blocks + 1, BLOCK) + values.shape[1:])
    return jnp.concatenate([padded[:-1], padded[1:]], axis=1)

def window_restore(win_grad):
    own_part = win_grad[:, BLOCK:]
    next_part = jnp.concatenate([win_grad[1:, :BLOCK], jnp.zeros_like(win_grad[:1, :BLOCK])], axis=0)
    total = own_part + next_part
    return total.reshape((total.shape[0] * BLOCK,) + total.shape[2:])

def block_mask(segment_row):
    token_count = segment_row.shape[0]
    blocks = token_count // BLOCK
    index_row = jnp.arange(token_count, dtype=jnp.int32)
    key_seg = windows(segment_row, -1)
    key_index = windows(index_row, -1)
    query_seg = segment_row.reshape(blocks, BLOCK)
    query_index = index_row.reshape(blocks, BLOCK)
    return (key_seg[:, None, :] == query_seg[:, :, None]) & (key_index[:, None, :] <= query_index[:, :, None])

def attn_scores(query_rot, key_rot, seg_mask):
    token_count, head_total_count = (query_rot.shape[0], query_rot.shape[1])
    blocks = token_count // BLOCK
    query_block = query_rot.reshape(blocks, BLOCK, head_total_count, HEAD_WIDTH).astype(jnp.float32)
    key_window = windows(key_rot, 0.0).astype(jnp.float32)
    logit_scores = jnp.einsum('pjlu,pvu->pljv', query_block, key_window) * SCORE_SCALE
    return (jnp.where(seg_mask[:, None], logit_scores, -jnp.inf), query_block, key_window)

def attend_forward(query_rot, key_rot, value_b, seg_mask):
    token_count, head_total_count = (query_rot.shape[0], query_rot.shape[1])
    logit_scores, query_block, key_window = attn_scores(query_rot, key_rot, seg_mask)
    value_window = windows(value_b, 0.0).astype(jnp.float32)
    row_max = lax.optimization_barrier(jnp.max(logit_scores, axis=-1, keepdims=True))
    log_total = row_max + jnp.log(lax.optimization_barrier(jnp.sum(jnp.exp(logit_scores - row_max), axis=-1, keepdims=True)))
    attention_weights = to_bf16(jnp.exp(logit_scores - log_total)).astype(jnp.float32)
    attention_mixed = jnp.einsum('ipjv,ivx->ijpx', attention_weights, value_window).reshape(token_count, head_total_count, HEAD_WIDTH)
    return (attention_mixed, log_total)

def attend_backward(query_rot, key_rot, value_b, seg_mask, attention_mixed, log_total, grad_out):
    token_count, head_total_count = (query_rot.shape[0], query_rot.shape[1])
    blocks = token_count // BLOCK
    logit_scores, query_block, key_window = attn_scores(query_rot, key_rot, seg_mask)
    value_window = windows(value_b, 0.0).astype(jnp.float32)
    attention_weights = jnp.exp(logit_scores - log_total)
    probability_rows = to_bf16(attention_weights).astype(jnp.float32)
    gradient_block = grad_out.reshape(blocks, BLOCK, head_total_count, HEAD_WIDTH).astype(jnp.float32)
    probability_gradient = jnp.einsum('pjlu,pvu->pljv', gradient_block, value_window)
    row_delta = lax.optimization_barrier(jnp.sum(grad_out.astype(jnp.float32) * attention_mixed, axis=-1))
    row_delta = row_delta.reshape(blocks, BLOCK, head_total_count).transpose(0, 2, 1)[..., None]
    score_gradient = to_bf16(attention_weights * (probability_gradient - row_delta) * SCORE_SCALE).astype(jnp.float32)
    query_gradient = jnp.einsum('ipjv,ivx->ijpx', score_gradient, key_window).reshape(token_count, head_total_count, HEAD_WIDTH)
    key_gradient = window_restore(jnp.einsum('vptl,vtpm->vlm', score_gradient, query_block))
    value_gradient = window_restore(jnp.einsum('vptl,vtpm->vlm', probability_rows, gradient_block))
    return (query_gradient, key_gradient, value_gradient)

def dot32(left, right):
    return jnp.dot(left, right, preferred_element_type=jnp.float32)

def device_pass(inputs, upstream, segment_row, weights):
    gain_attn_in, w_query, w_key, w_value, gain_query, gain_key, w_out, gain_attn_out, gain_ff_in, w_gate, w_up, w_down, gain_ff_out = weights
    token_count = inputs.shape[0]
    cos_tab, sin_tab = rope_tables(positions_of(segment_row))
    seg_mask = block_mask(segment_row)
    normed_in, hat_in, inv_in = rms_forward(inputs, gain_attn_in)
    normed_b = to_bf16(normed_in)
    query_lin = dot32(normed_b, w_query).reshape(token_count, H, HEAD_WIDTH)
    key_lin = dot32(normed_b, w_key).reshape(token_count, 1, HEAD_WIDTH)
    value_b = to_bf16(dot32(normed_b, w_value))
    query_n, query_hat, query_inv = rms_forward(query_lin, gain_query)
    key_n, key_hat, key_inv = rms_forward(key_lin, gain_key)
    query_b = to_bf16(rotate(query_n, cos_tab, sin_tab, 1.0))
    key_b = to_bf16(rotate(key_n, cos_tab, sin_tab, 1.0))[:, 0]
    group_size = H // N_TENSOR
    mixes = []
    totals = []
    for group in range(N_TENSOR):
        attention_mixed, log_total = attend_forward(query_b[:, group * group_size:(group + 1) * group_size], key_b, value_b, seg_mask)
        mixes.append(attention_mixed)
        totals.append(log_total)
    attn_mix_all = jnp.concatenate(mixes, axis=1)
    attn_flat = to_bf16(attn_mix_all.reshape(token_count, H * HEAD_WIDTH))
    attn_sum = dot32(attn_flat, w_out)
    branch_attn, hat_attn, inv_attn = rms_forward(attn_sum, gain_attn_out)
    middle = inputs + branch_attn
    normed_mid, hat_mid, inv_mid = rms_forward(middle, gain_ff_in)
    mid_b = to_bf16(normed_mid)
    gate_proj = dot32(mid_b, w_gate)
    up_proj = dot32(mid_b, w_up)
    tanh_part = jnp.tanh(GELU_C * (gate_proj + GELU_A * gate_proj * gate_proj * gate_proj))
    gelu_val = 0.5 * gate_proj * (1.0 + tanh_part)
    act_b = to_bf16(gelu_val * up_proj)
    ff_sum = dot32(act_b, w_down)
    branch_ff, hat_ff, inv_ff = rms_forward(ff_sum, gain_ff_out)
    output = middle + branch_ff
    grad_gain_ff_out = lax.optimization_barrier(jnp.sum(upstream * hat_ff, axis=0))
    grad_ff = to_bf16(rms_backward(hat_ff, inv_ff, gain_ff_out, upstream))
    grad_w_down = dot32(act_b.T, grad_ff)
    grad_act = dot32(grad_ff, w_down.T)
    gelu_deriv = 0.5 * (1.0 + tanh_part) + 0.5 * gate_proj * (1.0 - tanh_part * tanh_part) * GELU_C * (1.0 + 3.0 * GELU_A * gate_proj * gate_proj)
    grad_gate = to_bf16(grad_act * up_proj * gelu_deriv)
    grad_up = to_bf16(grad_act * gelu_val)
    grad_w_gate = dot32(mid_b.T, grad_gate)
    grad_w_up = dot32(mid_b.T, grad_up)
    grad_mid_n = dot32(grad_gate, w_gate.T) + dot32(grad_up, w_up.T)
    grad_gain_ff_in = lax.optimization_barrier(jnp.sum(grad_mid_n * hat_mid, axis=0))
    grad_middle = upstream + rms_backward(hat_mid, inv_mid, gain_ff_in, grad_mid_n)
    grad_gain_attn_out = lax.optimization_barrier(jnp.sum(grad_middle * hat_attn, axis=0))
    grad_attn_sum = to_bf16(rms_backward(hat_attn, inv_attn, gain_attn_out, grad_middle))
    grad_w_out = dot32(attn_flat.T, grad_attn_sum)
    grad_attn = to_bf16(dot32(grad_attn_sum, w_out.T)).reshape(token_count, H, HEAD_WIDTH)
    query_grads = []
    grad_w_key = jnp.zeros((D, HEAD_WIDTH), jnp.float32)
    grad_w_value = jnp.zeros((D, HEAD_WIDTH), jnp.float32)
    grad_gain_key = jnp.zeros((HEAD_WIDTH,), jnp.float32)
    grad_normed = jnp.zeros((token_count, D), jnp.float32)
    for group in range(N_TENSOR):
        head_slice = slice(group * group_size, (group + 1) * group_size)
        query_gradient, key_gradient, value_gradient = attend_backward(query_b[:, head_slice], key_b, value_b, seg_mask, mixes[group], totals[group], grad_attn[:, head_slice])
        query_grads.append(query_gradient)
        key_grad_n = rotate(key_gradient[:, None], cos_tab, sin_tab, -1.0)
        grad_gain_key = grad_gain_key + lax.optimization_barrier(jnp.sum(key_grad_n * key_hat, axis=(0, 1)))
        key_raw = to_bf16(rms_backward(key_hat, key_inv, gain_key, key_grad_n))[:, 0]
        value_raw = to_bf16(value_gradient)
        grad_w_key = grad_w_key + dot32(normed_b.T, key_raw)
        grad_w_value = grad_w_value + dot32(normed_b.T, value_raw)
        grad_normed = grad_normed + dot32(key_raw, w_key.T) + dot32(value_raw, w_value.T)
    query_grad_n = rotate(jnp.concatenate(query_grads, axis=1), cos_tab, sin_tab, -1.0)
    grad_gain_query = lax.optimization_barrier(jnp.sum(query_grad_n * query_hat, axis=(0, 1)))
    query_raw = to_bf16(rms_backward(query_hat, query_inv, gain_query, query_grad_n)).reshape(token_count, H * HEAD_WIDTH)
    grad_w_query = dot32(normed_b.T, query_raw)
    grad_normed = grad_normed + dot32(query_raw, w_query.T)
    grad_gain_attn_in = lax.optimization_barrier(jnp.sum(grad_normed * hat_in, axis=0))
    grad_input = grad_middle + rms_backward(hat_in, inv_in, gain_attn_in, grad_normed)
    grads = (grad_gain_attn_in, grad_w_query, grad_w_key, grad_w_value, grad_gain_query, grad_gain_key, grad_w_out, grad_gain_attn_out, grad_gain_ff_in, grad_w_gate, grad_w_up, grad_w_down, grad_gain_ff_out)
    return ((output, grad_input), grads)

def reference(residual_in, cotangent, segment_ids, gain_attn_in, w_query, w_key, w_value, gain_query, gain_key, w_out, gain_attn_out, gain_ff_in, w_gate, w_up, w_down, gain_ff_out):
    weights = (gain_attn_in, w_query, w_key, w_value, gain_query, gain_key, w_out, gain_attn_out, gain_ff_in, w_gate, w_up, w_down, gain_ff_out)

    def step_fn(running, device_row):
        results, grads = device_pass(device_row[0], device_row[1], device_row[2], weights)
        return (tuple((run_val + grad_val for run_val, grad_val in zip(running, grads))), results)
    zero_grads = tuple((jnp.zeros(weight.shape, jnp.float32) for weight in weights))
    totals, results = lax.scan(step_fn, zero_grads, (residual_in, cotangent, segment_ids))
    return (results[0], results[1], totals[0], totals[1], totals[2], totals[3], totals[4], totals[5], totals[6], totals[7], totals[8], totals[9], totals[10], totals[11], totals[12])
```

```python
import functools
import jax
import jax.numpy as jnp
import numpy as np
from jax import lax
from jax.experimental import pallas as pl
from jax.experimental.pallas import tpu as pltpu
from jax.sharding import PartitionSpec as P

HEAD_WIDTH = 256
BLOCK = 512
EPS = 1e-06
THETA = 1000000.0
SCORE_SCALE = 0.0625
GELU_C = 0.7978845608028654
GELU_A = 0.044715
HALF = HEAD_WIDTH // 2
QB = 256
WIN = BLOCK + QB
LANES = 128
BF = jnp.bfloat16
F32 = jnp.float32
VMEM_LIMIT = 60 << 20


def nn(a, b):
    return lax.dot_general(a, b, (((1,), (0,)), ((), ())), preferred_element_type=F32)


def nt(a, b):
    return lax.dot_general(a, b, (((1,), (1,)), ((), ())), preferred_element_type=F32)


def tn(a, b):
    return lax.dot_general(a, b, (((0,), (0,)), ((), ())), preferred_element_type=F32)


def rms_stats(v):
    inv = lax.rsqrt(jnp.mean(v * v, axis=-1, keepdims=True) + EPS)
    return v * inv, inv


def rms_back(hat, inv, gain, up):
    scaled = up * gain
    return inv * (scaled - hat * jnp.mean(scaled * hat, axis=-1, keepdims=True))


def rotate(v, cos, sin, direction):
    a, b = v[:, :HALF], v[:, HALF:]
    if direction > 0:
        return jnp.concatenate([a * cos - b * sin, b * cos + a * sin], axis=-1)
    return jnp.concatenate([a * cos + b * sin, b * cos - a * sin], axis=-1)


def column_of(row):
    n = row.shape[1]
    return jnp.transpose(jnp.broadcast_to(row, (LANES, n)))


def rope_table():
    freq = np.arange(HALF, dtype=np.float32)
    inv_freq = np.exp(freq * np.float32(-2.0 * np.log(THETA) / HEAD_WIDTH)).astype(np.float32)
    angles = np.arange(BLOCK, dtype=np.float32)[:, None] * inv_freq[None, :]
    parts = []
    for tab in (np.cos(angles.astype(np.float64)), np.sin(angles.astype(np.float64))):
        tab = tab.astype(np.float32)
        hi = tab.astype(BF)
        lo = (tab - hi.astype(np.float32)).astype(BF)
        parts += [hi, lo]
    return np.concatenate(parts, axis=1)


def project_kernel(me, x, seg, starts, table, g_in, wq_o, wq_x, wk, wv, gq, gk,
                   q_o, q_x, ql_o, ql_x, k_out, v_out, kl_out, nb_out, cos_out, sin_out):
    i = pl.program_id(0)
    rows = x.shape[1]
    hat, _ = rms_stats(x[0])
    nb = (hat * g_in[...]).astype(BF)
    nb_out[...] = nb
    seg_col = column_of(seg[...])
    lane = lax.broadcasted_iota(jnp.int32, (rows, LANES), 1)
    start = jnp.sum(jnp.where(seg_col == lane, starts[...], 0.0), axis=1, keepdims=True)
    row = lax.broadcasted_iota(jnp.int32, (rows, 1), 0) + me[0] + (i - 1) * rows
    pos = row - start.astype(jnp.int32)
    hot = (lax.broadcasted_iota(jnp.int32, (rows, BLOCK), 1) == pos).astype(F32).astype(BF)
    cs = nn(hot, table[...])
    cos = cs[:, :LANES] + cs[:, LANES : 2 * LANES]
    sin = cs[:, 2 * LANES : 3 * LANES] + cs[:, 3 * LANES :]
    cos_out[...] = cos
    sin_out[...] = sin
    k_lin = nn(nb, wk[...])
    kl_out[...] = k_lin
    k_hat, _ = rms_stats(k_lin)
    k_out[...] = rotate(k_hat * gk[...], cos, sin, 1).astype(BF)
    v_out[...] = nn(nb, wv[...]).astype(BF)

    @pl.when(i > 0)
    def _():
        for w, lin_out, out in ((wq_o, ql_o, q_o), (wq_x, ql_x, q_x)):
            lin = nn(nb, w[...])
            lin_out[...] = lin
            for h in range(lin.shape[1] // HEAD_WIDTH):
                cols = slice(h * HEAD_WIDTH, (h + 1) * HEAD_WIDTH)
                q_hat, _ = rms_stats(lin[:, cols])
                out[:, cols] = rotate(q_hat * gq[...], cos, sin, 1).astype(BF)


def score_mask(seg_q, seg_k, rows, width):
    lane = lax.broadcasted_iota(jnp.int32, (rows, width), 1)
    sub = lax.broadcasted_iota(jnp.int32, (rows, width), 0)
    return (seg_q == seg_k) & (lane <= sub + (width - rows))


def block_kernel(x, up, seg, q_o, q_x, k, v, wo_o, wo_x, wg_o, wg_x, wu_o, wu_x, wd_o, wd_x,
                 g_ao, g_fi, g_fo,
                 out, gmid_out, ga_o, ga_x, af_o, af_x, lse_out, delta_out, mid_out, gff_out, gas_out,
                 act_o, act_x, gg_o, gg_x, gu_o, gu_x, gains,
                 mix, gate_s, up_s):
    i = pl.program_id(0)
    rows = x.shape[1]
    base = pl.multiple_of(i * rows, rows)
    k_win = k[pl.ds(base, WIN), :]
    v_win = v[pl.ds(base, WIN), :]
    seg_k = seg[:, pl.ds(base, WIN)]
    seg_q = column_of(seg[:, pl.ds(base + BLOCK, rows)])[:, :1]
    mask = score_mask(seg_q, seg_k, rows, WIN)
    heads_per = q_o.shape[1] // HEAD_WIDTH
    lses = []
    for part, (q, af) in enumerate(((q_o, af_o), (q_x, af_x))):
        for h in range(heads_per):
            cols = slice(h * HEAD_WIDTH, (h + 1) * HEAD_WIDTH)
            s = jnp.where(mask, nt(q[:, cols], k_win) * SCORE_SCALE, -jnp.inf)
            top = jnp.max(s, axis=-1, keepdims=True)
            lse = top + jnp.log(jnp.sum(jnp.exp(s - top), axis=-1, keepdims=True))
            lses.append(lse)
            p = jnp.exp(s - lse).astype(BF)
            m = nn(p, v_win)
            mix[part * heads_per + h] = m
            af[:, cols] = m.astype(BF)
    inputs = x[0]
    upstream = up[0]
    attn_sum = nn(af_o[...], wo_o[...]) + nn(af_x[...], wo_x[...])
    hat_attn, inv_attn = rms_stats(attn_sum)
    middle = inputs + hat_attn * g_ao[...]
    hat_mid, inv_mid = rms_stats(middle)
    mid_b = (hat_mid * g_fi[...]).astype(BF)
    mid_out[...] = mid_b
    ff_sum = None
    for part, (wg, wu, wd, act) in enumerate(((wg_o, wu_o, wd_o, act_o), (wg_x, wu_x, wd_x, act_x))):
        gate = nn(mid_b, wg[...])
        upp = nn(mid_b, wu[...])
        gate_s[part] = gate
        up_s[part] = upp
        th = jnp.tanh(GELU_C * (gate + GELU_A * gate * gate * gate))
        a = (0.5 * gate * (1.0 + th) * upp).astype(BF)
        act[...] = a
        f = nn(a, wd[...])
        ff_sum = f if ff_sum is None else ff_sum + f
    hat_ff, inv_ff = rms_stats(ff_sum)
    out[...] = middle + hat_ff * g_fo[...]
    gff = rms_back(hat_ff, inv_ff, g_fo[...], upstream).astype(BF)
    gff_out[...] = gff
    gmn = None
    for part, (wg, wu, wd, gg_out, gu_out) in enumerate(
        ((wg_o, wu_o, wd_o, gg_o, gu_o), (wg_x, wu_x, wd_x, gg_x, gu_x))
    ):
        gact = nt(gff, wd[...])
        gate = gate_s[part]
        upp = up_s[part]
        sq = gate * gate
        th = jnp.tanh(GELU_C * (gate + GELU_A * gate * sq))
        onep = 0.5 * (1.0 + th)
        deriv = onep + 0.5 * gate * (1.0 - th * th) * (GELU_C * (1.0 + 3.0 * GELU_A * sq))
        gg = (gact * upp * deriv).astype(BF)
        gu = (gact * (gate * onep)).astype(BF)
        gg_out[...] = gg
        gu_out[...] = gu
        t = nt(gg, wg[...]) + nt(gu, wu[...])
        gmn = t if gmn is None else gmn + t
    gmid = upstream + rms_back(hat_mid, inv_mid, g_fi[...], gmn)
    gmid_out[...] = gmid
    gas = rms_back(hat_attn, inv_attn, g_ao[...], gmid).astype(BF)
    gas_out[...] = gas
    deltas = []
    for part, (wo, ga) in enumerate(((wo_o, ga_o), (wo_x, ga_x))):
        g = nt(gas, wo[...]).astype(BF)
        ga[...] = g
        for h in range(heads_per):
            gh = g[:, h * HEAD_WIDTH : (h + 1) * HEAD_WIDTH].astype(F32)
            deltas.append(jnp.sum(gh * mix[part * heads_per + h], axis=-1, keepdims=True))
    lane = lax.broadcasted_iota(jnp.int32, (rows, LANES), 1)
    lse_all = jnp.zeros((rows, LANES), F32)
    delta_all = jnp.zeros((rows, LANES), F32)
    for n, (a, b) in enumerate(zip(lses, deltas)):
        lse_all = jnp.where(lane == n, a, lse_all)
        delta_all = jnp.where(lane == n, b, delta_all)
    lse_out[...] = lse_all
    delta_out[...] = delta_all

    @pl.when(i == 0)
    def _():
        gains[...] = jnp.zeros_like(gains)

    gains[0:1, :] += jnp.sum(upstream * hat_ff, axis=0, keepdims=True)
    gains[1:2, :] += jnp.sum(gmn * hat_mid, axis=0, keepdims=True)
    gains[2:3, :] += jnp.sum(gmid * hat_attn, axis=0, keepdims=True)


def attn_back_kernel(first, seg, q, k, v, ga, lse, delta, ql, cos, sin, gq, qraw, dk, dv, gain):
    i = pl.program_id(0)
    rows = q.shape[0]
    base = pl.multiple_of(i * rows, rows)

    @pl.when(i == 0)
    def _():
        dk[...] = jnp.zeros_like(dk)
        dv[...] = jnp.zeros_like(dv)
        gain[...] = jnp.zeros_like(gain)

    k_win = k[pl.ds(base, WIN), :]
    v_win = v[pl.ds(base, WIN), :]
    seg_k = seg[:, pl.ds(base, WIN)]
    seg_q = column_of(seg[:, pl.ds(base + BLOCK, rows)])[:, :1]
    mask = score_mask(seg_q, seg_k, rows, WIN)
    dk_sum = None
    dv_sum = None
    g_sum = None
    for h in range(q.shape[1] // HEAD_WIDTH):
        cols = slice(h * HEAD_WIDTH, (h + 1) * HEAD_WIDTH)
        qh = q[:, cols]
        gh = ga[:, cols]
        s = jnp.where(mask, nt(qh, k_win) * SCORE_SCALE, -jnp.inf)
        p = jnp.exp(s - lse[:, first + h : first + h + 1])
        dp = nt(gh, v_win)
        ds = (p * (dp - delta[:, first + h : first + h + 1]) * SCORE_SCALE).astype(BF)
        pb = p.astype(BF)
        dq = nn(ds, k_win)
        a = tn(ds, qh)
        b = tn(pb, gh)
        dk_sum = a if dk_sum is None else dk_sum + a
        dv_sum = b if dv_sum is None else dv_sum + b
        dqn = rotate(dq, cos[...], sin[...], -1)
        hat, inv = rms_stats(ql[:, cols])
        g = jnp.sum(dqn * hat, axis=0, keepdims=True)
        g_sum = g if g_sum is None else g_sum + g
        qraw[:, cols] = rms_back(hat, inv, gq[...], dqn).astype(BF)
    dk[pl.ds(base, WIN), :] += dk_sum
    dv[pl.ds(base, WIN), :] += dv_sum
    gain[...] += g_sum


def input_back_kernel(x, gmid, dk_o, dk_x, dv_o, dv_x, dk_r, dv_r, kl, cos, sin, gk, g_in,
                      qr_o, qr_x, wq_o, wq_x, wk, wv, gin_out, kraw_out, vraw_out, gains, gain_k):
    i = pl.program_id(0)
    last = pl.num_programs(0) - 1
    tail = (i == last).astype(F32)
    dk = dk_o[...] + dk_x[...] + tail * dk_r[...].astype(F32)
    dv = dv_o[...] + dv_x[...] + tail * dv_r[...].astype(F32)
    dkn = rotate(dk, cos[...], sin[...], -1)
    k_hat, k_inv = rms_stats(kl[...])
    kraw = rms_back(k_hat, k_inv, gk[...], dkn).astype(BF)
    vraw = dv.astype(BF)
    kraw_out[...] = kraw
    vraw_out[...] = vraw
    gn = nt(kraw, wk[...]) + nt(vraw, wv[...]) + nt(qr_o[...], wq_o[...]) + nt(qr_x[...], wq_x[...])
    hat, inv = rms_stats(x[0])
    gin_out[...] = gmid[...] + rms_back(hat, inv, g_in[...], gn)

    @pl.when(i == 0)
    def _():
        gains[...] = jnp.zeros_like(gains)
        gain_k[...] = jnp.zeros_like(gain_k)

    gains[...] += jnp.sum(gn * hat, axis=0, keepdims=True)
    gain_k[...] += jnp.sum(dkn * k_hat, axis=0, keepdims=True)


def whole(shape):
    return pl.BlockSpec(shape, lambda *_: (0,) * len(shape), pipeline_mode=pl.Buffered(1))


def rows_of(n, width, shift=0):
    if shift:
        return pl.BlockSpec((n, width), lambda i, *_: (jnp.maximum(i - shift, 0), 0))
    return pl.BlockSpec((n, width), lambda i, *_: (i, 0))


def params():
    return pltpu.CompilerParams(dimension_semantics=("arbitrary",), vmem_limit_bytes=VMEM_LIMIT)


def sds(shape, dtype):
    return jax.ShapeDtypeStruct(shape, dtype)


def project(first_row, x3, seg_ext, starts, table, g_in, wq_o, wq_x, wk, wv, gq, gk):
    depth = x3.shape[2]
    ext = seg_ext.shape[1]
    own = ext - BLOCK
    part = wq_o.shape[1]
    n = BLOCK
    me_block = lambda i, me: (0, jnp.maximum(me[0] // n + i - 1, 0), 0)
    return pl.pallas_call(
        project_kernel,
        grid_spec=pltpu.PrefetchScalarGridSpec(
            num_scalar_prefetch=1,
            grid=(ext // n,),
            in_specs=[
                pl.BlockSpec((1, n, depth), me_block),
                pl.BlockSpec((1, n), lambda i, *_: (0, i)),
                whole((1, LANES)),
                whole(table.shape),
                whole((1, depth)),
                whole(wq_o.shape), whole(wq_x.shape), whole(wk.shape), whole(wv.shape),
                whole((1, HEAD_WIDTH)), whole((1, HEAD_WIDTH)),
            ],
            out_specs=[
                rows_of(n, part, 1), rows_of(n, part, 1), rows_of(n, part, 1), rows_of(n, part, 1),
                rows_of(n, HEAD_WIDTH), rows_of(n, HEAD_WIDTH), rows_of(n, HEAD_WIDTH, 1),
                rows_of(n, depth, 1), rows_of(n, LANES, 1), rows_of(n, LANES, 1),
            ],
        ),
        out_shape=[
            sds((own, part), BF), sds((own, part), BF), sds((own, part), F32), sds((own, part), F32),
            sds((ext, HEAD_WIDTH), BF), sds((ext, HEAD_WIDTH), BF), sds((own, HEAD_WIDTH), F32),
            sds((own, depth), BF), sds((own, LANES), F32), sds((own, LANES), F32),
        ],
        compiler_params=params(),
        name="project",
    )(first_row, x3, seg_ext, starts, table, g_in, wq_o, wq_x, wk, wv, gq, gk)


def block_pass(first_row, x3, up3, seg_ext, q_o, q_x, k, v, weights, g_ao, g_fi, g_fo):
    depth = x3.shape[2]
    own, part = q_o.shape
    n = QB
    hidden = weights[2].shape[1]
    mine = pl.BlockSpec((1, n, depth), lambda i, me: (0, me[0] // n + i, 0))
    kern = lambda me, *refs: block_kernel(*refs)
    heads = 2 * part // HEAD_WIDTH
    return pl.pallas_call(
        kern,
        grid_spec=pltpu.PrefetchScalarGridSpec(
            num_scalar_prefetch=1,
            grid=(own // n,),
            in_specs=[mine, mine, whole(seg_ext.shape), rows_of(n, part), rows_of(n, part),
                      whole(k.shape), whole(v.shape)]
            + [whole(w.shape) for w in weights]
            + [whole((1, depth))] * 3,
            out_specs=[rows_of(n, depth)] * 2 + [rows_of(n, part)] * 4 + [rows_of(n, LANES)] * 2
            + [rows_of(n, depth)] * 3 + [rows_of(n, hidden)] * 6
            + [pl.BlockSpec((8, depth), lambda i, *_: (0, 0))],
            scratch_shapes=[
                pltpu.VMEM((heads, n, HEAD_WIDTH), F32),
                pltpu.VMEM((2, n, hidden), F32),
                pltpu.VMEM((2, n, hidden), F32),
            ],
        ),
        out_shape=[sds((own, depth), F32)] * 2 + [sds((own, part), BF)] * 4 + [sds((own, LANES), F32)] * 2
        + [sds((own, depth), BF)] * 3 + [sds((own, hidden), BF)] * 6 + [sds((8, depth), F32)],
        compiler_params=params(),
        name="block",
    )(first_row, x3, up3, seg_ext, q_o, q_x, k, v, *weights, g_ao, g_fi, g_fo)


def attn_back(first, seg_ext, q, k, v, ga, lse, delta, ql, cos, sin, gq):
    own, part = q.shape
    n = QB
    ext = k.shape[0]
    acc = pl.BlockSpec((ext, HEAD_WIDTH), lambda i: (0, 0))
    return pl.pallas_call(
        functools.partial(attn_back_kernel, first),
        grid=(own // n,),
        in_specs=[whole(seg_ext.shape), rows_of(n, part), whole(k.shape), whole(v.shape), rows_of(n, part),
                  rows_of(n, LANES), rows_of(n, LANES), rows_of(n, part), rows_of(n, LANES), rows_of(n, LANES),
                  whole((1, HEAD_WIDTH))],
        out_specs=[rows_of(n, part), acc, acc, pl.BlockSpec((1, HEAD_WIDTH), lambda i: (0, 0))],
        out_shape=[sds((own, part), BF), sds((ext, HEAD_WIDTH), F32), sds((ext, HEAD_WIDTH), F32),
                   sds((1, HEAD_WIDTH), F32)],
        compiler_params=params(),
        name="attn_back",
    )(seg_ext, q, k, v, ga, lse, delta, ql, cos, sin, gq)


def input_back(first_row, x3, gmid, dks, dvs, dk_r, dv_r, kl, cos, sin, gk, g_in, qr_o, qr_x, wq_o, wq_x, wk, wv):
    depth = x3.shape[2]
    own, part = qr_o.shape
    n = BLOCK
    kern = lambda me, *refs: input_back_kernel(*refs)
    later = pl.BlockSpec((n, HEAD_WIDTH), lambda i, *_: (i + 1, 0))
    return pl.pallas_call(
        kern,
        grid_spec=pltpu.PrefetchScalarGridSpec(
            num_scalar_prefetch=1,
            grid=(own // n,),
            in_specs=[pl.BlockSpec((1, n, depth), lambda i, me: (0, me[0] // n + i, 0)), rows_of(n, depth),
                      later, later, later, later, whole((n, HEAD_WIDTH)), whole((n, HEAD_WIDTH)),
                      rows_of(n, HEAD_WIDTH), rows_of(n, LANES), rows_of(n, LANES),
                      whole((1, HEAD_WIDTH)), whole((1, depth)), rows_of(n, part), rows_of(n, part),
                      whole(wq_o.shape), whole(wq_x.shape), whole(wk.shape), whole(wv.shape)],
            out_specs=[rows_of(n, depth), rows_of(n, HEAD_WIDTH), rows_of(n, HEAD_WIDTH),
                       pl.BlockSpec((1, depth), lambda i, *_: (0, 0)),
                       pl.BlockSpec((1, HEAD_WIDTH), lambda i, *_: (0, 0))],
        ),
        out_shape=[sds((own, depth), F32), sds((own, HEAD_WIDTH), BF), sds((own, HEAD_WIDTH), BF),
                   sds((1, depth), F32), sds((1, HEAD_WIDTH), F32)],
        compiler_params=params(),
        name="input_back",
    )(first_row, x3, gmid, dks[0], dks[1], dvs[0], dvs[1], dk_r, dv_r, kl, cos, sin, gk, g_in,
      qr_o, qr_x, wq_o, wq_x, wk, wv)


def swap(value, n_tensor):
    return lax.ppermute(value, "tensor", [(t, n_tensor - 1 - t) for t in range(n_tensor)])


def pair_sum(left_x, left_o, right, n_tensor):
    sent = tn(left_x, right).astype(BF)
    got = swap(sent, n_tensor)
    return (tn(left_o, right) + got.astype(F32)).astype(BF)


def bit_of(index, b):
    return lax.rem(lax.div(index, 2**b), 2)


def bit_orders(n_bits):
    plain = tuple(range(n_bits))
    turned = plain[1:] + plain[:1]
    lead = (plain[2],) + plain[:2] + plain[3:] if n_bits > 2 else plain[::-1]
    return plain, turned, lead


def natural_index(me, j, fixed, free):
    index = 0
    for b, flip in fixed:
        mine = bit_of(me, b)
        index = index + (1 - mine if flip else mine) * 2**b
    for k, b in enumerate(free):
        index = index + lax.rem(lax.div(j, 2 ** (len(free) - 1 - k)), 2) * 2**b
    return index


def reduce_kernel(items, kv_order, n_gain, *refs):
    n_items = len(items)
    refs = list(refs)
    take = lambda count: [refs.pop(0) for _ in range(count)]
    ins = []
    for order, given in items:
        ins.append(take(2 if given else 1))
    kv_in, g_block, g_in, gq_o, gq_x, g_k = take(6)
    outs = take(n_items)
    kv_out, gain_out = take(2)
    recvs, curs = [], []
    for order, given in items:
        n = len(order)
        first = 1 if given else 0
        recvs.append({s: refs.pop(0) for s in range(first, n)})
        curs.append({s: refs.pop(0) for s in range(1, n)})
    n_bits = len(kv_order)
    kv_core = refs.pop(0)
    kv_recv = take(n_bits)
    kv_cur = take(n_bits)
    kv_all = refs.pop(0)
    gain_own = take(n_gain)
    gain_got = take(n_gain)
    send_sems, recv_sems = take(2)

    me = lax.axis_index("dp")
    core = lax.axis_index("tensor")
    partner = lambda b: me + (1 - 2 * bit_of(me, b)) * 2**b
    barrier = pltpu.get_barrier_semaphore()
    for b in range(n_bits):
        pl.semaphore_signal(barrier, inc=1, device_id={"dp": partner(b)}, device_id_type=pl.DeviceIdType.MESH)
    pl.semaphore_signal(barrier, inc=1, device_id={"tensor": 1 - core}, device_id_type=pl.DeviceIdType.MESH)
    pl.semaphore_wait(barrier, n_bits + 1)

    counter = [0]
    sent = []

    def send(src, dst, device):
        k = counter[0]
        counter[0] += 1
        copy = pltpu.make_async_remote_copy(
            src_ref=src, dst_ref=dst, send_sem=send_sems.at[k], recv_sem=recv_sems.at[k],
            device_id=device, device_id_type=pl.DeviceIdType.MESH)
        copy.start()
        sent.append(copy)
        return copy

    flying = {}

    def start(n, s):
        order, given = items[n]
        total = len(order)
        half = 2 ** (total - s - 1)
        device = {"dp": partner(order[s])}
        if s == 0:
            copies = []
            for j in range(half):
                index = natural_index(me, j, ((order[0], True),), order[1:])
                copies.append(send(ins[n][0].at[index], recvs[n][0].at[j], device))
            flying[n] = copies
        else:
            away = (1 - bit_of(me, order[s])) * half
            flying[n] = [send(curs[n][s].at[pl.ds(away, half)], recvs[n][s], device)]

    def finish(n, s):
        order, given = items[n]
        total = len(order)
        half = 2 ** (total - s - 1)
        for copy in flying.pop(n, ()):
            copy.wait_recv()
        got = ins[n][1] if given and s == 0 else recvs[n][s]

        def keep_index(j):
            if s == 0:
                return natural_index(me, j, ((order[0], False),), order[1:])
            return bit_of(me, order[s]) * half + j

        held = ins[n][0] if s == 0 else curs[n][s]
        if s == total - 1:
            outs[n][...] = held[keep_index(0)].astype(F32) + got[0].astype(F32)
            return

        def body(j, carry):
            curs[n][s + 1][j] = (held[keep_index(j)].astype(F32) + got[j].astype(F32)).astype(BF)
            return carry

        lax.fori_loop(0, half, body, 0)
        start(n, s + 1)

    gain_own[0][...] = jnp.zeros_like(gain_own[0])
    gain_own[0][0:3, :] = g_block[0:3, :]
    gain_own[0][3:4, :] = g_in[...]
    gain_own[0][4:5, :HEAD_WIDTH] = gq_o[...] + gq_x[...]
    gain_own[0][5:6, :HEAD_WIDTH] = g_k[...]

    def gain_start(s):
        device = {"tensor": 1 - core} if s == 0 else {"dp": partner(s - 1)}
        return send(gain_own[s], gain_got[s], device)

    kv_copy = send(kv_in.at[1 - core], kv_core, {"tensor": 1 - core})
    for n, (order, given) in enumerate(items):
        if given:
            finish(n, 0)
        else:
            start(n, 0)
    gain_copy = gain_start(0)
    kv_copy.wait_recv()

    def kv_first(j, carry):
        index = natural_index(me, j, (), kv_order)
        kv_cur[0][j] = (kv_in[core, index].astype(F32) + kv_core[index].astype(F32)).astype(BF)
        return carry

    lax.fori_loop(0, 2**n_bits, kv_first, 0)

    def kv_start(s):
        half = 2 ** (n_bits - s - 1)
        away = (1 - bit_of(me, kv_order[s])) * half
        return send(kv_cur[s].at[pl.ds(away, half)], kv_recv[s], {"dp": partner(kv_order[s])})

    spot = 0
    for k, b in enumerate(kv_order):
        spot = spot + bit_of(me, b) * 2 ** (n_bits - 1 - k)
    kv_copy = kv_start(0)
    depth_of = [len(order) for order, _ in items]
    for step in range(n_bits):
        half = 2 ** (n_bits - step - 1)
        kv_copy.wait_recv()
        base = bit_of(me, kv_order[step]) * half
        if step < n_bits - 1:

            def kv_body(j, carry, step=step, base=base):
                kv_cur[step + 1][j] = (kv_cur[step][base + j].astype(F32) + kv_recv[step][j].astype(F32)).astype(BF)
                return carry

            lax.fori_loop(0, half, kv_body, 0)
            kv_copy = kv_start(step + 1)
        else:
            kv_all[core, spot] = (kv_cur[step][base].astype(F32) + kv_recv[step][0].astype(F32)).astype(BF)
        gain_copy.wait_recv()
        gain_own[step + 1][...] = gain_own[step][...] + gain_got[step][...]
        gain_copy = gain_start(step + 1)
        for n in range(n_items):
            s = step + (1 if items[n][1] else 0)
            if s < depth_of[n]:
                finish(n, s)
    gain_copy.wait_recv()
    gain_out[...] = gain_own[n_bits][...] + gain_got[n_bits][...]
    for s in reversed(range(n_bits)):
        size = 2 ** (n_bits - 1 - s)
        begin = 0
        for k in range(s + 1):
            begin = begin + bit_of(me, kv_order[k]) * 2 ** (n_bits - 1 - k)
        region = kv_all.at[core, pl.ds(begin, size)]
        copy = send(region, region, {"dp": partner(kv_order[s])})
        copy.wait_recv()
    copy = send(kv_all.at[core], kv_all.at[core], {"tensor": 1 - core})
    copy.wait_recv()

    def unpack(j, carry):
        index = natural_index(me, j, (), kv_order)
        for t in range(2):
            kv_out[t, index] = kv_all[t, j].astype(F32)
        return carry

    lax.fori_loop(0, 2**n_bits, unpack, 0)
    for copy in sent:
        copy.wait_send()


def reduce_all(n_dp, items, kv, kv_order, g_block, g_in, gq_o, gq_x, g_k):
    n_bits = len(kv_order)
    spec = []
    operands = []
    scratch = []
    outs = []
    copies = 0
    for value, got, order in items:
        n, c, width = value.shape
        given = got is not None
        spec.append((tuple(order), given))
        operands += [value, got] if given else [value]
        outs.append(sds((c, width), F32))
        first = 1 if given else 0
        scratch += [pltpu.VMEM((2 ** (n_bits - s - 1), c, width), BF) for s in range(first, n_bits)]
        scratch += [pltpu.VMEM((2 ** (n_bits - s), c, width), BF) for s in range(1, n_bits)]
        copies += n_bits - 1 + (0 if given else n // 2)
    _, n, c, width = kv.shape
    scratch += [pltpu.VMEM((n, c, width), BF)]
    scratch += [pltpu.VMEM((2 ** (n_bits - s - 1), c, width), BF) for s in range(n_bits)]
    scratch += [pltpu.VMEM((2 ** (n_bits - s), c, width), BF) for s in range(n_bits)]
    scratch += [pltpu.VMEM((2, n, c, width), BF)]
    scratch += [pltpu.VMEM((8, width), F32) for _ in range(2 * (n_bits + 1))]
    copies += 2 * n_bits + 2 + n_bits + 1
    scratch += [pltpu.SemaphoreType.DMA((copies,)), pltpu.SemaphoreType.DMA((copies,))]
    outs += [sds(kv.shape, F32), sds((8, width), F32)]
    vmem = pl.BlockSpec(memory_space=pltpu.VMEM)
    operands += [kv, g_block, g_in, gq_o, gq_x, g_k]
    return pl.pallas_call(
        functools.partial(reduce_kernel, tuple(spec), tuple(kv_order), n_bits + 1),
        out_shape=outs,
        in_specs=[vmem] * len(operands),
        out_specs=[vmem] * len(outs),
        scratch_shapes=scratch,
        compiler_params=pltpu.CompilerParams(collective_id=0, has_side_effects=True, vmem_limit_bytes=VMEM_LIMIT),
        name="reduce_all",
    )(*operands)


def first_hop(value, order, n_dp):
    n, c, width = value.shape
    b = order[0]
    me = lax.axis_index("dp")
    away = 1 - bit_of(me, b)
    view = value.reshape(n // 2 ** (b + 1), 2, 2**b, c, width)
    sent = lax.dynamic_index_in_dim(view, away, 1, keepdims=False)
    n_bits = len(order)
    high = n_bits - 1 - b
    sent = sent.reshape((2,) * (n_bits - 1) + (c, width))
    remaining = [k for k in reversed(range(n_bits)) if k != b]
    axes = [remaining.index(k) for k in order[1:]]
    sent = sent.transpose(axes + [n_bits - 1, n_bits]).reshape(n // 2, c, width)
    return lax.ppermute(sent, "dp", [(i, i ^ 2**b) for i in range(n_dp)])


def on_device(n_dp, n_tensor, residual_in, cotangent, segment_ids, gain_attn_in, w_query, w_key, w_value,
              gain_query, gain_key, w_out, gain_attn_out, gain_ff_in, w_gate, w_up, w_down, gain_ff_out):
    tokens, depth = residual_in.shape[1:]
    own = tokens // n_tensor
    me = lax.axis_index("tensor")
    first_row = (me * own).astype(jnp.int32).reshape(1)
    seg = segment_ids[0]
    seg_pad = jnp.concatenate([jnp.full((BLOCK,), -1, jnp.int32), seg])
    seg_ext = lax.dynamic_slice_in_dim(seg_pad, me * own, own + BLOCK, 0)[None]
    starts = jnp.sum((seg[None, :] < jnp.arange(LANES, dtype=jnp.int32)[:, None]).astype(F32), axis=1)[None]
    row = lambda g: g[None]
    wq_x, wo_x, wg_x, wu_x, wd_x = (swap(w, n_tensor) for w in (w_query, w_out, w_gate, w_up, w_down))
    table = jnp.asarray(rope_table())
    q_o, q_x, ql_o, ql_x, k, v, kl, nb, cos, sin = project(
        first_row, residual_in, seg_ext, starts, table, row(gain_attn_in), w_query, wq_x, w_key, w_value,
        row(gain_query), row(gain_key))
    weights = (w_out, wo_x, w_gate, wg_x, w_up, wu_x, w_down, wd_x)
    (output, gmid, ga_o, ga_x, af_o, af_x, lse, delta, mid_b, gff, gas,
     act_o, act_x, gg_o, gg_x, gu_o, gu_x, gains) = block_pass(
        first_row, residual_in, cotangent, seg_ext, q_o, q_x, k, v, weights,
        row(gain_attn_out), row(gain_ff_in), row(gain_ff_out))

    n_bits = n_dp.bit_length() - 1
    plain, turned, lead = bit_orders(n_bits)
    chunks = lambda value: value.reshape(n_dp, value.shape[0] // n_dp, value.shape[1])

    def down_pair():
        sent = tn(gff, act_x).astype(BF)
        got = swap(sent, n_tensor)
        return (tn(gff, act_o) + got.astype(F32)).astype(BF)

    down = chunks(down_pair())
    down_got = first_hop(down, plain, n_dp)
    gate = chunks(pair_sum(gg_x, gg_o, mid_b, n_tensor))
    gate_got = first_hop(gate, turned, n_dp)
    upw = chunks(pair_sum(gu_x, gu_o, mid_b, n_tensor))
    upw_got = first_hop(upw, lead, n_dp)
    out_sent = swap(tn(gas, af_x).astype(BF), n_tensor)
    out_w = chunks((tn(gas, af_o) + out_sent.astype(F32)).astype(BF))

    heads = q_o.shape[1] // HEAD_WIDTH
    qr_o, dk_o, dv_o, gq_o = attn_back(0, seg_ext, q_o, k, v, ga_o, lse, delta, ql_o, cos, sin, row(gain_query))
    qr_x, dk_x, dv_x, gq_x = attn_back(heads, seg_ext, q_x, k, v, ga_x, lse, delta, ql_x, cos, sin, row(gain_query))
    front = jnp.concatenate([dk_o[:BLOCK] + dk_x[:BLOCK], dv_o[:BLOCK] + dv_x[:BLOCK]], axis=1).astype(BF)
    back = lax.ppermute(front, "tensor", [(t, t - 1) for t in range(1, n_tensor)])
    grad_input, kraw, vraw, gain_in, gain_k = input_back(
        first_row, residual_in, gmid, (dk_o, dk_x), (dv_o, dv_x), back[:, :HEAD_WIDTH], back[:, HEAD_WIDTH:],
        kl, cos, sin, row(gain_key), row(gain_attn_in), qr_o, qr_x, w_query, wq_x, w_key, w_value)
    query = chunks(pair_sum(qr_x, qr_o, nb, n_tensor))
    kv = jnp.stack([tn(kraw, nb), tn(vraw, nb)]).astype(BF)
    kv = kv.reshape(2, n_dp, kv.shape[1] // n_dp, depth)
    s_down, s_gate, s_up, s_out, s_query, kv_sum, gain_sum = reduce_all(
        n_dp,
        [(down, down_got, plain), (gate, gate_got, turned), (upw, upw_got, lead), (out_w, None, plain),
         (query, None, turned)],
        kv, lead, gains, gain_in, gq_o, gq_x, gain_k)
    kv_sum = kv_sum.reshape(2, HEAD_WIDTH, depth)
    return (
        output[None], grad_input[None], gain_sum[3], s_query.T, kv_sum[0].T, kv_sum[1].T,
        gain_sum[4, :HEAD_WIDTH], gain_sum[5, :HEAD_WIDTH],
        s_out.T, gain_sum[2], gain_sum[1], s_gate.T, s_up.T, s_down.T, gain_sum[0],
    )


def solution(mesh):
    n_dp, n_tensor = mesh.shape["dp"], mesh.shape["tensor"]
    return jax.shard_map(
        functools.partial(on_device, n_dp, n_tensor),
        mesh=mesh,
        in_specs=(
            P("dp", None, None), P("dp", None, None), P("dp", None), P(), P(None, "tensor"), P(), P(), P(), P(),
            P("tensor", None), P(), P(), P(None, "tensor"), P(None, "tensor"), P("tensor", None), P(),
        ),
        out_specs=(
            P("dp", "tensor", None), P("dp", "tensor", None), P(), P(None, ("tensor", "dp")), P(), P(), P(), P(),
            P("tensor", "dp"), P(), P(), P(None, ("tensor", "dp")), P(None, ("tensor", "dp")), P("tensor", "dp"),
            P(),
        ),
        check_vma=False,
    )
```

```python
import functools
import jax
import jax.numpy as jnp
import numpy as np
from jax import lax
from jax.experimental import pallas as pl
from jax.experimental.pallas import tpu as pltpu
from jax.sharding import PartitionSpec as P

HEAD_WIDTH = 256
BLOCK = 512
EPS = 1e-06
THETA = 1000000.0
SCORE_SCALE = 0.0625
GELU_C = 0.7978845608028654
GELU_A = 0.044715
HALF = HEAD_WIDTH // 2
QB = 256
WIN = BLOCK + QB
LANES = 128
BF = jnp.bfloat16
F32 = jnp.float32
VMEM_LIMIT = 60 << 20


def nn(a, b):
    return lax.dot_general(a, b, (((1,), (0,)), ((), ())), preferred_element_type=F32)


def nt(a, b):
    return lax.dot_general(a, b, (((1,), (1,)), ((), ())), preferred_element_type=F32)


def tn(a, b):
    return lax.dot_general(a, b, (((0,), (0,)), ((), ())), preferred_element_type=F32)


def rms_stats(v):
    inv = lax.rsqrt(jnp.mean(v * v, axis=-1, keepdims=True) + EPS)
    return v * inv, inv


def rms_back(hat, inv, gain, up):
    scaled = up * gain
    return inv * (scaled - hat * jnp.mean(scaled * hat, axis=-1, keepdims=True))


def rotate(v, cos, sin, direction):
    a, b = v[:, :HALF], v[:, HALF:]
    if direction > 0:
        return jnp.concatenate([a * cos - b * sin, b * cos + a * sin], axis=-1)
    return jnp.concatenate([a * cos + b * sin, b * cos - a * sin], axis=-1)


def column_of(row):
    n = row.shape[1]
    return jnp.transpose(jnp.broadcast_to(row, (LANES, n)))


def rope_table():
    freq = np.arange(HALF, dtype=np.float32)
    inv_freq = np.exp(freq * np.float32(-2.0 * np.log(THETA) / HEAD_WIDTH)).astype(np.float32)
    angles = np.arange(BLOCK, dtype=np.float32)[:, None] * inv_freq[None, :]
    parts = []
    for tab in (np.cos(angles.astype(np.float64)), np.sin(angles.astype(np.float64))):
        tab = tab.astype(np.float32)
        hi = tab.astype(BF)
        lo = (tab - hi.astype(np.float32)).astype(BF)
        parts += [hi, lo]
    return np.concatenate(parts, axis=1)


def project_kernel(me, x, seg, starts, table, rows8, wq_o, wq_x, wk, wv,
                   q_o, q_x, ql_o, ql_x, k_out, v_out, kl_out, nb_out, cos_out, sin_out):
    g_in, gq, gk = gain_refs(rows8, 0, 4, 5)
    i = pl.program_id(0)
    rows = x.shape[1]
    hat, _ = rms_stats(x[0])
    nb = (hat * g_in[...]).astype(BF)
    nb_out[...] = nb
    seg_col = column_of(seg[...])
    lane = lax.broadcasted_iota(jnp.int32, (rows, LANES), 1)
    start = jnp.sum(jnp.where(seg_col == lane, starts[...], 0.0), axis=1, keepdims=True)
    row = lax.broadcasted_iota(jnp.int32, (rows, 1), 0) + me[0] + (i - 1) * rows
    pos = row - start.astype(jnp.int32)
    hot = (lax.broadcasted_iota(jnp.int32, (rows, BLOCK), 1) == pos).astype(F32).astype(BF)
    cs = nn(hot, table[...])
    cos = cs[:, :LANES] + cs[:, LANES : 2 * LANES]
    sin = cs[:, 2 * LANES : 3 * LANES] + cs[:, 3 * LANES :]
    cos_out[...] = cos
    sin_out[...] = sin
    k_lin = nn(nb, wk[...])
    kl_out[...] = k_lin
    k_hat, _ = rms_stats(k_lin)
    k_out[...] = rotate(k_hat * gk[...], cos, sin, 1).astype(BF)
    v_out[...] = nn(nb, wv[...]).astype(BF)

    @pl.when(i > 0)
    def _():
        for w, lin_out, out in ((wq_o, ql_o, q_o), (wq_x, ql_x, q_x)):
            lin = nn(nb, w[...])
            lin_out[...] = lin
            for h in range(lin.shape[1] // HEAD_WIDTH):
                cols = slice(h * HEAD_WIDTH, (h + 1) * HEAD_WIDTH)
                q_hat, _ = rms_stats(lin[:, cols])
                out[:, cols] = (rotate(q_hat * gq[...], cos, sin, 1) * SCORE_SCALE).astype(BF)


def gain_refs(rows8, *which):
    width = rows8.shape[1]
    return [rows8.at[r : r + 1, : (width if r < 4 else HEAD_WIDTH)] for r in which]


def score_mask(seg_q, seg_k, rows, width):
    lane = lax.broadcasted_iota(jnp.int32, (rows, width), 1)
    sub = lax.broadcasted_iota(jnp.int32, (rows, width), 0)
    return (seg_q == seg_k) & (lane <= sub + (width - rows))


def block_kernel(x, up, seg, q_o, q_x, k, v, wo_o, wo_x, wg_o, wg_x, wu_o, wu_x, wd_o, wd_x,
                 rows8,
                 out, gmid_out, ga_o, ga_x, af_o, af_x, lse_out, delta_out, mid_out, gff_out, gas_out,
                 act_o, act_x, gg_o, gg_x, gu_o, gu_x, gains,
                 mix, gate_s, up_s):
    g_ao, g_fi, g_fo = gain_refs(rows8, 1, 2, 3)
    i = pl.program_id(0)
    rows = x.shape[1]
    base = pl.multiple_of(i * rows, rows)
    k_win = k[pl.ds(base, WIN), :]
    v_win = v[pl.ds(base, WIN), :]
    seg_k = seg[:, pl.ds(base, WIN)]
    seg_q = column_of(seg[:, pl.ds(base + BLOCK, rows)])[:, :1]
    mask = score_mask(seg_q, seg_k, rows, WIN)
    heads_per = q_o.shape[1] // HEAD_WIDTH
    lses = []
    for part, (q, af) in enumerate(((q_o, af_o), (q_x, af_x))):
        for h in range(heads_per):
            cols = slice(h * HEAD_WIDTH, (h + 1) * HEAD_WIDTH)
            s = jnp.where(mask, nt(q[:, cols], k_win), -jnp.inf)
            top = jnp.max(s, axis=-1, keepdims=True)
            e = jnp.exp(s - top)
            mass = jnp.sum(e, axis=-1, keepdims=True)
            lses.append(top + jnp.log(mass))
            p = (e * (1.0 / mass)).astype(BF)
            m = nn(p, v_win)
            mix[part * heads_per + h] = m
            af[:, cols] = m.astype(BF)
    inputs = x[0]
    upstream = up[0]
    attn_sum = nn(af_o[...], wo_o[...]) + nn(af_x[...], wo_x[...])
    hat_attn, inv_attn = rms_stats(attn_sum)
    middle = inputs + hat_attn * g_ao[...]
    hat_mid, inv_mid = rms_stats(middle)
    mid_b = (hat_mid * g_fi[...]).astype(BF)
    mid_out[...] = mid_b
    ff_sum = None
    for part, (wg, wu, wd, act) in enumerate(((wg_o, wu_o, wd_o, act_o), (wg_x, wu_x, wd_x, act_x))):
        gate = nn(mid_b, wg[...])
        upp = nn(mid_b, wu[...])
        sq = gate * gate
        th = jnp.tanh(gate * (GELU_C + (GELU_C * GELU_A) * sq))
        onep = 0.5 + 0.5 * th
        gelu = gate * onep
        deriv = onep + gate * (1.0 - th * th) * (0.5 * GELU_C + (1.5 * GELU_C * GELU_A) * sq)
        gate_s[part] = gelu
        up_s[part] = upp * deriv
        a = (gelu * upp).astype(BF)
        act[...] = a
        f = nn(a, wd[...])
        ff_sum = f if ff_sum is None else ff_sum + f
    hat_ff, inv_ff = rms_stats(ff_sum)
    out[...] = middle + hat_ff * g_fo[...]
    gff = rms_back(hat_ff, inv_ff, g_fo[...], upstream).astype(BF)
    gff_out[...] = gff
    gmn = None
    for part, (wg, wu, wd, gg_out, gu_out) in enumerate(
        ((wg_o, wu_o, wd_o, gg_o, gu_o), (wg_x, wu_x, wd_x, gg_x, gu_x))
    ):
        gact = nt(gff, wd[...])
        gg = (gact * up_s[part]).astype(BF)
        gu = (gact * gate_s[part]).astype(BF)
        gg_out[...] = gg
        gu_out[...] = gu
        t = nt(gg, wg[...]) + nt(gu, wu[...])
        gmn = t if gmn is None else gmn + t
    gmid = upstream + rms_back(hat_mid, inv_mid, g_fi[...], gmn)
    gmid_out[...] = gmid
    gas = rms_back(hat_attn, inv_attn, g_ao[...], gmid).astype(BF)
    gas_out[...] = gas
    deltas = []
    for part, (wo, ga) in enumerate(((wo_o, ga_o), (wo_x, ga_x))):
        g = nt(gas, wo[...]).astype(BF)
        ga[...] = g
        for h in range(heads_per):
            gh = g[:, h * HEAD_WIDTH : (h + 1) * HEAD_WIDTH].astype(F32)
            deltas.append(jnp.sum(gh * mix[part * heads_per + h], axis=-1, keepdims=True))
    lane = lax.broadcasted_iota(jnp.int32, (rows, LANES), 1)
    lse_all = jnp.zeros((rows, LANES), F32)
    delta_all = jnp.zeros((rows, LANES), F32)
    for n, (a, b) in enumerate(zip(lses, deltas)):
        lse_all = jnp.where(lane == n, a, lse_all)
        delta_all = jnp.where(lane == n, b, delta_all)
    lse_out[...] = jnp.transpose(lse_all)[:8]
    delta_out[...] = jnp.transpose(delta_all)[:8]

    @pl.when(i == 0)
    def _():
        gains[...] = jnp.zeros_like(gains)

    gains[0:1, :] += jnp.sum(upstream * hat_ff, axis=0, keepdims=True)
    gains[1:2, :] += jnp.sum(gmn * hat_mid, axis=0, keepdims=True)
    gains[2:3, :] += jnp.sum(gmid * hat_attn, axis=0, keepdims=True)


def attn_back_kernel(first, seg, q, k, v, ga, lse, delta, ql, cos, sin, rows8, qraw, dk, dv, gain):
    (gq,) = gain_refs(rows8, 4)
    i = pl.program_id(0)
    rows = q.shape[0]
    base = pl.multiple_of(i * rows, rows)

    @pl.when(i == 0)
    def _():
        dk[...] = jnp.zeros_like(dk)
        dv[...] = jnp.zeros_like(dv)
        gain[...] = jnp.zeros_like(gain)

    k_win = k[pl.ds(base, WIN), :]
    v_win = v[pl.ds(base, WIN), :]
    seg_k = column_of(seg[:, pl.ds(base, WIN)])[:, :1]
    seg_q = seg[:, pl.ds(base + BLOCK, rows)]
    lane = lax.broadcasted_iota(jnp.int32, (WIN, rows), 1)
    sub = lax.broadcasted_iota(jnp.int32, (WIN, rows), 0)
    mask = (seg_q == seg_k) & (sub <= lane + (WIN - rows))
    dk_sum = None
    dv_sum = None
    g_sum = None
    for h in range(q.shape[1] // HEAD_WIDTH):
        cols = slice(h * HEAD_WIDTH, (h + 1) * HEAD_WIDTH)
        at = slice(first + h, first + h + 1)
        qh = q[:, cols]
        gh = ga[:, cols]
        s = jnp.where(mask, nt(k_win, qh), -jnp.inf)
        p = jnp.exp(s - lse[at, :])
        ds = (p * (nt(v_win, gh) - delta[at, :])).astype(BF)
        dq = tn(ds, k_win) * SCORE_SCALE
        a = nn(ds, qh)
        b = nn(p.astype(BF), gh)
        dk_sum = a if dk_sum is None else dk_sum + a
        dv_sum = b if dv_sum is None else dv_sum + b
        dqn = rotate(dq, cos[...], sin[...], -1)
        hat, inv = rms_stats(ql[:, cols])
        g = jnp.sum(dqn * hat, axis=0, keepdims=True)
        g_sum = g if g_sum is None else g_sum + g
        qraw[:, cols] = rms_back(hat, inv, gq[...], dqn).astype(BF)
    dk[pl.ds(base, WIN), :] += dk_sum
    dv[pl.ds(base, WIN), :] += dv_sum
    gain[...] += g_sum


def input_back_kernel(x, gmid, dk_o, dk_x, dv_o, dv_x, dk_r, dv_r, kl, cos, sin, rows8,
                      qr_o, qr_x, wq_o, wq_x, wk, wv, nb, gin_out, kv_out, gains, gain_k, kv_acc):
    g_in, gk = gain_refs(rows8, 0, 5)
    i = pl.program_id(0)
    last = pl.num_programs(0) - 1
    tail = (i == last).astype(F32)
    dk = dk_o[...] + dk_x[...] + tail * dk_r[...].astype(F32)
    dv = dv_o[...] + dv_x[...] + tail * dv_r[...].astype(F32)
    dkn = rotate(dk, cos[...], sin[...], -1)
    k_hat, k_inv = rms_stats(kl[...])
    kraw = rms_back(k_hat, k_inv, gk[...], dkn).astype(BF)
    vraw = dv.astype(BF)
    kv_w = tn(jnp.concatenate([kraw, vraw], axis=1), nb[...])

    @pl.when(i == 0)
    def _():
        kv_acc[...] = jnp.zeros_like(kv_acc)

    kv_acc[...] += kv_w
    kv_out[...] = kv_acc[...].astype(BF)
    gn = nt(kraw, wk[...]) + nt(vraw, wv[...]) + nt(qr_o[...], wq_o[...]) + nt(qr_x[...], wq_x[...])
    hat, inv = rms_stats(x[0])
    gin_out[...] = gmid[...] + rms_back(hat, inv, g_in[...], gn)

    @pl.when(i == 0)
    def _():
        gains[...] = jnp.zeros_like(gains)
        gain_k[...] = jnp.zeros_like(gain_k)

    gains[...] += jnp.sum(gn * hat, axis=0, keepdims=True)
    gain_k[...] += jnp.sum(dkn * k_hat, axis=0, keepdims=True)


def whole(shape):
    return pl.BlockSpec(shape, lambda *_: (0,) * len(shape), pipeline_mode=pl.Buffered(1))


def rows_of(n, width, shift=0):
    if shift:
        return pl.BlockSpec((n, width), lambda i, *_: (jnp.maximum(i - shift, 0), 0))
    return pl.BlockSpec((n, width), lambda i, *_: (i, 0))


def params():
    return pltpu.CompilerParams(dimension_semantics=("arbitrary",), vmem_limit_bytes=VMEM_LIMIT)


def cost(us):
    return pl.CostEstimate(flops=us * 10**9, bytes_accessed=us * 10**6, transcendentals=0)


def sds(shape, dtype):
    return jax.ShapeDtypeStruct(shape, dtype)


def project(first_row, x3, seg_ext, starts, table, rows8, wq_o, wq_x, wk, wv):
    depth = x3.shape[2]
    ext = seg_ext.shape[1]
    own = ext - BLOCK
    part = wq_o.shape[1]
    n = BLOCK
    me_block = lambda i, me: (0, jnp.maximum(me[0] // n + i - 1, 0), 0)
    return pl.pallas_call(
        project_kernel,
        grid_spec=pltpu.PrefetchScalarGridSpec(
            num_scalar_prefetch=1,
            grid=(ext // n,),
            in_specs=[
                pl.BlockSpec((1, n, depth), me_block),
                pl.BlockSpec((1, n), lambda i, *_: (0, i)),
                whole((1, LANES)),
                whole(table.shape),
                whole(rows8.shape),
                whole(wq_o.shape), whole(wq_x.shape), whole(wk.shape), whole(wv.shape),
            ],
            out_specs=[
                rows_of(n, part, 1), rows_of(n, part, 1), rows_of(n, part, 1), rows_of(n, part, 1),
                rows_of(n, HEAD_WIDTH), rows_of(n, HEAD_WIDTH), rows_of(n, HEAD_WIDTH, 1),
                rows_of(n, depth, 1), rows_of(n, LANES, 1), rows_of(n, LANES, 1),
            ],
        ),
        out_shape=[
            sds((own, part), BF), sds((own, part), BF), sds((own, part), F32), sds((own, part), F32),
            sds((ext, HEAD_WIDTH), BF), sds((ext, HEAD_WIDTH), BF), sds((own, HEAD_WIDTH), F32),
            sds((own, depth), BF), sds((own, LANES), F32), sds((own, LANES), F32),
        ],
        compiler_params=params(),
        cost_estimate=cost(6),
        name="project",
    )(first_row, x3, seg_ext, starts, table, rows8, wq_o, wq_x, wk, wv)


def block_pass(first_row, x3, up3, seg_ext, q_o, q_x, k, v, weights, rows8):
    depth = x3.shape[2]
    own, part = q_o.shape
    n = QB
    hidden = weights[2].shape[1]
    mine = pl.BlockSpec((1, n, depth), lambda i, me: (0, me[0] // n + i, 0))
    kern = lambda me, *refs: block_kernel(*refs)
    heads = 2 * part // HEAD_WIDTH
    return pl.pallas_call(
        kern,
        grid_spec=pltpu.PrefetchScalarGridSpec(
            num_scalar_prefetch=1,
            grid=(own // n,),
            in_specs=[mine, mine, whole(seg_ext.shape), rows_of(n, part), rows_of(n, part),
                      whole(k.shape), whole(v.shape)]
            + [whole(w.shape) for w in weights]
            + [whole(rows8.shape)],
            out_specs=[rows_of(n, depth)] * 2 + [rows_of(n, part)] * 4 + [pl.BlockSpec((8, n), lambda i, *_: (0, i))] * 2
            + [rows_of(n, depth)] * 3 + [rows_of(n, hidden)] * 6
            + [pl.BlockSpec((8, depth), lambda i, *_: (0, 0))],
            scratch_shapes=[
                pltpu.VMEM((heads, n, HEAD_WIDTH), F32),
                pltpu.VMEM((2, n, hidden), F32),
                pltpu.VMEM((2, n, hidden), F32),
            ],
        ),
        out_shape=[sds((own, depth), F32)] * 2 + [sds((own, part), BF)] * 4 + [sds((8, own), F32)] * 2
        + [sds((own, depth), BF)] * 3 + [sds((own, hidden), BF)] * 6 + [sds((8, depth), F32)],
        compiler_params=params(),
        cost_estimate=cost(40),
        name="block",
    )(first_row, x3, up3, seg_ext, q_o, q_x, k, v, *weights, rows8)


def attn_back(first, seg_ext, q, k, v, ga, lse, delta, ql, cos, sin, rows8):
    own, part = q.shape
    n = QB
    ext = k.shape[0]
    acc = pl.BlockSpec((ext, HEAD_WIDTH), lambda i: (0, 0))
    return pl.pallas_call(
        functools.partial(attn_back_kernel, first),
        grid=(own // n,),
        in_specs=[whole(seg_ext.shape), rows_of(n, part), whole(k.shape), whole(v.shape), rows_of(n, part),
                  pl.BlockSpec((8, n), lambda i: (0, i)), pl.BlockSpec((8, n), lambda i: (0, i)), rows_of(n, part),
                  rows_of(n, LANES), rows_of(n, LANES),
                  whole(rows8.shape)],
        out_specs=[rows_of(n, part), acc, acc, pl.BlockSpec((1, HEAD_WIDTH), lambda i: (0, 0))],
        out_shape=[sds((own, part), BF), sds((ext, HEAD_WIDTH), F32), sds((ext, HEAD_WIDTH), F32),
                   sds((1, HEAD_WIDTH), F32)],
        compiler_params=params(),
        cost_estimate=cost(10),
        name="attn_back",
    )(seg_ext, q, k, v, ga, lse, delta, ql, cos, sin, rows8)


def input_back(first_row, x3, gmid, dks, dvs, dk_r, dv_r, kl, cos, sin, rows8, qr_o, qr_x, wq_o, wq_x, wk, wv, nb):
    depth = x3.shape[2]
    own, part = qr_o.shape
    n = BLOCK
    kern = lambda me, *refs: input_back_kernel(*refs)
    later = pl.BlockSpec((n, HEAD_WIDTH), lambda i, *_: (i + 1, 0))
    return pl.pallas_call(
        kern,
        grid_spec=pltpu.PrefetchScalarGridSpec(
            num_scalar_prefetch=1,
            grid=(own // n,),
            in_specs=[pl.BlockSpec((1, n, depth), lambda i, me: (0, me[0] // n + i, 0)), rows_of(n, depth),
                      later, later, later, later, whole((n, HEAD_WIDTH)), whole((n, HEAD_WIDTH)),
                      rows_of(n, HEAD_WIDTH), rows_of(n, LANES), rows_of(n, LANES),
                      whole(rows8.shape), rows_of(n, part), rows_of(n, part),
                      whole(wq_o.shape), whole(wq_x.shape), whole(wk.shape), whole(wv.shape), rows_of(n, depth)],
            out_specs=[rows_of(n, depth), pl.BlockSpec((2 * HEAD_WIDTH, depth), lambda i, *_: (0, 0)),
                       pl.BlockSpec((1, depth), lambda i, *_: (0, 0)),
                       pl.BlockSpec((1, HEAD_WIDTH), lambda i, *_: (0, 0))],
            scratch_shapes=[pltpu.VMEM((2 * HEAD_WIDTH, depth), F32)],
        ),
        out_shape=[sds((own, depth), F32), sds((2 * HEAD_WIDTH, depth), BF),
                   sds((1, depth), F32), sds((1, HEAD_WIDTH), F32)],
        cost_estimate=cost(8),
        compiler_params=params(),
        name="input_back",
    )(first_row, x3, gmid, dks[0], dks[1], dvs[0], dvs[1], dk_r, dv_r, kl, cos, sin, rows8,
      qr_o, qr_x, wq_o, wq_x, wk, wv, nb)


def swap(value, n_tensor):
    return lax.ppermute(value, "tensor", [(t, n_tensor - 1 - t) for t in range(n_tensor)])


def bit_of(index, b):
    return lax.rem(lax.div(index, 2**b), 2)


def bit_orders(n_bits):
    plain = tuple(range(n_bits))
    turned = plain[1:] + plain[:1]
    lead = (plain[2],) + plain[:2] + plain[3:] if n_bits > 2 else plain[::-1]
    return plain, turned, lead


def drop_bit(index, b):
    return lax.div(index, 2 ** (b + 1)) * 2**b + lax.rem(index, 2**b)


def natural_index(me, j, fixed, free):
    index = 0
    for b, flip in fixed:
        mine = bit_of(me, b)
        index = index + (1 - mine if flip else mine) * 2**b
    for k, b in enumerate(free):
        index = index + lax.rem(lax.div(j, 2 ** (len(free) - 1 - k)), 2) * 2**b
    return index


def reduce_kernel(items, kv_order, n_gain, *refs):
    n_items = len(items)
    refs = list(refs)
    take = lambda count: [refs.pop(0) for _ in range(count)]
    ins = [take(2) for _ in items]
    kv_in, g_block, g_in, gq_o, gq_x, g_k = take(6)
    outs = take(n_items)
    kv_out, gain_out = take(2)
    recvs, curs = [], []
    for order in items:
        n = len(order)
        recvs.append({s: refs.pop(0) for s in range(1, n)})
        curs.append({s: refs.pop(0) for s in range(1, n)})
    n_bits = len(kv_order)
    kv_core = refs.pop(0)
    kv_recv = take(n_bits)
    kv_cur = take(n_bits)
    kv_all = refs.pop(0)
    gain_own = take(n_gain)
    gain_got = take(n_gain)
    send_sems, recv_sems = take(2)

    me = lax.axis_index("dp")
    core = lax.axis_index("tensor")
    partner = lambda b: me + (1 - 2 * bit_of(me, b)) * 2**b
    barrier = pltpu.get_barrier_semaphore()
    for b in range(n_bits):
        pl.semaphore_signal(barrier, inc=1, device_id={"dp": partner(b)}, device_id_type=pl.DeviceIdType.MESH)
    pl.semaphore_signal(barrier, inc=1, device_id={"tensor": 1 - core}, device_id_type=pl.DeviceIdType.MESH)
    pl.semaphore_wait(barrier, n_bits + 1)

    counter = [0]
    sent = []

    def send(src, dst, device):
        k = counter[0]
        counter[0] += 1
        copy = pltpu.make_async_remote_copy(
            src_ref=src, dst_ref=dst, send_sem=send_sems.at[k], recv_sem=recv_sems.at[k],
            device_id=device, device_id_type=pl.DeviceIdType.MESH)
        copy.start()
        sent.append(copy)
        return copy

    flying = {}

    def start(n, s):
        order = items[n]
        half = 2 ** (len(order) - s - 1)
        away = (1 - bit_of(me, order[s])) * half
        flying[n] = send(curs[n][s].at[pl.ds(away, half)], recvs[n][s], {"dp": partner(order[s])})

    def finish(n, s):
        order = items[n]
        total = len(order)
        half = 2 ** (total - s - 1)
        if s:
            flying.pop(n).wait_recv()
        got = recvs[n][s] if s else ins[n][1]
        held = curs[n][s] if s else ins[n][0]

        def keep_index(j):
            if s == 0:
                return natural_index(me, j, ((order[0], False),), order[1:])
            return bit_of(me, order[s]) * half + j

        def total_at(j):
            index = keep_index(j)
            return held[index].astype(F32) + got[j if s else drop_bit(index, order[0])].astype(F32)

        if s == total - 1:
            outs[n][...] = total_at(0)
            return

        def body(j, carry):
            curs[n][s + 1][j] = total_at(j).astype(BF)
            return carry

        lax.fori_loop(0, half, body, 0)
        start(n, s + 1)

    kv_copy = send(kv_in.at[1 - core], kv_core, {"tensor": 1 - core})
    gain_own[0][...] = jnp.zeros_like(gain_own[0])
    gain_own[0][0:3, :] = g_block[0:3, :]
    gain_own[0][3:4, :] = g_in[...]
    gain_own[0][4:5, :HEAD_WIDTH] = gq_o[...] + gq_x[...]
    gain_own[0][5:6, :HEAD_WIDTH] = g_k[...]

    def gain_start(s):
        device = {"tensor": 1 - core} if s == 0 else {"dp": partner(s - 1)}
        return send(gain_own[s], gain_got[s], device)

    gain_copy = gain_start(0)
    for n in range(n_items):
        finish(n, 0)
    kv_copy.wait_recv()

    def kv_first(j, carry):
        index = natural_index(me, j, (), kv_order)
        kv_cur[0][j] = (kv_in[core, index].astype(F32) + kv_core[index].astype(F32)).astype(BF)
        return carry

    lax.fori_loop(0, 2**n_bits, kv_first, 0)

    def kv_start(s):
        half = 2 ** (n_bits - s - 1)
        away = (1 - bit_of(me, kv_order[s])) * half
        return send(kv_cur[s].at[pl.ds(away, half)], kv_recv[s], {"dp": partner(kv_order[s])})

    spot = 0
    for k, b in enumerate(kv_order):
        spot = spot + bit_of(me, b) * 2 ** (n_bits - 1 - k)
    kv_copy = kv_start(0)
    for step in range(n_bits):
        half = 2 ** (n_bits - step - 1)
        kv_copy.wait_recv()
        base = bit_of(me, kv_order[step]) * half
        if step < n_bits - 1:

            def kv_body(j, carry, step=step, base=base):
                kv_cur[step + 1][j] = (kv_cur[step][base + j].astype(F32) + kv_recv[step][j].astype(F32)).astype(BF)
                return carry

            lax.fori_loop(0, half, kv_body, 0)
            kv_copy = kv_start(step + 1)
        else:
            kv_all[core, spot] = (kv_cur[step][base].astype(F32) + kv_recv[step][0].astype(F32)).astype(BF)
        gain_copy.wait_recv()
        gain_own[step + 1][...] = gain_own[step][...] + gain_got[step][...]
        gain_copy = gain_start(step + 1)
        for n in range(n_items):
            if step + 1 < len(items[n]):
                finish(n, step + 1)
    gain_copy.wait_recv()
    gain_out[...] = gain_own[n_bits][...] + gain_got[n_bits][...]
    for s in reversed(range(n_bits)):
        size = 2 ** (n_bits - 1 - s)
        begin = 0
        for k in range(s + 1):
            begin = begin + bit_of(me, kv_order[k]) * 2 ** (n_bits - 1 - k)
        region = kv_all.at[core, pl.ds(begin, size)]
        copy = send(region, region, {"dp": partner(kv_order[s])})
        copy.wait_recv()
    copy = send(kv_all.at[core], kv_all.at[core], {"tensor": 1 - core})
    copy.wait_recv()

    def unpack(j, carry):
        index = natural_index(me, j, (), kv_order)
        for t in range(2):
            kv_out[t, index] = kv_all[t, j].astype(F32)
        return carry

    lax.fori_loop(0, 2**n_bits, unpack, 0)
    for copy in sent:
        copy.wait_send()


def reduce_all(n_dp, items, kv, kv_order, g_block, g_in, gq_o, gq_x, g_k):
    n_bits = len(kv_order)
    spec = []
    operands = []
    scratch = []
    outs = []
    copies = 0
    for value, got, order in items:
        n, c, width = value.shape
        spec.append(tuple(order))
        operands += [value, got]
        outs.append(sds((c, width), F32))
        scratch += [pltpu.VMEM((2 ** (n_bits - s - 1), c, width), BF) for s in range(1, n_bits)]
        scratch += [pltpu.VMEM((2 ** (n_bits - s), c, width), BF) for s in range(1, n_bits)]
        copies += n_bits - 1
    _, n, c, width = kv.shape
    scratch += [pltpu.VMEM((n, c, width), BF)]
    scratch += [pltpu.VMEM((2 ** (n_bits - s - 1), c, width), BF) for s in range(n_bits)]
    scratch += [pltpu.VMEM((2 ** (n_bits - s), c, width), BF) for s in range(n_bits)]
    scratch += [pltpu.VMEM((2, n, c, width), BF)]
    scratch += [pltpu.VMEM((8, width), F32) for _ in range(2 * (n_bits + 1))]
    copies += 2 * n_bits + 2 + n_bits + 1
    scratch += [pltpu.SemaphoreType.DMA((copies,)), pltpu.SemaphoreType.DMA((copies,))]
    outs += [sds(kv.shape, F32), sds((8, width), F32)]
    vmem = pl.BlockSpec(memory_space=pltpu.VMEM)
    operands += [kv, g_block, g_in, gq_o, gq_x, g_k]
    return pl.pallas_call(
        functools.partial(reduce_kernel, tuple(spec), tuple(kv_order), n_bits + 1),
        out_shape=outs,
        in_specs=[vmem] * len(operands),
        out_specs=[vmem] * len(outs),
        scratch_shapes=scratch,
        compiler_params=pltpu.CompilerParams(collective_id=0, has_side_effects=True, vmem_limit_bytes=VMEM_LIMIT),
        name="reduce_all",
    )(*operands)


def fold_kernel(specs, me_ref, *refs):
    me = me_ref[0]
    n = len(specs)
    for k, (rest, done) in enumerate(specs):
        held, got = refs[2 * k], refs[2 * k + 1]
        keep, away = refs[2 * n + 2 * k], refs[2 * n + 2 * k + 1]
        half = 2 ** (len(rest) - 1)
        mine = bit_of(me, rest[0]) * half
        other = half - mine

        def body(j, carry, held=held, got=got, keep=keep, away=away, rest=rest, done=done, mine=mine, other=other):
            for base, dst in ((other, away), (mine, keep)):
                at = base + j
                index = at if done is None else natural_index(me, at, ((done, False),), rest)
                other_index = at if done is None else drop_bit(index, done)
                dst[j] = (held[index].astype(F32) + got[other_index].astype(F32)).astype(BF)
            return carry

        lax.fori_loop(0, half, body, 0)


def fold(me, items):
    specs, operands, outs = [], [], []
    for held, got, rest, done in items:
        specs.append((tuple(rest), done))
        operands += [held, got]
        shape = (got.shape[0] // 2,) + got.shape[1:]
        outs += [sds(shape, BF), sds(shape, BF)]
    vmem = pl.BlockSpec(memory_space=pltpu.VMEM)
    res = pl.pallas_call(
        functools.partial(fold_kernel, tuple(specs)),
        out_shape=outs,
        in_specs=[pl.BlockSpec(memory_space=pltpu.SMEM)] + [vmem] * len(operands),
        out_specs=[vmem] * len(outs),
        compiler_params=pltpu.CompilerParams(vmem_limit_bytes=VMEM_LIMIT),
        name="fold",
    )(me, *operands)
    return list(zip(res[0::2], res[1::2]))


def hop(value, b, n_dp):
    return lax.ppermute(value, "dp", [(i, i ^ 2**b) for i in range(n_dp)])


def after(value, *others):
    return lax.optimization_barrier((value,) + others)[0]


def first_hop(value, b, n_dp):
    n, c, width = value.shape
    away = 1 - bit_of(lax.axis_index("dp"), b)
    view = value.reshape(n // 2 ** (b + 1), 2, 2**b, c, width)
    sent = lax.dynamic_index_in_dim(view, away, 1, keepdims=False).reshape(n // 2, c, width)
    return hop(sent, b, n_dp), sent


def on_device(n_dp, n_tensor, residual_in, cotangent, segment_ids, gain_attn_in, w_query, w_key, w_value,
              gain_query, gain_key, w_out, gain_attn_out, gain_ff_in, w_gate, w_up, w_down, gain_ff_out):
    tokens, depth = residual_in.shape[1:]
    own = tokens // n_tensor
    me = lax.axis_index("tensor")
    first_row = (me * own).astype(jnp.int32).reshape(1)
    seg = segment_ids[0]
    seg_pad = jnp.concatenate([jnp.full((BLOCK,), -1, jnp.int32), seg])
    seg_ext = lax.dynamic_slice_in_dim(seg_pad, me * own, own + BLOCK, 0)[None]
    starts = jnp.sum((seg[None, :] < jnp.arange(LANES, dtype=jnp.int32)[:, None]).astype(F32), axis=1)[None]
    fill = lambda g: jnp.pad(g, (0, depth - g.shape[0]))
    rows8 = jnp.stack([gain_attn_in, gain_attn_out, gain_ff_in, gain_ff_out, fill(gain_query), fill(gain_key),
                       jnp.zeros_like(gain_attn_in), jnp.zeros_like(gain_attn_in)])
    wq_x, wo_x, wg_x, wu_x, wd_x = (swap(w, n_tensor) for w in (w_query, w_out, w_gate, w_up, w_down))
    table = jnp.asarray(rope_table())
    q_o, q_x, ql_o, ql_x, k, v, kl, nb, cos, sin = project(
        first_row, residual_in, seg_ext, starts, table, rows8, w_query, wq_x, w_key, w_value)
    weights = (w_out, wo_x, w_gate, wg_x, w_up, wu_x, w_down, wd_x)
    (output, gmid, ga_o, ga_x, af_o, af_x, lse, delta, mid_b, gff, gas,
     act_o, act_x, gg_o, gg_x, gu_o, gu_x, gains) = block_pass(
        first_row, residual_in, cotangent, seg_ext, q_o, q_x, k, v, weights, rows8)

    n_bits = n_dp.bit_length() - 1
    plain, turned, lead = bit_orders(n_bits)
    chunks = lambda value: value.reshape(n_dp, value.shape[0] // n_dp, value.shape[1])
    spot = lax.axis_index("dp").astype(jnp.int32).reshape(1)

    pairs = [(gff, act_x, act_o, plain), (mid_b, gg_x, gg_o, turned), (mid_b, gu_x, gu_o, lead), (gas, af_x, af_o, plain)]
    grad = lambda left, units: tn(left, units) if left is not mid_b else tn(units, left)
    orders = [order for *_, order in pairs]
    gots = []
    last = ()
    for left, units, _, _ in pairs:
        sent = grad(left, after(units, *last)).astype(BF)
        last = (sent,)
        gots.append(swap(sent, n_tensor))
    state = []
    for (left, _, units, order), got in zip(pairs, gots):
        value = chunks((grad(left, after(units, *last)) + got.astype(F32)).astype(BF))
        arrived, away = first_hop(value, order[0], n_dp)
        last = (away,)
        state.append((value, arrived))

    def advance(state, stage):
        folded = fold(spot, [(held, got, order[stage:], order[0] if stage == 1 else None)
                             for (held, got), order in zip(state, orders)])
        return [(keep, hop(away, order[stage], n_dp)) for (keep, away), order in zip(folded, orders)], folded

    heads = q_o.shape[1] // HEAD_WIDTH
    ga_o = after(ga_o, *last)
    qr_o, dk_o, dv_o, gq_o = attn_back(0, seg_ext, q_o, k, v, ga_o, lse, delta, ql_o, cos, sin, rows8)
    state = [(after(value, dv_o), got) for value, got in state]
    state, folded = advance(state, 1)
    ga_x = after(ga_x, *(away for _, away in folded))
    qr_x, dk_x, dv_x, gq_x = attn_back(heads, seg_ext, q_x, k, v, ga_x, lse, delta, ql_x, cos, sin, rows8)
    state = [(after(value, qr_x), got) for value, got in state]
    state, folded = advance(state, 2)
    dk_x, dv_x, qr_x = lax.optimization_barrier((dk_x, dv_x, qr_x, *(away for _, away in folded)))[:3]
    front = jnp.concatenate([dk_o[:BLOCK] + dk_x[:BLOCK], dv_o[:BLOCK] + dv_x[:BLOCK]], axis=1).astype(BF)
    back = lax.ppermute(front, "tensor", [(t, t - 1) for t in range(1, n_tensor)])
    query_sent = tn(qr_x, nb).astype(BF)
    query_got = swap(query_sent, n_tensor)
    query = chunks((tn(qr_o, nb) + query_got.astype(F32)).astype(BF))
    query_hop, query_away = first_hop(query, turned[0], n_dp)
    state = [(after(value, query_away), got) for value, got in state]
    for stage in range(3, n_bits):
        state, folded = advance(state, stage)
    gmid = after(gmid, query_away, *(away for _, away in folded))
    grad_input, kv, gain_in, gain_k = input_back(
        first_row, residual_in, gmid, (dk_o, dk_x), (dv_o, dv_x), back[:, :HEAD_WIDTH], back[:, HEAD_WIDTH:],
        kl, cos, sin, rows8, qr_o, qr_x, w_query, wq_x, w_key, w_value, nb)
    kv = kv.reshape(2, n_dp, HEAD_WIDTH // n_dp, depth)
    s_query, kv_sum, gain_sum = reduce_all(
        n_dp, [(query, query_hop, turned)], kv, lead, gains, gain_in, gq_o, gq_x, gain_k)
    s_down, s_gate, s_up, s_out = [keep[0].astype(F32) + got[0].astype(F32) for keep, got in state]
    kv_sum = kv_sum.reshape(2, HEAD_WIDTH, depth)
    return (
        output[None], grad_input[None], gain_sum[3], s_query.T, kv_sum[0].T, kv_sum[1].T,
        gain_sum[4, :HEAD_WIDTH], gain_sum[5, :HEAD_WIDTH],
        s_out.T, gain_sum[2], gain_sum[1], s_gate.T, s_up.T, s_down.T, gain_sum[0],
    )


def solution(mesh):
    n_dp, n_tensor = mesh.shape["dp"], mesh.shape["tensor"]
    return jax.shard_map(
        functools.partial(on_device, n_dp, n_tensor),
        mesh=mesh,
        in_specs=(
            P("dp", None, None), P("dp", None, None), P("dp", None), P(), P(None, "tensor"), P(), P(), P(), P(),
            P("tensor", None), P(), P(), P(None, "tensor"), P(None, "tensor"), P("tensor", None), P(),
        ),
        out_specs=(
            P("dp", "tensor", None), P("dp", "tensor", None), P(), P(None, ("tensor", "dp")), P(), P(), P(), P(),
            P("tensor", "dp"), P(), P(), P(None, ("tensor", "dp")), P(None, ("tensor", "dp")), P("tensor", "dp"),
            P(),
        ),
        check_vma=False,
    )
```

```python
import functools
import jax
import jax.numpy as jnp
import numpy as np
from jax import lax
from jax.experimental import pallas as pl
from jax.experimental.pallas import tpu as pltpu
from jax.sharding import PartitionSpec as P

HEAD_WIDTH = 256
BLOCK = 512
EPS = 1e-06
THETA = 1000000.0
SCORE_SCALE = 0.0625
GELU_C = 0.7978845608028654
GELU_A = 0.044715
HALF = HEAD_WIDTH // 2
QB = 256
WIN = BLOCK + QB
LANES = 128
BF = jnp.bfloat16
F32 = jnp.float32
VMEM_LIMIT = 60 << 20


def nn(a, b):
    return lax.dot_general(a, b, (((1,), (0,)), ((), ())), preferred_element_type=F32)


def nt(a, b):
    return lax.dot_general(a, b, (((1,), (1,)), ((), ())), preferred_element_type=F32)


def tn(a, b):
    return lax.dot_general(a, b, (((0,), (0,)), ((), ())), preferred_element_type=F32)


def rms_stats(v):
    inv = lax.rsqrt(jnp.mean(v * v, axis=-1, keepdims=True) + EPS)
    return v * inv, inv


def rms_back(hat, inv, gain, up):
    scaled = up * gain
    return inv * (scaled - hat * jnp.mean(scaled * hat, axis=-1, keepdims=True))


def rotate(v, cos, sin, direction):
    a, b = v[:, :HALF], v[:, HALF:]
    if direction > 0:
        return jnp.concatenate([a * cos - b * sin, b * cos + a * sin], axis=-1)
    return jnp.concatenate([a * cos + b * sin, b * cos - a * sin], axis=-1)


def column_of(row):
    n = row.shape[1]
    return jnp.transpose(jnp.broadcast_to(row, (LANES, n)))


def rope_table():
    freq = np.arange(HALF, dtype=np.float32)
    inv_freq = np.exp(freq * np.float32(-2.0 * np.log(THETA) / HEAD_WIDTH)).astype(np.float32)
    angles = np.arange(BLOCK, dtype=np.float32)[:, None] * inv_freq[None, :]
    parts = []
    for tab in (np.cos(angles.astype(np.float64)), np.sin(angles.astype(np.float64))):
        tab = tab.astype(np.float32)
        hi = tab.astype(BF)
        lo = (tab - hi.astype(np.float32)).astype(BF)
        parts += [hi, lo]
    return np.concatenate(parts, axis=1)


def project_kernel(me, x, seg, starts, table, rows8, wq_o, wq_x, wk, wv,
                   q_o, q_x, ql_o, ql_x, k_out, v_out, kl_out, nb_out, cos_out, sin_out):
    g_in, gq, gk = gain_refs(rows8, 0, 4, 5)
    i = pl.program_id(0)
    rows = x.shape[1]
    hat, _ = rms_stats(x[0])
    nb = (hat * g_in[...]).astype(BF)
    nb_out[...] = nb
    seg_col = column_of(seg[...])
    lane = lax.broadcasted_iota(jnp.int32, (rows, LANES), 1)
    start = jnp.sum(jnp.where(seg_col == lane, starts[...], 0.0), axis=1, keepdims=True)
    row = lax.broadcasted_iota(jnp.int32, (rows, 1), 0) + me[0] + (i - 1) * rows
    pos = row - start.astype(jnp.int32)
    hot = (lax.broadcasted_iota(jnp.int32, (rows, BLOCK), 1) == pos).astype(F32).astype(BF)
    cs = nn(hot, table[...])
    cos = cs[:, :LANES] + cs[:, LANES : 2 * LANES]
    sin = cs[:, 2 * LANES : 3 * LANES] + cs[:, 3 * LANES :]
    cos_out[...] = cos
    sin_out[...] = sin
    k_lin = nn(nb, wk[...])
    kl_out[...] = k_lin
    k_hat, _ = rms_stats(k_lin)
    k_out[...] = rotate(k_hat * gk[...], cos, sin, 1).astype(BF)
    v_out[...] = nn(nb, wv[...]).astype(BF)

    @pl.when(i > 0)
    def _():
        for w, lin_out, out in ((wq_o, ql_o, q_o), (wq_x, ql_x, q_x)):
            lin = nn(nb, w[...])
            lin_out[...] = lin
            for h in range(lin.shape[1] // HEAD_WIDTH):
                cols = slice(h * HEAD_WIDTH, (h + 1) * HEAD_WIDTH)
                q_hat, _ = rms_stats(lin[:, cols])
                out[:, cols] = (rotate(q_hat * gq[...], cos, sin, 1) * SCORE_SCALE).astype(BF)


def gain_refs(rows8, *which):
    width = rows8.shape[1]
    return [rows8.at[r : r + 1, : (width if r < 4 else HEAD_WIDTH)] for r in which]


def score_mask(seg_q, seg_k, rows, width):
    lane = lax.broadcasted_iota(jnp.int32, (rows, width), 1)
    sub = lax.broadcasted_iota(jnp.int32, (rows, width), 0)
    return (seg_q == seg_k) & (lane <= sub + (width - rows))


def block_kernel(x, up, seg, q_o, q_x, k, v, wo_o, wo_x, wg_o, wg_x, wu_o, wu_x, wd_o, wd_x,
                 rows8,
                 out, gmid_out, ga_o, ga_x, af_o, af_x, lse_out, delta_out, mid_out, gff_out, gas_out,
                 act_o, act_x, gg_o, gg_x, gu_o, gu_x, gains,
                 mix, gate_s, up_s):
    g_ao, g_fi, g_fo = gain_refs(rows8, 1, 2, 3)
    i = pl.program_id(0)
    rows = x.shape[1]
    base = pl.multiple_of(i * rows, rows)
    k_win = k[pl.ds(base, WIN), :]
    v_win = v[pl.ds(base, WIN), :]
    seg_k = seg[:, pl.ds(base, WIN)]
    seg_q = column_of(seg[:, pl.ds(base + BLOCK, rows)])[:, :1]
    mask = score_mask(seg_q, seg_k, rows, WIN)
    heads_per = q_o.shape[1] // HEAD_WIDTH
    lses = []
    for part, (q, af) in enumerate(((q_o, af_o), (q_x, af_x))):
        for h in range(heads_per):
            cols = slice(h * HEAD_WIDTH, (h + 1) * HEAD_WIDTH)
            s = jnp.where(mask, nt(q[:, cols], k_win), -jnp.inf)
            top = jnp.max(s, axis=-1, keepdims=True)
            e = jnp.exp(s - top)
            mass = jnp.sum(e, axis=-1, keepdims=True)
            lses.append(top + jnp.log(mass))
            p = (e * (1.0 / mass)).astype(BF)
            m = nn(p, v_win)
            mix[part * heads_per + h] = m
            af[:, cols] = m.astype(BF)
    inputs = x[0]
    upstream = up[0]
    attn_sum = nn(af_o[...], wo_o[...]) + nn(af_x[...], wo_x[...])
    hat_attn, inv_attn = rms_stats(attn_sum)
    middle = inputs + hat_attn * g_ao[...]
    hat_mid, inv_mid = rms_stats(middle)
    mid_b = (hat_mid * g_fi[...]).astype(BF)
    mid_out[...] = mid_b
    ff_sum = None
    for part, (wg, wu, wd, act) in enumerate(((wg_o, wu_o, wd_o, act_o), (wg_x, wu_x, wd_x, act_x))):
        gate = nn(mid_b, wg[...])
        upp = nn(mid_b, wu[...])
        sq = gate * gate
        th = jnp.tanh(gate * (GELU_C + (GELU_C * GELU_A) * sq))
        onep = 0.5 + 0.5 * th
        gelu = gate * onep
        deriv = onep + gate * (1.0 - th * th) * (0.5 * GELU_C + (1.5 * GELU_C * GELU_A) * sq)
        gate_s[part] = gelu
        up_s[part] = upp * deriv
        a = (gelu * upp).astype(BF)
        act[...] = a
        f = nn(a, wd[...])
        ff_sum = f if ff_sum is None else ff_sum + f
    hat_ff, inv_ff = rms_stats(ff_sum)
    out[...] = middle + hat_ff * g_fo[...]
    gff = rms_back(hat_ff, inv_ff, g_fo[...], upstream).astype(BF)
    gff_out[...] = gff
    gmn = None
    for part, (wg, wu, wd, gg_out, gu_out) in enumerate(
        ((wg_o, wu_o, wd_o, gg_o, gu_o), (wg_x, wu_x, wd_x, gg_x, gu_x))
    ):
        gact = nt(gff, wd[...])
        gg = (gact * up_s[part]).astype(BF)
        gu = (gact * gate_s[part]).astype(BF)
        gg_out[...] = gg
        gu_out[...] = gu
        t = nt(gg, wg[...]) + nt(gu, wu[...])
        gmn = t if gmn is None else gmn + t
    gmid = upstream + rms_back(hat_mid, inv_mid, g_fi[...], gmn)
    gmid_out[...] = gmid
    gas = rms_back(hat_attn, inv_attn, g_ao[...], gmid).astype(BF)
    gas_out[...] = gas
    deltas = []
    for part, (wo, ga) in enumerate(((wo_o, ga_o), (wo_x, ga_x))):
        g = nt(gas, wo[...]).astype(BF)
        ga[...] = g
        for h in range(heads_per):
            gh = g[:, h * HEAD_WIDTH : (h + 1) * HEAD_WIDTH].astype(F32)
            deltas.append(jnp.sum(gh * mix[part * heads_per + h], axis=-1, keepdims=True))
    lane = lax.broadcasted_iota(jnp.int32, (rows, LANES), 1)
    lse_all = jnp.zeros((rows, LANES), F32)
    delta_all = jnp.zeros((rows, LANES), F32)
    for n, (a, b) in enumerate(zip(lses, deltas)):
        lse_all = jnp.where(lane == n, a, lse_all)
        delta_all = jnp.where(lane == n, b, delta_all)
    lse_out[...] = jnp.transpose(lse_all)[:8]
    delta_out[...] = jnp.transpose(delta_all)[:8]

    @pl.when(i == 0)
    def _():
        gains[...] = jnp.zeros_like(gains)

    gains[0:1, :] += jnp.sum(upstream * hat_ff, axis=0, keepdims=True)
    gains[1:2, :] += jnp.sum(gmn * hat_mid, axis=0, keepdims=True)
    gains[2:3, :] += jnp.sum(gmid * hat_attn, axis=0, keepdims=True)


def attn_back_kernel(seg, q_o, q_x, k, v, ga_o, ga_x, lse, delta, ql_o, ql_x, cos, sin, rows8,
                     qr_o, qr_x, dk_out, dv_out, front, gain, dk, dv):
    (gq,) = gain_refs(rows8, 4)
    i = pl.program_id(0)
    rows = q_o.shape[0]
    base = pl.multiple_of(i * rows, rows)

    @pl.when(i == 0)
    def _():
        dk[...] = jnp.zeros_like(dk)
        dv[...] = jnp.zeros_like(dv)
        gain[...] = jnp.zeros_like(gain)

    k_win = k[pl.ds(base, WIN), :]
    v_win = v[pl.ds(base, WIN), :]
    seg_k = column_of(seg[:, pl.ds(base, WIN)])[:, :1]
    seg_q = seg[:, pl.ds(base + BLOCK, rows)]
    lane = lax.broadcasted_iota(jnp.int32, (WIN, rows), 1)
    sub = lax.broadcasted_iota(jnp.int32, (WIN, rows), 0)
    mask = (seg_q == seg_k) & (sub <= lane + (WIN - rows))
    dk_sum = None
    dv_sum = None
    g_sum = None
    heads = q_o.shape[1] // HEAD_WIDTH
    for n in range(2 * heads):
        q, ga, ql, qraw = ((q_o, ga_o, ql_o, qr_o), (q_x, ga_x, ql_x, qr_x))[n // heads]
        h = n % heads
        cols = slice(h * HEAD_WIDTH, (h + 1) * HEAD_WIDTH)
        qh = q[:, cols]
        gh = ga[:, cols]
        s = jnp.where(mask, nt(k_win, qh), -jnp.inf)
        p = jnp.exp(s - lse[n : n + 1, :])
        ds = (p * (nt(v_win, gh) - delta[n : n + 1, :])).astype(BF)
        dq = tn(ds, k_win) * SCORE_SCALE
        a = nn(ds, qh)
        b = nn(p.astype(BF), gh)
        dk_sum = a if dk_sum is None else dk_sum + a
        dv_sum = b if dv_sum is None else dv_sum + b
        dqn = rotate(dq, cos[...], sin[...], -1)
        hat, inv = rms_stats(ql[:, cols])
        g = jnp.sum(dqn * hat, axis=0, keepdims=True)
        g_sum = g if g_sum is None else g_sum + g
        qraw[:, cols] = rms_back(hat, inv, gq[...], dqn).astype(BF)
    dk[pl.ds(base, WIN), :] += dk_sum
    dv[pl.ds(base, WIN), :] += dv_sum
    gain[...] += g_sum

    @pl.when(i == pl.num_programs(0) - 1)
    def _():
        front[:, :HEAD_WIDTH] = dk[:BLOCK, :].astype(BF)
        front[:, HEAD_WIDTH:] = dv[:BLOCK, :].astype(BF)
        dk_out[...] = dk[BLOCK:, :]
        dv_out[...] = dv[BLOCK:, :]


def input_back_kernel(x, gmid, dk_own, dv_own, back, kl, cos, sin, rows8,
                      qr_o, qr_x, wq_o, wq_x, wk, wv, nb, gin_out, kv_out, gains, gain_k, kv_acc):
    g_in, gk = gain_refs(rows8, 0, 5)
    i = pl.program_id(0)
    last = pl.num_programs(0) - 1
    tail = (i == last).astype(F32)
    dk = dk_own[...] + tail * back[:, :HEAD_WIDTH].astype(F32)
    dv = dv_own[...] + tail * back[:, HEAD_WIDTH:].astype(F32)
    dkn = rotate(dk, cos[...], sin[...], -1)
    k_hat, k_inv = rms_stats(kl[...])
    kraw = rms_back(k_hat, k_inv, gk[...], dkn).astype(BF)
    vraw = dv.astype(BF)
    kv_w = tn(jnp.concatenate([kraw, vraw], axis=1), nb[...])

    @pl.when(i == 0)
    def _():
        kv_acc[...] = jnp.zeros_like(kv_acc)

    kv_acc[...] += kv_w
    kv_out[...] = kv_acc[...].astype(BF)
    gn = nt(kraw, wk[...]) + nt(vraw, wv[...]) + nt(qr_o[...], wq_o[...]) + nt(qr_x[...], wq_x[...])
    hat, inv = rms_stats(x[0])
    gin_out[...] = gmid[...] + rms_back(hat, inv, g_in[...], gn)

    @pl.when(i == 0)
    def _():
        gains[...] = jnp.zeros_like(gains)
        gain_k[...] = jnp.zeros_like(gain_k)

    gains[...] += jnp.sum(gn * hat, axis=0, keepdims=True)
    gain_k[...] += jnp.sum(dkn * k_hat, axis=0, keepdims=True)


def whole(shape):
    return pl.BlockSpec(shape, lambda *_: (0,) * len(shape), pipeline_mode=pl.Buffered(1))


def rows_of(n, width, shift=0):
    if shift:
        return pl.BlockSpec((n, width), lambda i, *_: (jnp.maximum(i - shift, 0), 0))
    return pl.BlockSpec((n, width), lambda i, *_: (i, 0))


def params():
    return pltpu.CompilerParams(dimension_semantics=("arbitrary",), vmem_limit_bytes=VMEM_LIMIT)


def cost(us):
    return pl.CostEstimate(flops=us * 10**9, bytes_accessed=us * 10**6, transcendentals=0)


def sds(shape, dtype):
    return jax.ShapeDtypeStruct(shape, dtype)


def project(first_row, x3, seg_ext, starts, table, rows8, wq_o, wq_x, wk, wv):
    depth = x3.shape[2]
    ext = seg_ext.shape[1]
    own = ext - BLOCK
    part = wq_o.shape[1]
    n = BLOCK
    me_block = lambda i, me: (0, jnp.maximum(me[0] // n + i - 1, 0), 0)
    return pl.pallas_call(
        project_kernel,
        grid_spec=pltpu.PrefetchScalarGridSpec(
            num_scalar_prefetch=1,
            grid=(ext // n,),
            in_specs=[
                pl.BlockSpec((1, n, depth), me_block),
                pl.BlockSpec((1, n), lambda i, *_: (0, i)),
                whole((1, LANES)),
                whole(table.shape),
                whole(rows8.shape),
                whole(wq_o.shape), whole(wq_x.shape), whole(wk.shape), whole(wv.shape),
            ],
            out_specs=[
                rows_of(n, part, 1), rows_of(n, part, 1), rows_of(n, part, 1), rows_of(n, part, 1),
                rows_of(n, HEAD_WIDTH), rows_of(n, HEAD_WIDTH), rows_of(n, HEAD_WIDTH, 1),
                rows_of(n, depth, 1), rows_of(n, LANES, 1), rows_of(n, LANES, 1),
            ],
        ),
        out_shape=[
            sds((own, part), BF), sds((own, part), BF), sds((own, part), F32), sds((own, part), F32),
            sds((ext, HEAD_WIDTH), BF), sds((ext, HEAD_WIDTH), BF), sds((own, HEAD_WIDTH), F32),
            sds((own, depth), BF), sds((own, LANES), F32), sds((own, LANES), F32),
        ],
        compiler_params=params(),
        cost_estimate=cost(6),
        name="project",
    )(first_row, x3, seg_ext, starts, table, rows8, wq_o, wq_x, wk, wv)


def block_pass(first_row, x3, up3, seg_ext, q_o, q_x, k, v, weights, rows8):
    depth = x3.shape[2]
    own, part = q_o.shape
    n = QB
    hidden = weights[2].shape[1]
    mine = pl.BlockSpec((1, n, depth), lambda i, me: (0, me[0] // n + i, 0))
    kern = lambda me, *refs: block_kernel(*refs)
    heads = 2 * part // HEAD_WIDTH
    return pl.pallas_call(
        kern,
        grid_spec=pltpu.PrefetchScalarGridSpec(
            num_scalar_prefetch=1,
            grid=(own // n,),
            in_specs=[mine, mine, whole(seg_ext.shape), rows_of(n, part), rows_of(n, part),
                      whole(k.shape), whole(v.shape)]
            + [whole(w.shape) for w in weights]
            + [whole(rows8.shape)],
            out_specs=[rows_of(n, depth)] * 2 + [rows_of(n, part)] * 4 + [pl.BlockSpec((8, n), lambda i, *_: (0, i))] * 2
            + [rows_of(n, depth)] * 3 + [rows_of(n, hidden)] * 6
            + [pl.BlockSpec((8, depth), lambda i, *_: (0, 0))],
            scratch_shapes=[
                pltpu.VMEM((heads, n, HEAD_WIDTH), F32),
                pltpu.VMEM((2, n, hidden), F32),
                pltpu.VMEM((2, n, hidden), F32),
            ],
        ),
        out_shape=[sds((own, depth), F32)] * 2 + [sds((own, part), BF)] * 4 + [sds((8, own), F32)] * 2
        + [sds((own, depth), BF)] * 3 + [sds((own, hidden), BF)] * 6 + [sds((8, depth), F32)],
        compiler_params=params(),
        cost_estimate=cost(40),
        name="block",
    )(first_row, x3, up3, seg_ext, q_o, q_x, k, v, *weights, rows8)


def attn_back(seg_ext, q_o, q_x, k, v, ga_o, ga_x, lse, delta, ql_o, ql_x, cos, sin, rows8):
    own, part = q_o.shape
    n = QB
    ext = k.shape[0]
    fixed = lambda shape: pl.BlockSpec(shape, lambda i: (0, 0))
    stat = pl.BlockSpec((8, n), lambda i: (0, i))
    return pl.pallas_call(
        attn_back_kernel,
        grid=(own // n,),
        in_specs=[whole(seg_ext.shape), rows_of(n, part), rows_of(n, part), whole(k.shape), whole(v.shape),
                  rows_of(n, part), rows_of(n, part), stat, stat, rows_of(n, part), rows_of(n, part),
                  rows_of(n, LANES), rows_of(n, LANES), whole(rows8.shape)],
        out_specs=[rows_of(n, part), rows_of(n, part), fixed((own, HEAD_WIDTH)), fixed((own, HEAD_WIDTH)),
                   fixed((BLOCK, 2 * HEAD_WIDTH)), fixed((1, HEAD_WIDTH))],
        out_shape=[sds((own, part), BF), sds((own, part), BF), sds((own, HEAD_WIDTH), F32),
                   sds((own, HEAD_WIDTH), F32), sds((BLOCK, 2 * HEAD_WIDTH), BF), sds((1, HEAD_WIDTH), F32)],
        scratch_shapes=[pltpu.VMEM((ext, HEAD_WIDTH), F32), pltpu.VMEM((ext, HEAD_WIDTH), F32)],
        compiler_params=params(),
        cost_estimate=cost(20),
        name="attn_back",
    )(seg_ext, q_o, q_x, k, v, ga_o, ga_x, lse, delta, ql_o, ql_x, cos, sin, rows8)


def input_back(first_row, x3, gmid, dk, dv, back, kl, cos, sin, rows8, qr_o, qr_x, wq_o, wq_x, wk, wv, nb):
    depth = x3.shape[2]
    own, part = qr_o.shape
    n = BLOCK
    kern = lambda me, *refs: input_back_kernel(*refs)
    return pl.pallas_call(
        kern,
        grid_spec=pltpu.PrefetchScalarGridSpec(
            num_scalar_prefetch=1,
            grid=(own // n,),
            in_specs=[pl.BlockSpec((1, n, depth), lambda i, me: (0, me[0] // n + i, 0)), rows_of(n, depth),
                      rows_of(n, HEAD_WIDTH), rows_of(n, HEAD_WIDTH), whole(back.shape),
                      rows_of(n, HEAD_WIDTH), rows_of(n, LANES), rows_of(n, LANES),
                      whole(rows8.shape), rows_of(n, part), rows_of(n, part),
                      whole(wq_o.shape), whole(wq_x.shape), whole(wk.shape), whole(wv.shape), rows_of(n, depth)],
            out_specs=[rows_of(n, depth), pl.BlockSpec((2 * HEAD_WIDTH, depth), lambda i, *_: (0, 0)),
                       pl.BlockSpec((1, depth), lambda i, *_: (0, 0)),
                       pl.BlockSpec((1, HEAD_WIDTH), lambda i, *_: (0, 0))],
            scratch_shapes=[pltpu.VMEM((2 * HEAD_WIDTH, depth), F32)],
        ),
        out_shape=[sds((own, depth), F32), sds((2 * HEAD_WIDTH, depth), BF),
                   sds((1, depth), F32), sds((1, HEAD_WIDTH), F32)],
        cost_estimate=cost(8),
        compiler_params=params(),
        name="input_back",
    )(first_row, x3, gmid, dk, dv, back, kl, cos, sin, rows8,
      qr_o, qr_x, wq_o, wq_x, wk, wv, nb)


def swap(value, n_tensor):
    return lax.ppermute(value, "tensor", [(t, n_tensor - 1 - t) for t in range(n_tensor)])


def bit_of(index, b):
    return lax.rem(lax.div(index, 2**b), 2)


def bit_orders(n_bits):
    plain = tuple(range(n_bits))
    turned = plain[1:] + plain[:1]
    lead = (plain[2],) + plain[:2] + plain[3:] if n_bits > 2 else plain[::-1]
    return plain, turned, lead


def drop_bit(index, b):
    return lax.div(index, 2 ** (b + 1)) * 2**b + lax.rem(index, 2**b)


def natural_index(me, j, fixed, free):
    index = 0
    for b, flip in fixed:
        mine = bit_of(me, b)
        index = index + (1 - mine if flip else mine) * 2**b
    for k, b in enumerate(free):
        index = index + lax.rem(lax.div(j, 2 ** (len(free) - 1 - k)), 2) * 2**b
    return index


def reduce_kernel(items, kv_groups, n_bits, *refs):
    n_items = len(items)
    kv_order = sum(kv_groups, ())
    refs = list(refs)
    take = lambda count: [refs.pop(0) for _ in range(count)]
    ins = [take(2 if given else 1) for _, given in items]
    kv_in, g_block, g_in, g_q, g_k = take(5)
    outs = take(n_items)
    k_out, v_out, gain_out = take(3)
    recvs, curs = [], []
    for order, given in items:
        first = 1 if given else 0
        recvs.append({s: refs.pop(0) for s in range(first, n_bits)})
        curs.append({s: refs.pop(0) for s in range(1, n_bits)})
    kv_core = refs.pop(0)
    kv_recv = take(len(kv_groups))
    kv_cur = take(len(kv_groups))
    kv_all = refs.pop(0)
    gain_own = take(n_bits + 1)
    gain_got = take(n_bits + 1)
    send_sems, recv_sems = take(2)

    me = lax.axis_index("dp")
    core = lax.axis_index("tensor")

    def flipped(bits):
        return me + sum((1 - 2 * bit_of(me, b)) * 2**b for b in bits)

    def subsets(group):
        return [tuple(b for k, b in enumerate(group) if m >> k & 1) for m in range(1, 2 ** len(group))]

    peers = {(b,) for b in range(n_bits)} | {tuple(sorted(m)) for g in kv_groups for m in subsets(g)}
    barrier = pltpu.get_barrier_semaphore()
    for bits in sorted(peers):
        pl.semaphore_signal(barrier, inc=1, device_id={"dp": flipped(bits)}, device_id_type=pl.DeviceIdType.MESH)
    pl.semaphore_signal(barrier, inc=1, device_id={"tensor": 1 - core}, device_id_type=pl.DeviceIdType.MESH)
    pl.semaphore_wait(barrier, len(peers) + 1)

    sent = []

    def send(src, dst, device):
        k = len(sent)
        copy = pltpu.make_async_remote_copy(
            src_ref=src, dst_ref=dst, send_sem=send_sems.at[k], recv_sem=recv_sems.at[k],
            device_id=device, device_id_type=pl.DeviceIdType.MESH)
        copy.start()
        sent.append(copy)
        return copy

    flying = {}

    def start(n, s):
        order, _ = items[n]
        half = 2 ** (n_bits - s - 1)
        device = {"dp": flipped((order[s],))}
        if s == 0:
            flying[n] = [
                send(ins[n][0].at[natural_index(me, j, ((order[0], True),), order[1:])], recvs[n][0].at[j], device)
                for j in range(half)
            ]
        else:
            away = (1 - bit_of(me, order[s])) * half
            flying[n] = [send(curs[n][s].at[pl.ds(away, half)], recvs[n][s], device)]

    def finish(n, s):
        order, given = items[n]
        half = 2 ** (n_bits - s - 1)
        for copy in flying.pop(n, ()):
            copy.wait_recv()
        outside = given and s == 0
        got = ins[n][1] if outside else recvs[n][s]
        held = curs[n][s] if s else ins[n][0]

        def total_at(j):
            if s:
                index = bit_of(me, order[s]) * half + j
            else:
                index = natural_index(me, j, ((order[0], False),), order[1:])
            return held[index].astype(F32) + got[drop_bit(index, order[0]) if outside else j].astype(F32)

        if s == n_bits - 1:
            outs[n][...] = total_at(0)
            return

        def body(j, carry):
            curs[n][s + 1][j] = total_at(j).astype(BF)
            return carry

        lax.fori_loop(0, half, body, 0)
        start(n, s + 1)

    kv_copies = [send(kv_in.at[1 - core], kv_core, {"tensor": 1 - core})]
    for n in range(n_items):
        if not items[n][1]:
            start(n, 0)
    gain_own[0][...] = jnp.zeros_like(gain_own[0])
    gain_own[0][0:3, :] = g_block[0:3, :]
    gain_own[0][3:4, :] = g_in[...]
    gain_own[0][4:5, :HEAD_WIDTH] = g_q[...]
    gain_own[0][5:6, :HEAD_WIDTH] = g_k[...]

    def gain_start(s):
        device = {"tensor": 1 - core} if s == 0 else {"dp": flipped((s - 1,))}
        return send(gain_own[s], gain_got[s], device)

    gain_copies = [gain_start(0)]
    kv_copies[0].wait_recv()

    def kv_first(j, carry):
        index = natural_index(me, j, (), kv_order)
        kv_cur[0][j] = (kv_in[core, index].astype(F32) + kv_core[index].astype(F32)).astype(BF)
        return carry

    lax.fori_loop(0, 2**n_bits, kv_first, 0)

    def rest_of(g):
        return 2 ** (n_bits - sum(len(x) for x in kv_groups[: g + 1]))

    def block_index(group, bits):
        index = 0
        for k, b in enumerate(group):
            mine = bit_of(me, b)
            index = index + (1 - mine if b in bits else mine) * 2 ** (len(group) - 1 - k)
        return index

    def kv_start(g):
        rest = rest_of(g)
        return [send(kv_cur[g].at[pl.ds(block_index(kv_groups[g], m) * rest, rest)], kv_recv[g].at[c],
                     {"dp": flipped(m)}) for c, m in enumerate(subsets(kv_groups[g]))]

    spot = 0
    for k, b in enumerate(kv_order):
        spot = spot + bit_of(me, b) * 2 ** (n_bits - 1 - k)
    kv_copies = kv_start(0)
    for n in range(n_items):
        if items[n][1]:
            finish(n, 0)
    todo = [(n, s) for s in range(n_bits) for n in range(-1, n_items) if s or n < 0 or not items[n][1]]
    todo = todo + [(-1, n_bits)]
    todo.sort(key=lambda e: e[1] - (1 if e[0] >= 0 and items[e[0]][1] else 0))

    def advance():
        rank = lambda e: e[1] - (1 if e[0] >= 0 and items[e[0]][1] else 0)
        now = rank(todo[0]) if todo else 0
        while todo and rank(todo[0]) == now:
            n, s = todo.pop(0)
            if n >= 0:
                finish(n, s)
                continue
            gain_copies[s].wait_recv()
            if s == n_bits:
                gain_out[...] = gain_own[s][...] + gain_got[s][...]
            else:
                gain_own[s + 1][...] = gain_own[s][...] + gain_got[s][...]
                gain_copies.append(gain_start(s + 1))

    for g in range(len(kv_groups)):
        rest = rest_of(g)
        for copy in kv_copies:
            copy.wait_recv()
        base = block_index(kv_groups[g], ()) * rest

        def kv_total(j, g=g, base=base):
            total = kv_cur[g][base + j].astype(F32)
            for c in range(2 ** len(kv_groups[g]) - 1):
                total = total + kv_recv[g][c, j].astype(F32)
            return total.astype(BF)

        if g < len(kv_groups) - 1:

            def kv_body(j, carry, g=g, kv_total=kv_total):
                kv_cur[g + 1][j] = kv_total(j)
                return carry

            lax.fori_loop(0, rest, kv_body, 0)
            kv_copies = kv_start(g + 1)
        else:
            kv_all[core, spot] = kv_total(0)
        advance()
    for g in reversed(range(len(kv_groups))):
        size = rest_of(g)
        begin = 0
        for k, b in enumerate(sum(kv_groups[: g + 1], ())):
            begin = begin + bit_of(me, b) * 2 ** (n_bits - 1 - k)
        region = kv_all.at[core, pl.ds(begin, size)]
        copies = [send(region, region, {"dp": flipped(m)}) for m in subsets(kv_groups[g])]
        advance()
        for copy in copies:
            copy.wait_recv()
    copy = send(kv_all.at[core], kv_all.at[core], {"tensor": 1 - core})
    while todo:
        advance()
    copy.wait_recv()

    def unpack(j, carry):
        index = natural_index(me, j, (), kv_order)
        k_out[index] = kv_all[0, j].astype(F32)
        v_out[index] = kv_all[1, j].astype(F32)
        return carry

    lax.fori_loop(0, 2**n_bits, unpack, 0)
    for copy in sent:
        copy.wait_send()


def reduce_all(n_dp, items, kv, kv_order, g_block, g_in, g_q, g_k):
    n_bits = len(kv_order)
    groups = tuple(tuple(kv_order[k : k + 2]) for k in range(0, n_bits, 2))
    spec = []
    operands = []
    scratch = []
    outs = []
    copies = 0
    for value, got, order in items:
        n, c, width = value.shape
        given = got is not None
        spec.append((tuple(order), given))
        operands += [value, got] if given else [value]
        outs.append(sds((c, width), F32))
        first = 1 if given else 0
        scratch += [pltpu.VMEM((2 ** (n_bits - s - 1), c, width), BF) for s in range(first, n_bits)]
        scratch += [pltpu.VMEM((2 ** (n_bits - s), c, width), BF) for s in range(1, n_bits)]
        copies += n_bits - 1 + (0 if given else n // 2)
    _, n, c, width = kv.shape
    scratch += [pltpu.VMEM((n, c, width), BF)]
    sizes = [2 ** (n_bits - sum(len(x) for x in groups[:g])) for g in range(len(groups) + 1)]
    scratch += [pltpu.VMEM((2 ** len(groups[g]) - 1, sizes[g + 1], c, width), BF) for g in range(len(groups))]
    scratch += [pltpu.VMEM((sizes[g], c, width), BF) for g in range(len(groups))]
    scratch += [pltpu.VMEM((2, n, c, width), BF)]
    scratch += [pltpu.VMEM((8, width), F32) for _ in range(2 * (n_bits + 1))]
    copies += 2 + 2 * sum(2 ** len(g) - 1 for g in groups) + n_bits + 1
    scratch += [pltpu.SemaphoreType.DMA((copies,)), pltpu.SemaphoreType.DMA((copies,))]
    outs += [sds(kv.shape[1:], F32), sds(kv.shape[1:], F32), sds((8, width), F32)]
    vmem = pl.BlockSpec(memory_space=pltpu.VMEM)
    operands += [kv, g_block, g_in, g_q, g_k]
    return pl.pallas_call(
        functools.partial(reduce_kernel, tuple(spec), groups, n_bits),
        out_shape=outs,
        in_specs=[vmem] * len(operands),
        out_specs=[vmem] * len(outs),
        scratch_shapes=scratch,
        compiler_params=pltpu.CompilerParams(collective_id=0, has_side_effects=True, vmem_limit_bytes=VMEM_LIMIT),
        name="reduce_all",
    )(*operands)


def hop(value, b, n_dp):
    return lax.ppermute(value, "dp", [(i, i ^ 2**b) for i in range(n_dp)])


def after(value, *others):
    return lax.optimization_barrier((value,) + others)[0]


def first_hop(value, b, n_dp):
    n, c, width = value.shape
    away = 1 - bit_of(lax.axis_index("dp"), b)
    view = value.reshape(n // 2 ** (b + 1), 2, 2**b, c, width)
    sent = lax.dynamic_index_in_dim(view, away, 1, keepdims=False).reshape(n // 2, c, width)
    return hop(sent, b, n_dp), sent


def on_device(n_dp, n_tensor, residual_in, cotangent, segment_ids, gain_attn_in, w_query, w_key, w_value,
              gain_query, gain_key, w_out, gain_attn_out, gain_ff_in, w_gate, w_up, w_down, gain_ff_out):
    tokens, depth = residual_in.shape[1:]
    own = tokens // n_tensor
    me = lax.axis_index("tensor")
    first_row = (me * own).astype(jnp.int32).reshape(1)
    seg = segment_ids[0]
    seg_pad = jnp.concatenate([jnp.full((BLOCK,), -1, jnp.int32), seg])
    seg_ext = lax.dynamic_slice_in_dim(seg_pad, me * own, own + BLOCK, 0)[None]
    starts = jnp.sum((seg[None, :] < jnp.arange(LANES, dtype=jnp.int32)[:, None]).astype(F32), axis=1)[None]
    fill = lambda g: jnp.pad(g, (0, depth - g.shape[0]))
    rows8 = jnp.stack([gain_attn_in, gain_attn_out, gain_ff_in, gain_ff_out, fill(gain_query), fill(gain_key),
                       jnp.zeros_like(gain_attn_in), jnp.zeros_like(gain_attn_in)])
    wq_x, wo_x, wg_x, wu_x, wd_x = (swap(w, n_tensor) for w in (w_query, w_out, w_gate, w_up, w_down))
    table = jnp.asarray(rope_table())
    q_o, q_x, ql_o, ql_x, k, v, kl, nb, cos, sin = project(
        first_row, residual_in, seg_ext, starts, table, rows8, w_query, wq_x, w_key, w_value)
    weights = (w_out, wo_x, w_gate, wg_x, w_up, wu_x, w_down, wd_x)
    (output, gmid, ga_o, ga_x, af_o, af_x, lse, delta, mid_b, gff, gas,
     act_o, act_x, gg_o, gg_x, gu_o, gu_x, gains) = block_pass(
        first_row, residual_in, cotangent, seg_ext, q_o, q_x, k, v, weights, rows8)

    n_bits = n_dp.bit_length() - 1
    plain, turned, lead = bit_orders(n_bits)
    chunks = lambda value: value.reshape(n_dp, value.shape[0] // n_dp, value.shape[1])
    spot = lax.axis_index("dp").astype(jnp.int32).reshape(1)

    pairs = [(gff, act_x, act_o, plain), (mid_b, gg_x, gg_o, turned), (mid_b, gu_x, gu_o, lead), (gas, af_x, af_o, plain)]
    grad = lambda left, units: tn(left, units) if left is not mid_b else tn(units, left)
    orders = [order for *_, order in pairs]
    gots = []
    last = ()
    for left, units, _, _ in pairs:
        sent = grad(left, after(units, *last)).astype(BF)
        last = (sent,)
        gots.append(swap(sent, n_tensor))
    state = []
    for (left, _, units, order), got in zip(pairs, gots):
        value = chunks((grad(left, after(units, *last)) + got.astype(F32)).astype(BF))
        arrived, away = first_hop(value, order[0], n_dp)
        last = (away,)
        state.append((value, arrived))

    ga_o = after(ga_o, *last)
    qr_o, qr_x, dk, dv, front, gain_q = attn_back(
        seg_ext, q_o, q_x, k, v, ga_o, ga_x, lse, delta, ql_o, ql_x, cos, sin, rows8)
    front, qr_x, *arrived = lax.optimization_barrier((front, qr_x, *(got for _, got in state)))
    state = [(value, got) for (value, _), got in zip(state, arrived)]
    back = lax.ppermute(front, "tensor", [(t, t - 1) for t in range(1, n_tensor)])
    query_sent = tn(qr_x, nb).astype(BF)
    query_got = swap(query_sent, n_tensor)
    grad_input, kv, gain_in, gain_k = input_back(
        first_row, residual_in, after(gmid, query_sent), dk, dv, back, kl, cos, sin, rows8, qr_o, qr_x,
        w_query, wq_x, w_key, w_value, nb)
    query = chunks((tn(after(qr_o, gain_k), nb) + query_got.astype(F32)).astype(BF))
    kv = kv.reshape(2, n_dp, HEAD_WIDTH // n_dp, depth)
    items = [(value, got, order) for (value, got), order in zip(state, orders)]
    *shares, k_sum, v_sum, gain_sum = reduce_all(
        n_dp, items + [(query, None, plain)], kv, plain, gains, gain_in, gain_q, gain_k)
    s_down, s_gate, s_up, s_out, s_query = shares
    k_sum = k_sum.reshape(HEAD_WIDTH, depth)
    v_sum = v_sum.reshape(HEAD_WIDTH, depth)
    return (
        output[None], grad_input[None], gain_sum[3], s_query.T, k_sum.T, v_sum.T,
        gain_sum[4, :HEAD_WIDTH], gain_sum[5, :HEAD_WIDTH],
        s_out.T, gain_sum[2], gain_sum[1], s_gate.T, s_up.T, s_down.T, gain_sum[0],
    )


def solution(mesh):
    n_dp, n_tensor = mesh.shape["dp"], mesh.shape["tensor"]
    return jax.shard_map(
        functools.partial(on_device, n_dp, n_tensor),
        mesh=mesh,
        in_specs=(
            P("dp", None, None), P("dp", None, None), P("dp", None), P(), P(None, "tensor"), P(), P(), P(), P(),
            P("tensor", None), P(), P(), P(None, "tensor"), P(None, "tensor"), P("tensor", None), P(),
        ),
        out_specs=(
            P("dp", "tensor", None), P("dp", "tensor", None), P(), P(None, ("tensor", "dp")), P(), P(), P(), P(),
            P("tensor", "dp"), P(), P(), P(None, ("tensor", "dp")), P(None, ("tensor", "dp")), P("tensor", "dp"),
            P(),
        ),
        check_vma=False,
    )
```

```python
import functools
import jax
import jax.numpy as jnp
import numpy as np
from jax import lax
from jax.experimental import pallas as pl
from jax.experimental.pallas import tpu as pltpu
from jax.sharding import PartitionSpec as P

HEAD_WIDTH = 256
BLOCK = 512
EPS = 1e-06
THETA = 1000000.0
SCORE_SCALE = 0.0625
GELU_C = 0.7978845608028654
GELU_A = 0.044715
HALF = HEAD_WIDTH // 2
QB = 256
WIN = BLOCK + QB
LANES = 128
BF = jnp.bfloat16
F32 = jnp.float32
VMEM_LIMIT = 60 << 20


def nn(a, b):
    return lax.dot_general(a, b, (((1,), (0,)), ((), ())), preferred_element_type=F32)


def nt(a, b):
    return lax.dot_general(a, b, (((1,), (1,)), ((), ())), preferred_element_type=F32)


def tn(a, b):
    return lax.dot_general(a, b, (((0,), (0,)), ((), ())), preferred_element_type=F32)


def rms_stats(v):
    inv = lax.rsqrt(jnp.mean(v * v, axis=-1, keepdims=True) + EPS)
    return v * inv, inv


def rms_back(hat, inv, gain, up):
    scaled = up * gain
    return inv * (scaled - hat * jnp.mean(scaled * hat, axis=-1, keepdims=True))


def rotate(v, cos, sin, direction):
    a, b = v[:, :HALF], v[:, HALF:]
    if direction > 0:
        return jnp.concatenate([a * cos - b * sin, b * cos + a * sin], axis=-1)
    return jnp.concatenate([a * cos + b * sin, b * cos - a * sin], axis=-1)


def column_of(row):
    n = row.shape[1]
    return jnp.transpose(jnp.broadcast_to(row, (LANES, n)))


def rope_table():
    freq = np.arange(HALF, dtype=np.float32)
    inv_freq = np.exp(freq * np.float32(-2.0 * np.log(THETA) / HEAD_WIDTH)).astype(np.float32)
    angles = np.arange(BLOCK, dtype=np.float32)[:, None] * inv_freq[None, :]
    parts = []
    for tab in (np.cos(angles.astype(np.float64)), np.sin(angles.astype(np.float64))):
        tab = tab.astype(np.float32)
        hi = tab.astype(BF)
        lo = (tab - hi.astype(np.float32)).astype(BF)
        parts += [hi, lo]
    return np.concatenate(parts, axis=1)


def project_kernel(me, x, seg, starts, table, rows8, wq_o, wq_x, wk, wv,
                   q_o, q_x, ql_o, ql_x, k_out, v_out, kl_out, nb_out, cos_out, sin_out):
    g_in, gq, gk = gain_refs(rows8, 0, 4, 5)
    i = pl.program_id(0)
    rows = x.shape[1]
    hat, _ = rms_stats(x[0])
    nb = (hat * g_in[...]).astype(BF)
    nb_out[...] = nb
    seg_col = column_of(seg[...])
    lane = lax.broadcasted_iota(jnp.int32, (rows, LANES), 1)
    start = jnp.sum(jnp.where(seg_col == lane, starts[...], 0.0), axis=1, keepdims=True)
    row = lax.broadcasted_iota(jnp.int32, (rows, 1), 0) + me[0] + (i - 1) * rows
    pos = row - start.astype(jnp.int32)
    hot = (lax.broadcasted_iota(jnp.int32, (rows, BLOCK), 1) == pos).astype(F32).astype(BF)
    cs = nn(hot, table[...])
    cos = cs[:, :LANES] + cs[:, LANES : 2 * LANES]
    sin = cs[:, 2 * LANES : 3 * LANES] + cs[:, 3 * LANES :]
    cos_out[...] = cos
    sin_out[...] = sin
    k_lin = nn(nb, wk[...])
    kl_out[...] = k_lin
    k_hat, _ = rms_stats(k_lin)
    k_out[...] = rotate(k_hat * gk[...], cos, sin, 1).astype(BF)
    v_out[...] = nn(nb, wv[...]).astype(BF)

    @pl.when(i > 0)
    def _():
        for w, lin_out, out in ((wq_o, ql_o, q_o), (wq_x, ql_x, q_x)):
            lin = nn(nb, w[...])
            lin_out[...] = lin
            for h in range(lin.shape[1] // HEAD_WIDTH):
                cols = slice(h * HEAD_WIDTH, (h + 1) * HEAD_WIDTH)
                q_hat, _ = rms_stats(lin[:, cols])
                out[:, cols] = (rotate(q_hat * gq[...], cos, sin, 1) * SCORE_SCALE).astype(BF)


def gain_refs(rows8, *which):
    width = rows8.shape[1]
    return [rows8.at[r : r + 1, : (width if r < 4 else HEAD_WIDTH)] for r in which]


def score_mask(seg_q, seg_k, rows, width):
    lane = lax.broadcasted_iota(jnp.int32, (rows, width), 1)
    sub = lax.broadcasted_iota(jnp.int32, (rows, width), 0)
    return (seg_q == seg_k) & (lane <= sub + (width - rows))


def block_kernel(x, up, seg, q_o, q_x, k, v, wo_o, wo_x, wg_o, wg_x, wu_o, wu_x, wd_o, wd_x,
                 rows8,
                 out, gmid_out, ga_o, ga_x, af_o, af_x, lse_out, delta_out, mid_out, gff_out, gas_out,
                 act_o, act_x, gg_o, gg_x, gu_o, gu_x, gains,
                 mix, gate_s, up_s):
    g_ao, g_fi, g_fo = gain_refs(rows8, 1, 2, 3)
    i = pl.program_id(0)
    rows = x.shape[1]
    base = pl.multiple_of(i * rows, rows)
    k_win = k[pl.ds(base, WIN), :]
    v_win = v[pl.ds(base, WIN), :]
    seg_k = seg[:, pl.ds(base, WIN)]
    seg_q = column_of(seg[:, pl.ds(base + BLOCK, rows)])[:, :1]
    mask = score_mask(seg_q, seg_k, rows, WIN)
    heads_per = q_o.shape[1] // HEAD_WIDTH
    lses = []
    for part, (q, af) in enumerate(((q_o, af_o), (q_x, af_x))):
        for h in range(heads_per):
            cols = slice(h * HEAD_WIDTH, (h + 1) * HEAD_WIDTH)
            s = jnp.where(mask, nt(q[:, cols], k_win), -jnp.inf)
            top = jnp.max(s, axis=-1, keepdims=True)
            e = jnp.exp(s - top)
            mass = jnp.sum(e, axis=-1, keepdims=True)
            lses.append(top + jnp.log(mass))
            p = (e * (1.0 / mass)).astype(BF)
            m = nn(p, v_win)
            mix[part * heads_per + h] = m
            af[:, cols] = m.astype(BF)
    inputs = x[0]
    upstream = up[0]
    attn_sum = nn(af_o[...], wo_o[...]) + nn(af_x[...], wo_x[...])
    hat_attn, inv_attn = rms_stats(attn_sum)
    middle = inputs + hat_attn * g_ao[...]
    hat_mid, inv_mid = rms_stats(middle)
    mid_b = (hat_mid * g_fi[...]).astype(BF)
    mid_out[...] = mid_b
    ff_sum = None
    for part, (wg, wu, wd, act) in enumerate(((wg_o, wu_o, wd_o, act_o), (wg_x, wu_x, wd_x, act_x))):
        gate = nn(mid_b, wg[...])
        upp = nn(mid_b, wu[...])
        sq = gate * gate
        th = jnp.tanh(gate * (GELU_C + (GELU_C * GELU_A) * sq))
        onep = 0.5 + 0.5 * th
        gelu = gate * onep
        deriv = onep + gate * (1.0 - th * th) * (0.5 * GELU_C + (1.5 * GELU_C * GELU_A) * sq)
        gate_s[part] = gelu
        up_s[part] = upp * deriv
        a = (gelu * upp).astype(BF)
        act[...] = a
        f = nn(a, wd[...])
        ff_sum = f if ff_sum is None else ff_sum + f
    hat_ff, inv_ff = rms_stats(ff_sum)
    out[...] = middle + hat_ff * g_fo[...]
    gff = rms_back(hat_ff, inv_ff, g_fo[...], upstream).astype(BF)
    gff_out[...] = gff
    gmn = None
    for part, (wg, wu, wd, gg_out, gu_out) in enumerate(
        ((wg_o, wu_o, wd_o, gg_o, gu_o), (wg_x, wu_x, wd_x, gg_x, gu_x))
    ):
        gact = nt(gff, wd[...])
        gg = (gact * up_s[part]).astype(BF)
        gu = (gact * gate_s[part]).astype(BF)
        gg_out[...] = gg
        gu_out[...] = gu
        t = nt(gg, wg[...]) + nt(gu, wu[...])
        gmn = t if gmn is None else gmn + t
    gmid = upstream + rms_back(hat_mid, inv_mid, g_fi[...], gmn)
    gmid_out[...] = gmid
    gas = rms_back(hat_attn, inv_attn, g_ao[...], gmid).astype(BF)
    gas_out[...] = gas
    deltas = []
    for part, (wo, ga) in enumerate(((wo_o, ga_o), (wo_x, ga_x))):
        g = nt(gas, wo[...]).astype(BF)
        ga[...] = g
        for h in range(heads_per):
            gh = g[:, h * HEAD_WIDTH : (h + 1) * HEAD_WIDTH].astype(F32)
            deltas.append(jnp.sum(gh * mix[part * heads_per + h], axis=-1, keepdims=True))
    lane = lax.broadcasted_iota(jnp.int32, (rows, LANES), 1)
    lse_all = jnp.zeros((rows, LANES), F32)
    delta_all = jnp.zeros((rows, LANES), F32)
    for n, (a, b) in enumerate(zip(lses, deltas)):
        lse_all = jnp.where(lane == n, a, lse_all)
        delta_all = jnp.where(lane == n, b, delta_all)
    lse_out[...] = jnp.transpose(lse_all)[:8]
    delta_out[...] = jnp.transpose(delta_all)[:8]

    @pl.when(i == 0)
    def _():
        gains[...] = jnp.zeros_like(gains)

    gains[0:1, :] += jnp.sum(upstream * hat_ff, axis=0, keepdims=True)
    gains[1:2, :] += jnp.sum(gmn * hat_mid, axis=0, keepdims=True)
    gains[2:3, :] += jnp.sum(gmid * hat_attn, axis=0, keepdims=True)


def attn_back_kernel(seg, q_o, q_x, k, v, ga_o, ga_x, lse, delta, ql_o, ql_x, cos, sin, rows8,
                     qr_o, qr_x, dk_out, dv_out, front, gain, dk, dv):
    (gq,) = gain_refs(rows8, 4)
    i = pl.program_id(0)
    rows = q_o.shape[0]
    base = pl.multiple_of(i * rows, rows)

    @pl.when(i == 0)
    def _():
        dk[...] = jnp.zeros_like(dk)
        dv[...] = jnp.zeros_like(dv)
        gain[...] = jnp.zeros_like(gain)

    k_win = k[pl.ds(base, WIN), :]
    v_win = v[pl.ds(base, WIN), :]
    seg_k = column_of(seg[:, pl.ds(base, WIN)])[:, :1]
    seg_q = seg[:, pl.ds(base + BLOCK, rows)]
    lane = lax.broadcasted_iota(jnp.int32, (WIN, rows), 1)
    sub = lax.broadcasted_iota(jnp.int32, (WIN, rows), 0)
    mask = (seg_q == seg_k) & (sub <= lane + (WIN - rows))
    dk_sum = None
    dv_sum = None
    g_sum = None
    heads = q_o.shape[1] // HEAD_WIDTH
    for n in range(2 * heads):
        q, ga, ql, qraw = ((q_o, ga_o, ql_o, qr_o), (q_x, ga_x, ql_x, qr_x))[n // heads]
        h = n % heads
        cols = slice(h * HEAD_WIDTH, (h + 1) * HEAD_WIDTH)
        qh = q[:, cols]
        gh = ga[:, cols]
        s = jnp.where(mask, nt(k_win, qh), -jnp.inf)
        p = jnp.exp(s - lse[n : n + 1, :])
        ds = (p * (nt(v_win, gh) - delta[n : n + 1, :])).astype(BF)
        dq = tn(ds, k_win) * SCORE_SCALE
        a = nn(ds, qh)
        b = nn(p.astype(BF), gh)
        dk_sum = a if dk_sum is None else dk_sum + a
        dv_sum = b if dv_sum is None else dv_sum + b
        dqn = rotate(dq, cos[...], sin[...], -1)
        hat, inv = rms_stats(ql[:, cols])
        g = jnp.sum(dqn * hat, axis=0, keepdims=True)
        g_sum = g if g_sum is None else g_sum + g
        qraw[:, cols] = rms_back(hat, inv, gq[...], dqn).astype(BF)
    dk[pl.ds(base, WIN), :] += dk_sum
    dv[pl.ds(base, WIN), :] += dv_sum
    gain[...] += g_sum

    @pl.when(i == pl.num_programs(0) - 1)
    def _():
        front[:, :HEAD_WIDTH] = dk[:BLOCK, :].astype(BF)
        front[:, HEAD_WIDTH:] = dv[:BLOCK, :].astype(BF)
        dk_out[...] = dk[BLOCK:, :]
        dv_out[...] = dv[BLOCK:, :]


def whole(shape):
    return pl.BlockSpec(shape, lambda *_: (0,) * len(shape), pipeline_mode=pl.Buffered(1))


def rows_of(n, width, shift=0):
    if shift:
        return pl.BlockSpec((n, width), lambda i, *_: (jnp.maximum(i - shift, 0), 0))
    return pl.BlockSpec((n, width), lambda i, *_: (i, 0))


def params():
    return pltpu.CompilerParams(dimension_semantics=("arbitrary",), vmem_limit_bytes=VMEM_LIMIT)


def cost(us):
    return pl.CostEstimate(flops=us * 10**9, bytes_accessed=us * 10**6, transcendentals=0)


def sds(shape, dtype):
    return jax.ShapeDtypeStruct(shape, dtype)


def project(first_row, x3, seg_ext, starts, table, rows8, wq_o, wq_x, wk, wv):
    depth = x3.shape[2]
    ext = seg_ext.shape[1]
    own = ext - BLOCK
    part = wq_o.shape[1]
    n = BLOCK
    me_block = lambda i, me: (0, jnp.maximum(me[0] // n + i - 1, 0), 0)
    return pl.pallas_call(
        project_kernel,
        grid_spec=pltpu.PrefetchScalarGridSpec(
            num_scalar_prefetch=1,
            grid=(ext // n,),
            in_specs=[
                pl.BlockSpec((1, n, depth), me_block),
                pl.BlockSpec((1, n), lambda i, *_: (0, i)),
                whole((1, LANES)),
                whole(table.shape),
                whole(rows8.shape),
                whole(wq_o.shape), whole(wq_x.shape), whole(wk.shape), whole(wv.shape),
            ],
            out_specs=[
                rows_of(n, part, 1), rows_of(n, part, 1), rows_of(n, part, 1), rows_of(n, part, 1),
                rows_of(n, HEAD_WIDTH), rows_of(n, HEAD_WIDTH), rows_of(n, HEAD_WIDTH, 1),
                rows_of(n, depth, 1), rows_of(n, LANES, 1), rows_of(n, LANES, 1),
            ],
        ),
        out_shape=[
            sds((own, part), BF), sds((own, part), BF), sds((own, part), F32), sds((own, part), F32),
            sds((ext, HEAD_WIDTH), BF), sds((ext, HEAD_WIDTH), BF), sds((own, HEAD_WIDTH), F32),
            sds((own, depth), BF), sds((own, LANES), F32), sds((own, LANES), F32),
        ],
        compiler_params=params(),
        cost_estimate=cost(6),
        name="project",
    )(first_row, x3, seg_ext, starts, table, rows8, wq_o, wq_x, wk, wv)


def block_pass(first_row, x3, up3, seg_ext, q_o, q_x, k, v, weights, rows8):
    depth = x3.shape[2]
    own, part = q_o.shape
    n = QB
    hidden = weights[2].shape[1]
    mine = pl.BlockSpec((1, n, depth), lambda i, me: (0, me[0] // n + i, 0))
    kern = lambda me, *refs: block_kernel(*refs)
    heads = 2 * part // HEAD_WIDTH
    return pl.pallas_call(
        kern,
        grid_spec=pltpu.PrefetchScalarGridSpec(
            num_scalar_prefetch=1,
            grid=(own // n,),
            in_specs=[mine, mine, whole(seg_ext.shape), rows_of(n, part), rows_of(n, part),
                      whole(k.shape), whole(v.shape)]
            + [whole(w.shape) for w in weights]
            + [whole(rows8.shape)],
            out_specs=[rows_of(n, depth)] * 2 + [rows_of(n, part)] * 4 + [pl.BlockSpec((8, n), lambda i, *_: (0, i))] * 2
            + [rows_of(n, depth)] * 3 + [rows_of(n, hidden)] * 6
            + [pl.BlockSpec((8, depth), lambda i, *_: (0, 0))],
            scratch_shapes=[
                pltpu.VMEM((heads, n, HEAD_WIDTH), F32),
                pltpu.VMEM((2, n, hidden), F32),
                pltpu.VMEM((2, n, hidden), F32),
            ],
        ),
        out_shape=[sds((own, depth), F32)] * 2 + [sds((own, part), BF)] * 4 + [sds((8, own), F32)] * 2
        + [sds((own, depth), BF)] * 3 + [sds((own, hidden), BF)] * 6 + [sds((8, depth), F32)],
        compiler_params=params(),
        cost_estimate=cost(40),
        name="block",
    )(first_row, x3, up3, seg_ext, q_o, q_x, k, v, *weights, rows8)


def attn_back(seg_ext, q_o, q_x, k, v, ga_o, ga_x, lse, delta, ql_o, ql_x, cos, sin, rows8):
    own, part = q_o.shape
    n = QB
    ext = k.shape[0]
    fixed = lambda shape: pl.BlockSpec(shape, lambda i: (0, 0))
    stat = pl.BlockSpec((8, n), lambda i: (0, i))
    return pl.pallas_call(
        attn_back_kernel,
        grid=(own // n,),
        in_specs=[whole(seg_ext.shape), rows_of(n, part), rows_of(n, part), whole(k.shape), whole(v.shape),
                  rows_of(n, part), rows_of(n, part), stat, stat, rows_of(n, part), rows_of(n, part),
                  rows_of(n, LANES), rows_of(n, LANES), whole(rows8.shape)],
        out_specs=[rows_of(n, part), rows_of(n, part), fixed((own, HEAD_WIDTH)), fixed((own, HEAD_WIDTH)),
                   fixed((BLOCK, 2 * HEAD_WIDTH)), fixed((1, HEAD_WIDTH))],
        out_shape=[sds((own, part), BF), sds((own, part), BF), sds((own, HEAD_WIDTH), F32),
                   sds((own, HEAD_WIDTH), F32), sds((BLOCK, 2 * HEAD_WIDTH), BF), sds((1, HEAD_WIDTH), F32)],
        scratch_shapes=[pltpu.VMEM((ext, HEAD_WIDTH), F32), pltpu.VMEM((ext, HEAD_WIDTH), F32)],
        compiler_params=params(),
        cost_estimate=cost(20),
        name="attn_back",
    )(seg_ext, q_o, q_x, k, v, ga_o, ga_x, lse, delta, ql_o, ql_x, cos, sin, rows8)


def swap(value, n_tensor):
    return lax.ppermute(value, "tensor", [(t, n_tensor - 1 - t) for t in range(n_tensor)])


def bit_of(index, b):
    return lax.rem(lax.div(index, 2**b), 2)


def bit_orders(n_bits):
    plain = tuple(range(n_bits))
    turned = plain[1:] + plain[:1]
    lead = (plain[2],) + plain[:2] + plain[3:] if n_bits > 2 else plain[::-1]
    return plain, turned, lead


def drop_bit(index, b):
    return lax.div(index, 2 ** (b + 1)) * 2**b + lax.rem(index, 2**b)


def natural_index(me, j, fixed, free):
    index = 0
    for b, flip in fixed:
        mine = bit_of(me, b)
        index = index + (1 - mine if flip else mine) * 2**b
    for k, b in enumerate(free):
        index = index + lax.rem(lax.div(j, 2 ** (len(free) - 1 - k)), 2) * 2**b
    return index


def finish_kernel(items, kv_groups, n_bits, *refs):
    n_items = len(items)
    kv_order = sum(kv_groups, ())
    refs = list(refs)
    take = lambda count: [refs.pop(0) for _ in range(count)]
    ins = [take(2) for _, given in items if given]
    front, rows8, g_block, g_q = take(4)
    far = take(14)
    outs = take(n_items)
    k_out, v_out, gain_out, gin_far = take(4)
    near = take(14)
    local_sems = refs.pop(0)
    front_got, kraw, vraw, kv_in, query_sent, query_got, query, gin, g_in, g_k = take(10)
    ins.append([query])
    recvs, curs = [], []
    for order, given in items:
        first = 1 if given else 0
        recvs.append({s: refs.pop(0) for s in range(first, n_bits)})
        curs.append({s: refs.pop(0) for s in range(1, n_bits)})
    kv_core = refs.pop(0)
    kv_recv = take(len(kv_groups))
    kv_cur = take(len(kv_groups))
    kv_all = refs.pop(0)
    gain_own = take(n_bits + 1)
    gain_got = take(n_bits + 1)
    send_sems, recv_sems = take(2)

    me = lax.axis_index("dp")
    core = lax.axis_index("tensor")

    def flipped(bits):
        return me + sum((1 - 2 * bit_of(me, b)) * 2**b for b in bits)

    def subsets(group):
        return [tuple(b for k, b in enumerate(group) if m >> k & 1) for m in range(1, 2 ** len(group))]

    peers = {(b,) for b in range(n_bits)} | {tuple(sorted(m)) for g in kv_groups for m in subsets(g)}
    barrier = pltpu.get_barrier_semaphore()
    for bits in sorted(peers):
        pl.semaphore_signal(barrier, inc=1, device_id={"dp": flipped(bits)}, device_id_type=pl.DeviceIdType.MESH)
    pl.semaphore_signal(barrier, inc=1, device_id={"tensor": 1 - core}, device_id_type=pl.DeviceIdType.MESH)
    pl.semaphore_wait(barrier, len(peers) + 1)

    sent = []

    def send(src, dst, device):
        k = len(sent)
        copy = pltpu.make_async_remote_copy(
            src_ref=src, dst_ref=dst, send_sem=send_sems.at[k], recv_sem=recv_sems.at[k],
            device_id=device, device_id_type=pl.DeviceIdType.MESH)
        copy.start()
        sent.append(copy)
        return copy

    flying = {}

    def start(n, s):
        order, _ = items[n]
        half = 2 ** (n_bits - s - 1)
        device = {"dp": flipped((order[s],))}
        if s == 0:
            flying[n] = [
                send(ins[n][0].at[natural_index(me, j, ((order[0], True),), order[1:])], recvs[n][0].at[j], device)
                for j in range(half)
            ]
        else:
            away = (1 - bit_of(me, order[s])) * half
            flying[n] = [send(curs[n][s].at[pl.ds(away, half)], recvs[n][s], device)]

    def finish(n, s):
        order, given = items[n]
        half = 2 ** (n_bits - s - 1)
        for copy in flying.pop(n, ()):
            copy.wait_recv()
        outside = given and s == 0
        got = ins[n][1] if outside else recvs[n][s]
        held = curs[n][s] if s else ins[n][0]

        def total_at(j):
            if s:
                index = bit_of(me, order[s]) * half + j
            else:
                index = natural_index(me, j, ((order[0], False),), order[1:])
            return held[index].astype(F32) + got[drop_bit(index, order[0]) if outside else j].astype(F32)

        if s == n_bits - 1:
            outs[n][...] = total_at(0)
            return

        def body(j, carry):
            curs[n][s + 1][j] = total_at(j).astype(BF)
            return carry

        lax.fori_loop(0, half, body, 0)
        start(n, s + 1)

    other_core = {"tensor": 1 - core}
    own, depth = gin.shape
    sources = list(far)
    sources[0] = far[0].at[0, pl.ds(pl.multiple_of(core * own, own), own), :]
    names = ("x", "gmid", "wq_o", "wq_x", "wk", "wv", "dk", "dv", "kl", "cos", "sin", "qr_o", "qr_x", "nb")
    fetch = {name: pltpu.make_async_copy(s, d, local_sems.at[k])
             for k, (name, s, d) in enumerate(zip(names, sources, near))}
    buf = dict(zip(names, near))
    for name in ("nb", "qr_x", "dk", "dv", "kl", "cos", "sin", "qr_o", "wk", "wv", "wq_o", "wq_x", "x", "gmid"):
        fetch[name].start()
    front_copy = send(front, front_got, other_core)
    for n in range(n_items):
        if items[n][1]:
            finish(n, 0)
    fetch["nb"].wait()
    fetch["qr_x"].wait()
    query_sent[...] = tn(buf["qr_x"][...], buf["nb"][...]).astype(BF)
    query_copy = send(query_sent, query_got, other_core)
    for name in ("dk", "dv", "kl", "cos", "sin"):
        fetch[name].wait()
    front_copy.wait_recv()
    gk_row, gin_row = rows8[5:6, :HEAD_WIDTH], rows8[0:1, :]
    g_k[...] = jnp.zeros_like(g_k)
    g_in[...] = jnp.zeros_like(g_in)
    blocks = own // BLOCK

    def kv_rows(i, carry):
        at = pl.ds(pl.multiple_of(i * BLOCK, BLOCK), BLOCK)
        tail = ((i == blocks - 1) & (core == 0)).astype(F32)
        dk = buf["dk"][at, :] + tail * front_got[:, :HEAD_WIDTH].astype(F32)
        dv = buf["dv"][at, :] + tail * front_got[:, HEAD_WIDTH:].astype(F32)
        dkn = rotate(dk, buf["cos"][at, :], buf["sin"][at, :], -1)
        k_hat, k_inv = rms_stats(buf["kl"][at, :])
        kraw[at, :] = rms_back(k_hat, k_inv, gk_row, dkn).astype(BF)
        vraw[at, :] = dv.astype(BF)
        g_k[...] += jnp.sum(dkn * k_hat, axis=0, keepdims=True)
        return carry

    lax.fori_loop(0, blocks, kv_rows, 0)
    n_chunk, rows_k = kv_in.shape[1:3]
    for t, raw in enumerate((kraw, vraw)):
        kv_in[t] = tn(raw[...], buf["nb"][...]).astype(BF).reshape(n_chunk, rows_k, depth)
    kv_copies = [send(kv_in.at[1 - core], kv_core, other_core)]
    fetch["qr_o"].wait()
    query_copy.wait_recv()
    own_query = tn(buf["qr_o"][...], buf["nb"][...]) + query_got[...].astype(F32)
    query[...] = own_query.astype(BF).reshape(query.shape)
    start(n_items - 1, 0)
    def gain_start(s):
        device = {"tensor": 1 - core} if s == 0 else {"dp": flipped((s - 1,))}
        return send(gain_own[s], gain_got[s], device)

    kv_copies[0].wait_recv()

    def kv_first(j, carry):
        index = natural_index(me, j, (), kv_order)
        kv_cur[0][j] = (kv_in[core, index].astype(F32) + kv_core[index].astype(F32)).astype(BF)
        return carry

    lax.fori_loop(0, 2**n_bits, kv_first, 0)

    def rest_of(g):
        return 2 ** (n_bits - sum(len(x) for x in kv_groups[: g + 1]))

    def block_index(group, bits):
        index = 0
        for k, b in enumerate(group):
            mine = bit_of(me, b)
            index = index + (1 - mine if b in bits else mine) * 2 ** (len(group) - 1 - k)
        return index

    def kv_start(g):
        rest = rest_of(g)
        return [send(kv_cur[g].at[pl.ds(block_index(kv_groups[g], m) * rest, rest)], kv_recv[g].at[c],
                     {"dp": flipped(m)}) for c, m in enumerate(subsets(kv_groups[g]))]

    spot = 0
    for k, b in enumerate(kv_order):
        spot = spot + bit_of(me, b) * 2 ** (n_bits - 1 - k)
    kv_copies = kv_start(0)
    for name in ("wk", "wv", "wq_o", "wq_x", "x", "gmid"):
        fetch[name].wait()

    def input_rows(i, carry):
        at = pl.ds(pl.multiple_of(i * QB, QB), QB)
        gn = nt(kraw[at, :], buf["wk"][...]) + nt(vraw[at, :], buf["wv"][...])
        gn = gn + nt(buf["qr_o"][at, :], buf["wq_o"][...]) + nt(buf["qr_x"][at, :], buf["wq_x"][...])
        hat, inv = rms_stats(buf["x"][at, :])
        gin[at, :] = buf["gmid"][at, :] + rms_back(hat, inv, gin_row, gn)
        g_in[...] += jnp.sum(gn * hat, axis=0, keepdims=True)
        return carry

    lax.fori_loop(0, own // QB, input_rows, 0)
    gin_copy = pltpu.make_async_copy(gin, gin_far, local_sems.at[len(names)])
    gin_copy.start()
    gain_own[0][...] = jnp.zeros_like(gain_own[0])
    gain_own[0][0:3, :] = g_block[0:3, :]
    gain_own[0][3:4, :] = g_in[...]
    gain_own[0][4:5, :HEAD_WIDTH] = g_q[...]
    gain_own[0][5:6, :HEAD_WIDTH] = g_k[...]
    gain_copies = [gain_start(0)]
    todo = [(n, s) for s in range(n_bits) for n in range(-1, n_items) if s or n < 0 or not items[n][1]]
    todo = todo + [(-1, n_bits)]
    todo.sort(key=lambda e: e[1] - (1 if e[0] >= 0 and items[e[0]][1] else 0))

    def advance():
        rank = lambda e: e[1] - (1 if e[0] >= 0 and items[e[0]][1] else 0)
        now = rank(todo[0]) if todo else 0
        while todo and rank(todo[0]) == now:
            n, s = todo.pop(0)
            if n >= 0:
                finish(n, s)
                continue
            gain_copies[s].wait_recv()
            if s == n_bits:
                gain_out[...] = gain_own[s][...] + gain_got[s][...]
            else:
                gain_own[s + 1][...] = gain_own[s][...] + gain_got[s][...]
                gain_copies.append(gain_start(s + 1))

    for g in range(len(kv_groups)):
        rest = rest_of(g)
        for copy in kv_copies:
            copy.wait_recv()
        base = block_index(kv_groups[g], ()) * rest

        def kv_total(j, g=g, base=base):
            total = kv_cur[g][base + j].astype(F32)
            for c in range(2 ** len(kv_groups[g]) - 1):
                total = total + kv_recv[g][c, j].astype(F32)
            return total.astype(BF)

        if g < len(kv_groups) - 1:

            def kv_body(j, carry, g=g, kv_total=kv_total):
                kv_cur[g + 1][j] = kv_total(j)
                return carry

            lax.fori_loop(0, rest, kv_body, 0)
            kv_copies = kv_start(g + 1)
        else:
            kv_all[core, spot] = kv_total(0)
        advance()
    for g in reversed(range(len(kv_groups))):
        size = rest_of(g)
        begin = 0
        for k, b in enumerate(sum(kv_groups[: g + 1], ())):
            begin = begin + bit_of(me, b) * 2 ** (n_bits - 1 - k)
        region = kv_all.at[core, pl.ds(begin, size)]
        copies = [send(region, region, {"dp": flipped(m)}) for m in subsets(kv_groups[g])]
        advance()
        for copy in copies:
            copy.wait_recv()
    copy = send(kv_all.at[core], kv_all.at[core], {"tensor": 1 - core})
    while todo:
        advance()
    copy.wait_recv()

    def unpack(j, carry):
        index = natural_index(me, j, (), kv_order)
        k_out[index] = kv_all[0, j].astype(F32)
        v_out[index] = kv_all[1, j].astype(F32)
        return carry

    lax.fori_loop(0, 2**n_bits, unpack, 0)
    gin_copy.wait()
    for copy in sent:
        copy.wait_send()


def finish_all(n_dp, items, order, kv_order, front, rows8, g_block, g_q, far):
    n_bits = len(kv_order)
    own, part = far[11].shape
    depth = far[1].shape[1]
    groups = tuple(tuple(kv_order[k : k + 2]) for k in range(0, n_bits, 2))
    spec, operands, outs, comm = [], [], [], []
    copies = 3
    shapes = [value.shape for value, _, _ in items] + [(n_dp, part // n_dp, depth)]
    for k, (n, c, width) in enumerate(shapes):
        given = k < len(items)
        spec.append((tuple(items[k][2] if given else order), given))
        if given:
            operands += [items[k][0], items[k][1]]
        outs.append(sds((c, width), F32))
        first = 1 if given else 0
        comm += [pltpu.VMEM((2 ** (n_bits - s - 1), c, width), BF) for s in range(first, n_bits)]
        comm += [pltpu.VMEM((2 ** (n_bits - s), c, width), BF) for s in range(1, n_bits)]
        copies += n_bits - 1 + (0 if given else n // 2)
    n, c, width = n_dp, HEAD_WIDTH // n_dp, depth
    comm += [pltpu.VMEM((n, c, width), BF)]
    sizes = [2 ** (n_bits - sum(len(x) for x in groups[:g])) for g in range(len(groups) + 1)]
    comm += [pltpu.VMEM((2 ** len(groups[g]) - 1, sizes[g + 1], c, width), BF) for g in range(len(groups))]
    comm += [pltpu.VMEM((sizes[g], c, width), BF) for g in range(len(groups))]
    comm += [pltpu.VMEM((2, n, c, width), BF)]
    comm += [pltpu.VMEM((8, width), F32) for _ in range(2 * (n_bits + 1))]
    copies += 2 + 2 * sum(2 ** len(g) - 1 for g in groups) + n_bits + 1
    comm += [pltpu.SemaphoreType.DMA((copies,)), pltpu.SemaphoreType.DMA((copies,))]
    outs += [sds((n, c, width), F32), sds((n, c, width), F32), sds((8, width), F32), sds((own, depth), F32)]
    near = [pltpu.VMEM((own, depth), F32)] + [pltpu.VMEM(a.shape, a.dtype) for a in far[1:]]
    scratch = near + [
        pltpu.SemaphoreType.DMA((len(far) + 1,)),
        pltpu.VMEM(front.shape, BF), pltpu.VMEM((own, HEAD_WIDTH), BF), pltpu.VMEM((own, HEAD_WIDTH), BF),
        pltpu.VMEM((2, n, c, width), BF), pltpu.VMEM((part, depth), BF), pltpu.VMEM((part, depth), BF),
        pltpu.VMEM((n_dp, part // n_dp, depth), BF), pltpu.VMEM((own, depth), F32), pltpu.VMEM((1, depth), F32),
        pltpu.VMEM((1, HEAD_WIDTH), F32),
    ] + comm
    vmem = pl.BlockSpec(memory_space=pltpu.VMEM)
    anywhere = pl.BlockSpec(memory_space=pl.ANY)
    operands += [front, rows8, g_block, g_q]
    return pl.pallas_call(
        functools.partial(finish_kernel, tuple(spec), groups, n_bits),
        out_shape=outs,
        in_specs=[vmem] * len(operands) + [anywhere] * len(far),
        out_specs=[vmem] * (len(outs) - 1) + [anywhere],
        scratch_shapes=scratch,
        compiler_params=pltpu.CompilerParams(collective_id=0, has_side_effects=True, vmem_limit_bytes=VMEM_LIMIT),
        name="finish_all",
    )(*operands, *far)


def hop(value, b, n_dp):
    return lax.ppermute(value, "dp", [(i, i ^ 2**b) for i in range(n_dp)])


def after(value, *others):
    return lax.optimization_barrier((value,) + others)[0]


def first_hop(value, b, n_dp):
    n, c, width = value.shape
    away = 1 - bit_of(lax.axis_index("dp"), b)
    view = value.reshape(n // 2 ** (b + 1), 2, 2**b, c, width)
    sent = lax.dynamic_index_in_dim(view, away, 1, keepdims=False).reshape(n // 2, c, width)
    return hop(sent, b, n_dp), sent


def on_device(n_dp, n_tensor, residual_in, cotangent, segment_ids, gain_attn_in, w_query, w_key, w_value,
              gain_query, gain_key, w_out, gain_attn_out, gain_ff_in, w_gate, w_up, w_down, gain_ff_out):
    tokens, depth = residual_in.shape[1:]
    own = tokens // n_tensor
    me = lax.axis_index("tensor")
    first_row = (me * own).astype(jnp.int32).reshape(1)
    seg = segment_ids[0]
    seg_pad = jnp.concatenate([jnp.full((BLOCK,), -1, jnp.int32), seg])
    seg_ext = lax.dynamic_slice_in_dim(seg_pad, me * own, own + BLOCK, 0)[None]
    starts = jnp.sum((seg[None, :] < jnp.arange(LANES, dtype=jnp.int32)[:, None]).astype(F32), axis=1)[None]
    fill = lambda g: jnp.pad(g, (0, depth - g.shape[0]))
    rows8 = jnp.stack([gain_attn_in, gain_attn_out, gain_ff_in, gain_ff_out, fill(gain_query), fill(gain_key),
                       jnp.zeros_like(gain_attn_in), jnp.zeros_like(gain_attn_in)])
    wq_x, wo_x, wg_x, wu_x, wd_x = (swap(w, n_tensor) for w in (w_query, w_out, w_gate, w_up, w_down))
    table = jnp.asarray(rope_table())
    q_o, q_x, ql_o, ql_x, k, v, kl, nb, cos, sin = project(
        first_row, residual_in, seg_ext, starts, table, rows8, w_query, wq_x, w_key, w_value)
    weights = (w_out, wo_x, w_gate, wg_x, w_up, wu_x, w_down, wd_x)
    (output, gmid, ga_o, ga_x, af_o, af_x, lse, delta, mid_b, gff, gas,
     act_o, act_x, gg_o, gg_x, gu_o, gu_x, gains) = block_pass(
        first_row, residual_in, cotangent, seg_ext, q_o, q_x, k, v, weights, rows8)

    n_bits = n_dp.bit_length() - 1
    plain, turned, lead = bit_orders(n_bits)
    chunks = lambda value: value.reshape(n_dp, value.shape[0] // n_dp, value.shape[1])
    spot = lax.axis_index("dp").astype(jnp.int32).reshape(1)

    pairs = [(gff, act_x, act_o, plain), (mid_b, gg_x, gg_o, turned), (mid_b, gu_x, gu_o, lead), (gas, af_x, af_o, plain)]
    grad = lambda left, units: tn(left, units) if left is not mid_b else tn(units, left)
    orders = [order for *_, order in pairs]
    gots = []
    last = ()
    for left, units, _, _ in pairs:
        sent = grad(left, after(units, *last)).astype(BF)
        last = (sent,)
        gots.append(swap(sent, n_tensor))
    state = []
    for (left, _, units, order), got in zip(pairs, gots):
        value = chunks((grad(left, after(units, *last)) + got.astype(F32)).astype(BF))
        arrived, away = first_hop(value, order[0], n_dp)
        last = (away,)
        state.append((value, arrived))

    ga_o = after(ga_o, *last)
    qr_o, qr_x, dk, dv, front, gain_q = attn_back(
        seg_ext, q_o, q_x, k, v, ga_o, ga_x, lse, delta, ql_o, ql_x, cos, sin, rows8)
    front, qr_x, *arrived = lax.optimization_barrier((front, qr_x, *(got for _, got in state)))
    state = [(value, got) for (value, _), got in zip(state, arrived)]
    items = [(value, got, order) for (value, got), order in zip(state, orders)]
    far = (residual_in, gmid, w_query, wq_x, w_key, w_value, dk, dv, kl, cos, sin, qr_o, qr_x, nb)
    *shares, k_sum, v_sum, gain_sum, grad_input = finish_all(
        n_dp, items, plain, plain, front, rows8, gains, gain_q, far)
    s_down, s_gate, s_up, s_out, s_query = shares
    k_sum = k_sum.reshape(HEAD_WIDTH, depth)
    v_sum = v_sum.reshape(HEAD_WIDTH, depth)
    return (
        output[None], grad_input[None], gain_sum[3], s_query.T, k_sum.T, v_sum.T,
        gain_sum[4, :HEAD_WIDTH], gain_sum[5, :HEAD_WIDTH],
        s_out.T, gain_sum[2], gain_sum[1], s_gate.T, s_up.T, s_down.T, gain_sum[0],
    )


def solution(mesh):
    n_dp, n_tensor = mesh.shape["dp"], mesh.shape["tensor"]
    return jax.shard_map(
        functools.partial(on_device, n_dp, n_tensor),
        mesh=mesh,
        in_specs=(
            P("dp", None, None), P("dp", None, None), P("dp", None), P(), P(None, "tensor"), P(), P(), P(), P(),
            P("tensor", None), P(), P(), P(None, "tensor"), P(None, "tensor"), P("tensor", None), P(),
        ),
        out_specs=(
            P("dp", "tensor", None), P("dp", "tensor", None), P(), P(None, ("tensor", "dp")), P(), P(), P(), P(),
            P("tensor", "dp"), P(), P(), P(None, ("tensor", "dp")), P(None, ("tensor", "dp")), P("tensor", "dp"),
            P(),
        ),
        check_vma=False,
    )
```

```python
import functools
import jax
import jax.numpy as jnp
import numpy as np
from jax import lax
from jax.experimental import pallas as pl
from jax.experimental.pallas import tpu as pltpu
from jax.sharding import PartitionSpec as P

HEAD_WIDTH = 256
BLOCK = 512
EPS = 1e-06
THETA = 1000000.0
SCORE_SCALE = 0.0625
GELU_C = 0.7978845608028654
GELU_A = 0.044715
HALF = HEAD_WIDTH // 2
QB = 256
WIN = BLOCK + QB
LANES = 128
BF = jnp.bfloat16
F32 = jnp.float32
VMEM_LIMIT = 60 << 20


def nn(a, b):
    return lax.dot_general(a, b, (((1,), (0,)), ((), ())), preferred_element_type=F32)


def nt(a, b):
    return lax.dot_general(a, b, (((1,), (1,)), ((), ())), preferred_element_type=F32)


def tn(a, b):
    return lax.dot_general(a, b, (((0,), (0,)), ((), ())), preferred_element_type=F32)


def rms_stats(v):
    inv = lax.rsqrt(jnp.mean(v * v, axis=-1, keepdims=True) + EPS)
    return v * inv, inv


def rms_back(hat, inv, gain, up):
    scaled = up * gain
    return inv * (scaled - hat * jnp.mean(scaled * hat, axis=-1, keepdims=True))


def rotate(v, cos, sin, direction):
    a, b = v[:, :HALF], v[:, HALF:]
    if direction > 0:
        return jnp.concatenate([a * cos - b * sin, b * cos + a * sin], axis=-1)
    return jnp.concatenate([a * cos + b * sin, b * cos - a * sin], axis=-1)


def column_of(row):
    n = row.shape[1]
    return jnp.transpose(jnp.broadcast_to(row, (LANES, n)))


def rope_table():
    freq = np.arange(HALF, dtype=np.float32)
    inv_freq = np.exp(freq * np.float32(-2.0 * np.log(THETA) / HEAD_WIDTH)).astype(np.float32)
    angles = np.arange(BLOCK, dtype=np.float32)[:, None] * inv_freq[None, :]
    parts = []
    for tab in (np.cos(angles.astype(np.float64)), np.sin(angles.astype(np.float64))):
        tab = tab.astype(np.float32)
        hi = tab.astype(BF)
        lo = (tab - hi.astype(np.float32)).astype(BF)
        parts += [hi, lo]
    return np.concatenate(parts, axis=1)


def project_kernel(me, x, seg, starts, table, rows8, wq_o, wq_x, wk, wv,
                   q_o, q_x, ql_o, ql_x, k_out, v_out, kl_out, nb_out, cos_out, sin_out):
    g_in, gq, gk = gain_refs(rows8, 0, 4, 5)
    i = pl.program_id(0)
    rows = x.shape[1]
    hat, _ = rms_stats(x[0])
    nb = (hat * g_in[...]).astype(BF)
    nb_out[...] = nb
    seg_col = column_of(seg[...])
    lane = lax.broadcasted_iota(jnp.int32, (rows, LANES), 1)
    start = jnp.sum(jnp.where(seg_col == lane, starts[...], 0.0), axis=1, keepdims=True)
    row = lax.broadcasted_iota(jnp.int32, (rows, 1), 0) + me[0] + (i - 1) * rows
    pos = row - start.astype(jnp.int32)
    hot = (lax.broadcasted_iota(jnp.int32, (rows, BLOCK), 1) == pos).astype(F32).astype(BF)
    cs = nn(hot, table[...])
    cos = cs[:, :LANES] + cs[:, LANES : 2 * LANES]
    sin = cs[:, 2 * LANES : 3 * LANES] + cs[:, 3 * LANES :]
    cos_out[...] = cos
    sin_out[...] = sin
    k_lin = nn(nb, wk[...])
    kl_out[...] = k_lin
    k_hat, _ = rms_stats(k_lin)
    k_out[...] = rotate(k_hat * gk[...], cos, sin, 1).astype(BF)
    v_out[...] = nn(nb, wv[...]).astype(BF)

    @pl.when(i > 0)
    def _():
        for w, lin_out, out in ((wq_o, ql_o, q_o), (wq_x, ql_x, q_x)):
            lin = nn(nb, w[...])
            lin_out[...] = lin
            for h in range(lin.shape[1] // HEAD_WIDTH):
                cols = slice(h * HEAD_WIDTH, (h + 1) * HEAD_WIDTH)
                q_hat, _ = rms_stats(lin[:, cols])
                out[:, cols] = (rotate(q_hat * gq[...], cos, sin, 1) * SCORE_SCALE).astype(BF)


def gain_refs(rows8, *which):
    width = rows8.shape[1]
    return [rows8.at[r : r + 1, : (width if r < 4 else HEAD_WIDTH)] for r in which]


def score_mask(seg_q, seg_k, rows, width):
    lane = lax.broadcasted_iota(jnp.int32, (rows, width), 1)
    sub = lax.broadcasted_iota(jnp.int32, (rows, width), 0)
    return (seg_q == seg_k) & (lane <= sub + (width - rows))


def block_kernel(x, up, seg, q_o, q_x, k, v, wo_o, wo_x, wg_o, wg_x, wu_o, wu_x, wd_o, wd_x,
                 rows8,
                 out, gmid_out, ga_o, ga_x, af_o, af_x, lse_out, delta_out, mid_out, gff_out, gas_out,
                 act_o, act_x, gg_o, gg_x, gu_o, gu_x, gains,
                 mix, gate_s, up_s):
    g_ao, g_fi, g_fo = gain_refs(rows8, 1, 2, 3)
    i = pl.program_id(0)
    rows = x.shape[1]
    base = pl.multiple_of(i * rows, rows)
    k_win = k[pl.ds(base, WIN), :]
    v_win = v[pl.ds(base, WIN), :]
    seg_k = seg[:, pl.ds(base, WIN)]
    seg_q = column_of(seg[:, pl.ds(base + BLOCK, rows)])[:, :1]
    mask = score_mask(seg_q, seg_k, rows, WIN)
    heads_per = q_o.shape[1] // HEAD_WIDTH
    lses = []
    for part, (q, af) in enumerate(((q_o, af_o), (q_x, af_x))):
        for h in range(heads_per):
            cols = slice(h * HEAD_WIDTH, (h + 1) * HEAD_WIDTH)
            s = jnp.where(mask, nt(q[:, cols], k_win), -jnp.inf)
            top = jnp.max(s, axis=-1, keepdims=True)
            e = jnp.exp(s - top)
            mass = jnp.sum(e, axis=-1, keepdims=True)
            lses.append(top + jnp.log(mass))
            p = (e * (1.0 / mass)).astype(BF)
            m = nn(p, v_win)
            mix[part * heads_per + h] = m
            af[:, cols] = m.astype(BF)
    inputs = x[0]
    upstream = up[0]
    attn_sum = nn(af_o[...], wo_o[...]) + nn(af_x[...], wo_x[...])
    hat_attn, inv_attn = rms_stats(attn_sum)
    middle = inputs + hat_attn * g_ao[...]
    hat_mid, inv_mid = rms_stats(middle)
    mid_b = (hat_mid * g_fi[...]).astype(BF)
    mid_out[...] = mid_b
    ff_sum = None
    for part, (wg, wu, wd, act) in enumerate(((wg_o, wu_o, wd_o, act_o), (wg_x, wu_x, wd_x, act_x))):
        gate = nn(mid_b, wg[...])
        upp = nn(mid_b, wu[...])
        sq = gate * gate
        th = jnp.tanh(gate * (GELU_C + (GELU_C * GELU_A) * sq))
        onep = 0.5 + 0.5 * th
        gelu = gate * onep
        deriv = onep + gate * (1.0 - th * th) * (0.5 * GELU_C + (1.5 * GELU_C * GELU_A) * sq)
        gate_s[part] = gelu
        up_s[part] = upp * deriv
        a = (gelu * upp).astype(BF)
        act[...] = a
        f = nn(a, wd[...])
        ff_sum = f if ff_sum is None else ff_sum + f
    hat_ff, inv_ff = rms_stats(ff_sum)
    out[...] = middle + hat_ff * g_fo[...]
    gff = rms_back(hat_ff, inv_ff, g_fo[...], upstream).astype(BF)
    gff_out[...] = gff
    gmn = None
    for part, (wg, wu, wd, gg_out, gu_out) in enumerate(
        ((wg_o, wu_o, wd_o, gg_o, gu_o), (wg_x, wu_x, wd_x, gg_x, gu_x))
    ):
        gact = nt(gff, wd[...])
        gg = (gact * up_s[part]).astype(BF)
        gu = (gact * gate_s[part]).astype(BF)
        gg_out[...] = gg
        gu_out[...] = gu
        t = nt(gg, wg[...]) + nt(gu, wu[...])
        gmn = t if gmn is None else gmn + t
    gmid = upstream + rms_back(hat_mid, inv_mid, g_fi[...], gmn)
    gmid_out[...] = gmid
    gas = rms_back(hat_attn, inv_attn, g_ao[...], gmid).astype(BF)
    gas_out[...] = gas
    deltas = []
    for part, (wo, ga) in enumerate(((wo_o, ga_o), (wo_x, ga_x))):
        g = nt(gas, wo[...]).astype(BF)
        ga[...] = g
        for h in range(heads_per):
            gh = g[:, h * HEAD_WIDTH : (h + 1) * HEAD_WIDTH].astype(F32)
            deltas.append(jnp.sum(gh * mix[part * heads_per + h], axis=-1, keepdims=True))
    lane = lax.broadcasted_iota(jnp.int32, (rows, LANES), 1)
    lse_all = jnp.zeros((rows, LANES), F32)
    delta_all = jnp.zeros((rows, LANES), F32)
    for n, (a, b) in enumerate(zip(lses, deltas)):
        lse_all = jnp.where(lane == n, a, lse_all)
        delta_all = jnp.where(lane == n, b, delta_all)
    lse_out[...] = jnp.transpose(lse_all)[:8]
    delta_out[...] = jnp.transpose(delta_all)[:8]

    @pl.when(i == 0)
    def _():
        gains[...] = jnp.zeros_like(gains)

    gains[0:1, :] += jnp.sum(upstream * hat_ff, axis=0, keepdims=True)
    gains[1:2, :] += jnp.sum(gmn * hat_mid, axis=0, keepdims=True)
    gains[2:3, :] += jnp.sum(gmid * hat_attn, axis=0, keepdims=True)


def attn_rows(i, seg, buf, lse, delta, gq, qr_o, qr_x, dk, dv, gain):
    rows = QB
    base = pl.multiple_of(i * rows, rows)
    mine = pl.ds(base, rows)
    k_win = buf["k"][pl.ds(base, WIN), :]
    v_win = buf["v"][pl.ds(base, WIN), :]
    seg_k = column_of(seg[:, pl.ds(base, WIN)])[:, :1]
    seg_q = seg[:, pl.ds(base + BLOCK, rows)]
    lane = lax.broadcasted_iota(jnp.int32, (WIN, rows), 1)
    sub = lax.broadcasted_iota(jnp.int32, (WIN, rows), 0)
    mask = (seg_q == seg_k) & (sub <= lane + (WIN - rows))
    cos = buf["cos"][mine, :]
    sin = buf["sin"][mine, :]
    dk_sum = None
    dv_sum = None
    g_sum = None
    heads = qr_o.shape[1] // HEAD_WIDTH
    for n in range(2 * heads):
        side = "ox"[n // heads]
        qraw = (qr_o, qr_x)[n // heads]
        h = n % heads
        cols = slice(h * HEAD_WIDTH, (h + 1) * HEAD_WIDTH)
        qh = buf["q_" + side][mine, cols]
        gh = buf["ga_" + side][mine, cols]
        s = jnp.where(mask, nt(k_win, qh), -jnp.inf)
        p = jnp.exp(s - lse[n : n + 1, mine])
        ds = (p * (nt(v_win, gh) - delta[n : n + 1, mine])).astype(BF)
        dq = tn(ds, k_win) * SCORE_SCALE
        a = nn(ds, qh)
        b = nn(p.astype(BF), gh)
        dk_sum = a if dk_sum is None else dk_sum + a
        dv_sum = b if dv_sum is None else dv_sum + b
        dqn = rotate(dq, cos, sin, -1)
        hat, inv = rms_stats(buf["ql_" + side][mine, cols])
        g = jnp.sum(dqn * hat, axis=0, keepdims=True)
        g_sum = g if g_sum is None else g_sum + g
        qraw[mine, cols] = rms_back(hat, inv, gq, dqn).astype(BF)
    dk[pl.ds(base, WIN), :] += dk_sum
    dv[pl.ds(base, WIN), :] += dv_sum
    gain[...] += g_sum


def whole(shape):
    return pl.BlockSpec(shape, lambda *_: (0,) * len(shape), pipeline_mode=pl.Buffered(1))


def rows_of(n, width, shift=0):
    if shift:
        return pl.BlockSpec((n, width), lambda i, *_: (jnp.maximum(i - shift, 0), 0))
    return pl.BlockSpec((n, width), lambda i, *_: (i, 0))


def params():
    return pltpu.CompilerParams(dimension_semantics=("arbitrary",), vmem_limit_bytes=VMEM_LIMIT)


def cost(us):
    return pl.CostEstimate(flops=us * 10**9, bytes_accessed=us * 10**6, transcendentals=0)


def sds(shape, dtype):
    return jax.ShapeDtypeStruct(shape, dtype)


def project(first_row, x3, seg_ext, starts, table, rows8, wq_o, wq_x, wk, wv):
    depth = x3.shape[2]
    ext = seg_ext.shape[1]
    own = ext - BLOCK
    part = wq_o.shape[1]
    n = BLOCK
    me_block = lambda i, me: (0, jnp.maximum(me[0] // n + i - 1, 0), 0)
    return pl.pallas_call(
        project_kernel,
        grid_spec=pltpu.PrefetchScalarGridSpec(
            num_scalar_prefetch=1,
            grid=(ext // n,),
            in_specs=[
                pl.BlockSpec((1, n, depth), me_block),
                pl.BlockSpec((1, n), lambda i, *_: (0, i)),
                whole((1, LANES)),
                whole(table.shape),
                whole(rows8.shape),
                whole(wq_o.shape), whole(wq_x.shape), whole(wk.shape), whole(wv.shape),
            ],
            out_specs=[
                rows_of(n, part, 1), rows_of(n, part, 1), rows_of(n, part, 1), rows_of(n, part, 1),
                rows_of(n, HEAD_WIDTH), rows_of(n, HEAD_WIDTH), rows_of(n, HEAD_WIDTH, 1),
                rows_of(n, depth, 1), rows_of(n, LANES, 1), rows_of(n, LANES, 1),
            ],
        ),
        out_shape=[
            sds((own, part), BF), sds((own, part), BF), sds((own, part), F32), sds((own, part), F32),
            sds((ext, HEAD_WIDTH), BF), sds((ext, HEAD_WIDTH), BF), sds((own, HEAD_WIDTH), F32),
            sds((own, depth), BF), sds((own, LANES), F32), sds((own, LANES), F32),
        ],
        compiler_params=params(),
        cost_estimate=cost(6),
        name="project",
    )(first_row, x3, seg_ext, starts, table, rows8, wq_o, wq_x, wk, wv)


def block_pass(first_row, x3, up3, seg_ext, q_o, q_x, k, v, weights, rows8):
    depth = x3.shape[2]
    own, part = q_o.shape
    n = QB
    hidden = weights[2].shape[1]
    mine = pl.BlockSpec((1, n, depth), lambda i, me: (0, me[0] // n + i, 0))
    kern = lambda me, *refs: block_kernel(*refs)
    heads = 2 * part // HEAD_WIDTH
    return pl.pallas_call(
        kern,
        grid_spec=pltpu.PrefetchScalarGridSpec(
            num_scalar_prefetch=1,
            grid=(own // n,),
            in_specs=[mine, mine, whole(seg_ext.shape), rows_of(n, part), rows_of(n, part),
                      whole(k.shape), whole(v.shape)]
            + [whole(w.shape) for w in weights]
            + [whole(rows8.shape)],
            out_specs=[rows_of(n, depth)] * 2 + [rows_of(n, part)] * 4 + [pl.BlockSpec((8, n), lambda i, *_: (0, i))] * 2
            + [rows_of(n, depth)] * 3 + [rows_of(n, hidden)] * 6
            + [pl.BlockSpec((8, depth), lambda i, *_: (0, 0))],
            scratch_shapes=[
                pltpu.VMEM((heads, n, HEAD_WIDTH), F32),
                pltpu.VMEM((2, n, hidden), F32),
                pltpu.VMEM((2, n, hidden), F32),
            ],
        ),
        out_shape=[sds((own, depth), F32)] * 2 + [sds((own, part), BF)] * 4 + [sds((8, own), F32)] * 2
        + [sds((own, depth), BF)] * 3 + [sds((own, hidden), BF)] * 6 + [sds((8, depth), F32)],
        compiler_params=params(),
        cost_estimate=cost(40),
        name="block",
    )(first_row, x3, up3, seg_ext, q_o, q_x, k, v, *weights, rows8)


def swap(value, n_tensor):
    return lax.ppermute(value, "tensor", [(t, n_tensor - 1 - t) for t in range(n_tensor)])


def bit_of(index, b):
    return lax.rem(lax.div(index, 2**b), 2)


def bit_orders(n_bits):
    plain = tuple(range(n_bits))
    turned = plain[1:] + plain[:1]
    lead = (plain[2],) + plain[:2] + plain[3:] if n_bits > 2 else plain[::-1]
    return plain, turned, lead


def natural_index(me, j, fixed, free):
    index = 0
    for b, flip in fixed:
        mine = bit_of(me, b)
        index = index + (1 - mine if flip else mine) * 2**b
    for k, b in enumerate(free):
        index = index + lax.rem(lax.div(j, 2 ** (len(free) - 1 - k)), 2) * 2**b
    return index


NAMES = ("x", "gmid", "wq_o", "wq_x", "wk", "wv", "kl", "cos", "sin", "nb", "k", "v", "q_o", "q_x", "ga_o", "ga_x",
         "ql_o", "ql_x")


def finish_kernel(items, kv_groups, n_bits, *refs):
    n_items = len(items)
    kv_order = sum(kv_groups, ())
    refs = list(refs)
    take = lambda count: [refs.pop(0) for _ in range(count)]
    ins = [take(1) for _, early in items if early]
    seg, lse, delta, rows8, g_block = take(5)
    far = take(len(NAMES))
    outs = take(n_items)
    k_out, v_out, gain_out, gin_far = take(4)
    near = take(len(NAMES))
    local_sems = refs.pop(0)
    (front, front_got, dk_all, dv_all, qr_o, qr_x, kraw, vraw, kv_in, query_sent, query_got, query,
     g_in, g_k, g_q) = take(15)
    ins.append([query])
    recvs, curs = [], []
    for _ in items:
        recvs.append({s: refs.pop(0) for s in range(n_bits)})
        curs.append({s: refs.pop(0) for s in range(1, n_bits)})
    kv_core = refs.pop(0)
    kv_recv = take(len(kv_groups))
    kv_cur = take(len(kv_groups))
    kv_all = refs.pop(0)
    gain_own = take(n_bits + 1)
    gain_got = take(n_bits + 1)
    send_sems, recv_sems = take(2)

    me = lax.axis_index("dp")
    core = lax.axis_index("tensor")

    def flipped(bits):
        return me + sum((1 - 2 * bit_of(me, b)) * 2**b for b in bits)

    def subsets(group):
        return [tuple(b for k, b in enumerate(group) if m >> k & 1) for m in range(1, 2 ** len(group))]

    peers = {(b,) for b in range(n_bits)} | {tuple(sorted(m)) for g in kv_groups for m in subsets(g)}
    barrier = pltpu.get_barrier_semaphore()
    for bits in sorted(peers):
        pl.semaphore_signal(barrier, inc=1, device_id={"dp": flipped(bits)}, device_id_type=pl.DeviceIdType.MESH)
    pl.semaphore_signal(barrier, inc=1, device_id={"tensor": 1 - core}, device_id_type=pl.DeviceIdType.MESH)
    pl.semaphore_wait(barrier, len(peers) + 1)

    sent = []

    def send(src, dst, device):
        k = len(sent)
        copy = pltpu.make_async_remote_copy(
            src_ref=src, dst_ref=dst, send_sem=send_sems.at[k], recv_sem=recv_sems.at[k],
            device_id=device, device_id_type=pl.DeviceIdType.MESH)
        copy.start()
        sent.append(copy)
        return copy

    flying = {}

    def start(n, s):
        order, _ = items[n]
        half = 2 ** (n_bits - s - 1)
        device = {"dp": flipped((order[s],))}
        if s == 0:
            flying[n] = [
                send(ins[n][0].at[natural_index(me, j, ((order[0], True),), order[1:])], recvs[n][0].at[j], device)
                for j in range(half)
            ]
        else:
            away = (1 - bit_of(me, order[s])) * half
            flying[n] = [send(curs[n][s].at[pl.ds(away, half)], recvs[n][s], device)]

    def finish(n, s):
        order, _ = items[n]
        half = 2 ** (n_bits - s - 1)
        for copy in flying.pop(n):
            copy.wait_recv()
        got = recvs[n][s]
        held = curs[n][s] if s else ins[n][0]

        def total_at(j):
            if s:
                index = bit_of(me, order[s]) * half + j
            else:
                index = natural_index(me, j, ((order[0], False),), order[1:])
            return held[index].astype(F32) + got[j].astype(F32)

        if s == n_bits - 1:
            outs[n][...] = total_at(0)
            return

        def body(j, carry):
            curs[n][s + 1][j] = total_at(j).astype(BF)
            return carry

        lax.fori_loop(0, half, body, 0)
        start(n, s + 1)

    other_core = {"tensor": 1 - core}
    own, depth = near[0].shape
    sources = list(far)
    sources[0] = far[0].at[0, pl.ds(pl.multiple_of(core * own, own), own), :]
    buf = dict(zip(NAMES, near))
    fetch = {name: pltpu.make_async_copy(s, d, local_sems.at[k])
             for k, (name, s, d) in enumerate(zip(NAMES, sources, near))}
    first_use = ("k", "v", "q_o", "ga_o", "cos", "sin", "ql_o", "q_x", "ga_x", "ql_x")
    second_use = ("nb", "kl", "wk", "wv", "wq_o", "wq_x", "x", "gmid")
    for name in first_use:
        fetch[name].start()
    for n in range(n_items):
        if items[n][1]:
            start(n, 0)
    for name in second_use:
        fetch[name].start()
    dk_all[...] = jnp.zeros_like(dk_all)
    dv_all[...] = jnp.zeros_like(dv_all)
    g_q[...] = jnp.zeros_like(g_q)
    gq_row = rows8[4:5, :HEAD_WIDTH]
    for name in first_use:
        fetch[name].wait()

    def attn_body(i, carry):
        attn_rows(i, seg, buf, lse, delta, gq_row, qr_o, qr_x, dk_all, dv_all, g_q)
        return carry

    lax.fori_loop(0, own // QB, attn_body, 0)
    front[:, :HEAD_WIDTH] = dk_all[:BLOCK, :].astype(BF)
    front[:, HEAD_WIDTH:] = dv_all[:BLOCK, :].astype(BF)
    front_copy = send(front, front_got, other_core)
    fetch["nb"].wait()
    query_sent[...] = tn(qr_x[...], buf["nb"][...]).astype(BF)
    query_copy = send(query_sent, query_got, other_core)
    for n in range(n_items):
        if items[n][1]:
            finish(n, 0)
    fetch["kl"].wait()
    front_copy.wait_recv()
    gk_row, gin_row = rows8[5:6, :HEAD_WIDTH], rows8[0:1, :]
    g_k[...] = jnp.zeros_like(g_k)
    g_in[...] = jnp.zeros_like(g_in)
    blocks = own // BLOCK

    def kv_rows(i, carry):
        at = pl.ds(pl.multiple_of(i * BLOCK, BLOCK), BLOCK)
        tail = ((i == blocks - 1) & (core == 0)).astype(F32)
        later = pl.ds(pl.multiple_of((i + 1) * BLOCK, BLOCK), BLOCK)
        dk = dk_all[later, :] + tail * front_got[:, :HEAD_WIDTH].astype(F32)
        dv = dv_all[later, :] + tail * front_got[:, HEAD_WIDTH:].astype(F32)
        dkn = rotate(dk, buf["cos"][at, :], buf["sin"][at, :], -1)
        k_hat, k_inv = rms_stats(buf["kl"][at, :])
        kraw[at, :] = rms_back(k_hat, k_inv, gk_row, dkn).astype(BF)
        vraw[at, :] = dv.astype(BF)
        g_k[...] += jnp.sum(dkn * k_hat, axis=0, keepdims=True)
        return carry

    lax.fori_loop(0, blocks, kv_rows, 0)
    n_chunk, rows_k = kv_in.shape[1:3]
    for t, raw in enumerate((kraw, vraw)):
        kv_in[t] = tn(raw[...], buf["nb"][...]).astype(BF).reshape(n_chunk, rows_k, depth)
    kv_copies = [send(kv_in.at[1 - core], kv_core, other_core)]
    query_copy.wait_recv()
    own_query = tn(qr_o[...], buf["nb"][...]) + query_got[...].astype(F32)
    query[...] = own_query.astype(BF).reshape(query.shape)
    start(n_items - 1, 0)
    def gain_start(s):
        device = {"tensor": 1 - core} if s == 0 else {"dp": flipped((s - 1,))}
        return send(gain_own[s], gain_got[s], device)

    kv_copies[0].wait_recv()

    def kv_first(j, carry):
        index = natural_index(me, j, (), kv_order)
        kv_cur[0][j] = (kv_in[core, index].astype(F32) + kv_core[index].astype(F32)).astype(BF)
        return carry

    lax.fori_loop(0, 2**n_bits, kv_first, 0)

    def rest_of(g):
        return 2 ** (n_bits - sum(len(x) for x in kv_groups[: g + 1]))

    def block_index(group, bits):
        index = 0
        for k, b in enumerate(group):
            mine = bit_of(me, b)
            index = index + (1 - mine if b in bits else mine) * 2 ** (len(group) - 1 - k)
        return index

    def kv_start(g):
        rest = rest_of(g)
        return [send(kv_cur[g].at[pl.ds(block_index(kv_groups[g], m) * rest, rest)], kv_recv[g].at[c],
                     {"dp": flipped(m)}) for c, m in enumerate(subsets(kv_groups[g]))]

    spot = 0
    for k, b in enumerate(kv_order):
        spot = spot + bit_of(me, b) * 2 ** (n_bits - 1 - k)
    kv_copies = kv_start(0)
    for name in ("wk", "wv", "wq_o", "wq_x", "x", "gmid"):
        fetch[name].wait()

    def input_rows(i, carry):
        at = pl.ds(pl.multiple_of(i * QB, QB), QB)
        gn = nt(kraw[at, :], buf["wk"][...]) + nt(vraw[at, :], buf["wv"][...])
        gn = gn + nt(qr_o[at, :], buf["wq_o"][...]) + nt(qr_x[at, :], buf["wq_x"][...])
        hat, inv = rms_stats(buf["x"][at, :])
        buf["x"][at, :] = buf["gmid"][at, :] + rms_back(hat, inv, gin_row, gn)
        g_in[...] += jnp.sum(gn * hat, axis=0, keepdims=True)
        return carry

    lax.fori_loop(0, own // QB, input_rows, 0)
    gin_copy = pltpu.make_async_copy(buf["x"], gin_far, local_sems.at[len(NAMES)])
    gin_copy.start()
    gain_own[0][...] = jnp.zeros_like(gain_own[0])
    gain_own[0][0:3, :] = g_block[0:3, :]
    gain_own[0][3:4, :] = g_in[...]
    gain_own[0][4:5, :HEAD_WIDTH] = g_q[...]
    gain_own[0][5:6, :HEAD_WIDTH] = g_k[...]
    gain_copies = [gain_start(0)]
    todo = [(n, s) for s in range(n_bits) for n in range(-1, n_items) if s or n < 0 or not items[n][1]]
    todo = todo + [(-1, n_bits)]
    todo.sort(key=lambda e: e[1] - (1 if e[0] >= 0 and items[e[0]][1] else 0))

    def advance():
        rank = lambda e: e[1] - (1 if e[0] >= 0 and items[e[0]][1] else 0)
        now = rank(todo[0]) if todo else 0
        while todo and rank(todo[0]) == now:
            n, s = todo.pop(0)
            if n >= 0:
                finish(n, s)
                continue
            gain_copies[s].wait_recv()
            if s == n_bits:
                gain_out[...] = gain_own[s][...] + gain_got[s][...]
            else:
                gain_own[s + 1][...] = gain_own[s][...] + gain_got[s][...]
                gain_copies.append(gain_start(s + 1))

    for g in range(len(kv_groups)):
        rest = rest_of(g)
        for copy in kv_copies:
            copy.wait_recv()
        base = block_index(kv_groups[g], ()) * rest

        def kv_total(j, g=g, base=base):
            total = kv_cur[g][base + j].astype(F32)
            for c in range(2 ** len(kv_groups[g]) - 1):
                total = total + kv_recv[g][c, j].astype(F32)
            return total.astype(BF)

        if g < len(kv_groups) - 1:

            def kv_body(j, carry, g=g, kv_total=kv_total):
                kv_cur[g + 1][j] = kv_total(j)
                return carry

            lax.fori_loop(0, rest, kv_body, 0)
            kv_copies = kv_start(g + 1)
        else:
            kv_all[core, spot] = kv_total(0)
        advance()
    for g in reversed(range(len(kv_groups))):
        size = rest_of(g)
        begin = 0
        for k, b in enumerate(sum(kv_groups[: g + 1], ())):
            begin = begin + bit_of(me, b) * 2 ** (n_bits - 1 - k)
        region = kv_all.at[core, pl.ds(begin, size)]
        copies = [send(region, region, {"dp": flipped(m)}) for m in subsets(kv_groups[g])]
        advance()
        for copy in copies:
            copy.wait_recv()
    copy = send(kv_all.at[core], kv_all.at[core], {"tensor": 1 - core})
    while todo:
        advance()
    copy.wait_recv()

    def unpack(j, carry):
        index = natural_index(me, j, (), kv_order)
        k_out[index] = kv_all[0, j].astype(F32)
        v_out[index] = kv_all[1, j].astype(F32)
        return carry

    lax.fori_loop(0, 2**n_bits, unpack, 0)
    gin_copy.wait()
    for copy in sent:
        copy.wait_send()


def finish_all(n_dp, items, order, kv_order, small, far):
    n_bits = len(kv_order)
    own, part = far[12].shape
    ext = far[10].shape[0]
    depth = far[1].shape[1]
    groups = tuple(tuple(kv_order[k : k + 2]) for k in range(0, n_bits, 2))
    spec, operands, outs, comm = [], [], [], []
    copies = 3
    shapes = [value.shape for value, _ in items] + [(n_dp, part // n_dp, depth)]
    for k, (n, c, width) in enumerate(shapes):
        early = k < len(items)
        spec.append((tuple(items[k][1] if early else order), early))
        if early:
            operands.append(items[k][0])
        outs.append(sds((c, width), F32))
        comm += [pltpu.VMEM((2 ** (n_bits - s - 1), c, width), BF) for s in range(n_bits)]
        comm += [pltpu.VMEM((2 ** (n_bits - s), c, width), BF) for s in range(1, n_bits)]
        copies += n_bits - 1 + n // 2
    n, c, width = n_dp, HEAD_WIDTH // n_dp, depth
    comm += [pltpu.VMEM((n, c, width), BF)]
    sizes = [2 ** (n_bits - sum(len(x) for x in groups[:g])) for g in range(len(groups) + 1)]
    comm += [pltpu.VMEM((2 ** len(groups[g]) - 1, sizes[g + 1], c, width), BF) for g in range(len(groups))]
    comm += [pltpu.VMEM((sizes[g], c, width), BF) for g in range(len(groups))]
    comm += [pltpu.VMEM((2, n, c, width), BF)]
    comm += [pltpu.VMEM((8, width), F32) for _ in range(2 * (n_bits + 1))]
    copies += 2 + 2 * sum(2 ** len(g) - 1 for g in groups) + n_bits + 1
    comm += [pltpu.SemaphoreType.DMA((copies,)), pltpu.SemaphoreType.DMA((copies,))]
    outs += [sds((n, c, width), F32), sds((n, c, width), F32), sds((8, width), F32), sds((own, depth), F32)]
    near = [pltpu.VMEM((own, depth), F32)] + [pltpu.VMEM(a.shape, a.dtype) for a in far[1:]]
    scratch = near + [
        pltpu.SemaphoreType.DMA((len(far) + 1,)),
        pltpu.VMEM((BLOCK, 2 * HEAD_WIDTH), BF), pltpu.VMEM((BLOCK, 2 * HEAD_WIDTH), BF),
        pltpu.VMEM((ext, HEAD_WIDTH), F32), pltpu.VMEM((ext, HEAD_WIDTH), F32),
        pltpu.VMEM((own, part), BF), pltpu.VMEM((own, part), BF),
        pltpu.VMEM((own, HEAD_WIDTH), BF), pltpu.VMEM((own, HEAD_WIDTH), BF),
        pltpu.VMEM((2, n, c, width), BF), pltpu.VMEM((part, depth), BF), pltpu.VMEM((part, depth), BF),
        pltpu.VMEM((n_dp, part // n_dp, depth), BF), pltpu.VMEM((1, depth), F32),
        pltpu.VMEM((1, HEAD_WIDTH), F32), pltpu.VMEM((1, HEAD_WIDTH), F32),
    ] + comm
    vmem = pl.BlockSpec(memory_space=pltpu.VMEM)
    anywhere = pl.BlockSpec(memory_space=pl.ANY)
    operands += list(small)
    return pl.pallas_call(
        functools.partial(finish_kernel, tuple(spec), groups, n_bits),
        out_shape=outs,
        in_specs=[vmem] * len(operands) + [anywhere] * len(far),
        out_specs=[vmem] * (len(outs) - 1) + [anywhere],
        scratch_shapes=scratch,
        compiler_params=pltpu.CompilerParams(collective_id=0, has_side_effects=True, vmem_limit_bytes=VMEM_LIMIT),
        name="finish_all",
    )(*operands, *far)


def after(value, *others):
    return lax.optimization_barrier((value,) + others)[0]


def on_device(n_dp, n_tensor, residual_in, cotangent, segment_ids, gain_attn_in, w_query, w_key, w_value,
              gain_query, gain_key, w_out, gain_attn_out, gain_ff_in, w_gate, w_up, w_down, gain_ff_out):
    tokens, depth = residual_in.shape[1:]
    own = tokens // n_tensor
    me = lax.axis_index("tensor")
    first_row = (me * own).astype(jnp.int32).reshape(1)
    seg = segment_ids[0]
    seg_pad = jnp.concatenate([jnp.full((BLOCK,), -1, jnp.int32), seg])
    seg_ext = lax.dynamic_slice_in_dim(seg_pad, me * own, own + BLOCK, 0)[None]
    starts = jnp.sum((seg[None, :] < jnp.arange(LANES, dtype=jnp.int32)[:, None]).astype(F32), axis=1)[None]
    fill = lambda g: jnp.pad(g, (0, depth - g.shape[0]))
    rows8 = jnp.stack([gain_attn_in, gain_attn_out, gain_ff_in, gain_ff_out, fill(gain_query), fill(gain_key),
                       jnp.zeros_like(gain_attn_in), jnp.zeros_like(gain_attn_in)])
    wq_x, wo_x, wg_x, wu_x, wd_x = (swap(w, n_tensor) for w in (w_query, w_out, w_gate, w_up, w_down))
    table = jnp.asarray(rope_table())
    q_o, q_x, ql_o, ql_x, k, v, kl, nb, cos, sin = project(
        first_row, residual_in, seg_ext, starts, table, rows8, w_query, wq_x, w_key, w_value)
    weights = (w_out, wo_x, w_gate, wg_x, w_up, wu_x, w_down, wd_x)
    (output, gmid, ga_o, ga_x, af_o, af_x, lse, delta, mid_b, gff, gas,
     act_o, act_x, gg_o, gg_x, gu_o, gu_x, gains) = block_pass(
        first_row, residual_in, cotangent, seg_ext, q_o, q_x, k, v, weights, rows8)

    n_bits = n_dp.bit_length() - 1
    plain, turned, lead = bit_orders(n_bits)
    chunks = lambda value: value.reshape(n_dp, value.shape[0] // n_dp, value.shape[1])

    pairs = [(gff, act_x, act_o, plain), (mid_b, gg_x, gg_o, turned), (mid_b, gu_x, gu_o, lead), (gas, af_x, af_o, plain)]
    grad = lambda left, units: tn(left, units) if left is not mid_b else tn(units, left)
    gots = []
    last = ()
    for left, units, _, _ in pairs:
        sent = grad(left, after(units, *last)).astype(BF)
        last = (sent,)
        gots.append(swap(sent, n_tensor))
    items = []
    for (left, _, units, order), got in zip(pairs, gots):
        items.append((chunks((grad(left, after(units, *last)) + got.astype(F32)).astype(BF)), order))
    far = (residual_in, gmid, w_query, wq_x, w_key, w_value, kl, cos, sin, nb, k, v, q_o, q_x, ga_o, ga_x, ql_o, ql_x)
    *shares, k_sum, v_sum, gain_sum, grad_input = finish_all(
        n_dp, items, plain, plain, (seg_ext, lse, delta, rows8, gains), far)
    s_down, s_gate, s_up, s_out, s_query = shares
    k_sum = k_sum.reshape(HEAD_WIDTH, depth)
    v_sum = v_sum.reshape(HEAD_WIDTH, depth)
    return (
        output[None], grad_input[None], gain_sum[3], s_query.T, k_sum.T, v_sum.T,
        gain_sum[4, :HEAD_WIDTH], gain_sum[5, :HEAD_WIDTH],
        s_out.T, gain_sum[2], gain_sum[1], s_gate.T, s_up.T, s_down.T, gain_sum[0],
    )


def solution(mesh):
    n_dp, n_tensor = mesh.shape["dp"], mesh.shape["tensor"]
    return jax.shard_map(
        functools.partial(on_device, n_dp, n_tensor),
        mesh=mesh,
        in_specs=(
            P("dp", None, None), P("dp", None, None), P("dp", None), P(), P(None, "tensor"), P(), P(), P(), P(),
            P("tensor", None), P(), P(), P(None, "tensor"), P(None, "tensor"), P("tensor", None), P(),
        ),
        out_specs=(
            P("dp", "tensor", None), P("dp", "tensor", None), P(), P(None, ("tensor", "dp")), P(), P(), P(), P(),
            P("tensor", "dp"), P(), P(), P(None, ("tensor", "dp")), P(None, ("tensor", "dp")), P("tensor", "dp"),
            P(),
        ),
        check_vma=False,
    )
```

```python
import functools
import jax
import jax.numpy as jnp
import numpy as np
from jax import lax
from jax.experimental import pallas as pl
from jax.experimental.pallas import tpu as pltpu
from jax.sharding import PartitionSpec as P

HEAD_WIDTH = 256
BLOCK = 512
EPS = 1e-06
THETA = 1000000.0
SCORE_SCALE = 0.0625
GELU_C = 0.7978845608028654
GELU_A = 0.044715
HALF = HEAD_WIDTH // 2
QB = 256
WIN = BLOCK + QB
LANES = 128
BF = jnp.bfloat16
F32 = jnp.float32
VMEM_LIMIT = 60 << 20


def nn(a, b):
    return lax.dot_general(a, b, (((1,), (0,)), ((), ())), preferred_element_type=F32)


def nt(a, b):
    return lax.dot_general(a, b, (((1,), (1,)), ((), ())), preferred_element_type=F32)


def tn(a, b):
    return lax.dot_general(a, b, (((0,), (0,)), ((), ())), preferred_element_type=F32)


def rms_stats(v):
    inv = lax.rsqrt(jnp.mean(v * v, axis=-1, keepdims=True) + EPS)
    return v * inv, inv


def rms_back(hat, inv, gain, up):
    scaled = up * gain
    return inv * (scaled - hat * jnp.mean(scaled * hat, axis=-1, keepdims=True))


def rotate(v, cos, sin, direction):
    a, b = v[:, :HALF], v[:, HALF:]
    if direction > 0:
        return jnp.concatenate([a * cos - b * sin, b * cos + a * sin], axis=-1)
    return jnp.concatenate([a * cos + b * sin, b * cos - a * sin], axis=-1)


def column_of(row):
    n = row.shape[1]
    return jnp.transpose(jnp.broadcast_to(row, (LANES, n)))


def rope_table():
    freq = np.arange(HALF, dtype=np.float32)
    inv_freq = np.exp(freq * np.float32(-2.0 * np.log(THETA) / HEAD_WIDTH)).astype(np.float32)
    angles = np.arange(BLOCK, dtype=np.float32)[:, None] * inv_freq[None, :]
    parts = []
    for tab in (np.cos(angles.astype(np.float64)), np.sin(angles.astype(np.float64))):
        tab = tab.astype(np.float32)
        hi = tab.astype(BF)
        lo = (tab - hi.astype(np.float32)).astype(BF)
        parts += [hi, lo]
    return np.concatenate(parts, axis=1)


def project_kernel(me, x, seg, table, g1, g2, g3, g4, g5, g6, wq_o, wq_x, wk, wv,
                   q_o, q_x, ql_o, ql_x, k_out, v_out, kl_out, nb_out, cos_out, sin_out, seg_out, rows8):
    i = pl.program_id(0)
    rows = x.shape[1]

    @pl.when(i == 0)
    def _():
        rows8[...] = jnp.zeros_like(rows8)
        for r, g in enumerate((g1, g2, g3, g4, g5, g6)):
            rows8[r : r + 1, : g.shape[0]] = g[...].reshape(1, g.shape[0])

    g_in, gq, gk = gain_refs(rows8, 0, 4, 5)
    hat, _ = rms_stats(x[0])
    nb = (hat * g_in[...]).astype(BF)
    nb_out[...] = nb
    base = me[0] + (i - 1) * rows
    seg_row = seg[:, pl.ds(pl.multiple_of(jnp.maximum(base, 0), rows), rows)]
    seg_row = jnp.where(base < 0, -1, seg_row)
    seg_out[...] = seg_row
    before = (seg[...] < column_of(seg_row)[:, :1]).astype(F32)
    start = jnp.sum(before, axis=1, keepdims=True)
    pos = lax.broadcasted_iota(jnp.int32, (rows, 1), 0) + base - start.astype(jnp.int32)
    hot = (lax.broadcasted_iota(jnp.int32, (rows, BLOCK), 1) == pos).astype(F32).astype(BF)
    cs = nn(hot, table[...])
    cos = cs[:, :LANES] + cs[:, LANES : 2 * LANES]
    sin = cs[:, 2 * LANES : 3 * LANES] + cs[:, 3 * LANES :]
    cos_out[...] = cos
    sin_out[...] = sin
    k_lin = nn(nb, wk[...])
    kl_out[...] = k_lin
    k_hat, _ = rms_stats(k_lin)
    k_out[...] = rotate(k_hat * gk[...], cos, sin, 1).astype(BF)
    v_out[...] = nn(nb, wv[...]).astype(BF)

    @pl.when(i > 0)
    def _():
        for w, lin_out, out in ((wq_o, ql_o, q_o), (wq_x, ql_x, q_x)):
            lin = nn(nb, w[...])
            lin_out[...] = lin
            for h in range(lin.shape[1] // HEAD_WIDTH):
                cols = slice(h * HEAD_WIDTH, (h + 1) * HEAD_WIDTH)
                q_hat, _ = rms_stats(lin[:, cols])
                out[:, cols] = (rotate(q_hat * gq[...], cos, sin, 1) * SCORE_SCALE).astype(BF)


def gain_refs(rows8, *which):
    width = rows8.shape[1]
    return [rows8.at[r : r + 1, : (width if r < 4 else HEAD_WIDTH)] for r in which]


def score_mask(seg_q, seg_k, rows, width):
    lane = lax.broadcasted_iota(jnp.int32, (rows, width), 1)
    sub = lax.broadcasted_iota(jnp.int32, (rows, width), 0)
    return (seg_q == seg_k) & (lane <= sub + (width - rows))


def block_kernel(x, up, seg, q_o, q_x, k, v, wo_o, wo_x, wg_o, wg_x, wu_o, wu_x, wd_o, wd_x,
                 rows8,
                 out, gmid_out, ga_o, ga_x, af_o, af_x, lse_out, delta_out, mid_out, gff_out, gas_out,
                 act_o, act_x, gg_o, gg_x, gu_o, gu_x, gains,
                 mix, gate_s, up_s):
    g_ao, g_fi, g_fo = gain_refs(rows8, 1, 2, 3)
    i = pl.program_id(0)
    rows = x.shape[1]
    base = pl.multiple_of(i * rows, rows)
    k_win = k[pl.ds(base, WIN), :]
    v_win = v[pl.ds(base, WIN), :]
    seg_k = seg[:, pl.ds(base, WIN)]
    seg_q = column_of(seg[:, pl.ds(base + BLOCK, rows)])[:, :1]
    mask = score_mask(seg_q, seg_k, rows, WIN)
    heads_per = q_o.shape[1] // HEAD_WIDTH
    lses = []
    for part, (q, af) in enumerate(((q_o, af_o), (q_x, af_x))):
        for h in range(heads_per):
            cols = slice(h * HEAD_WIDTH, (h + 1) * HEAD_WIDTH)
            s = jnp.where(mask, nt(q[:, cols], k_win), -jnp.inf)
            top = jnp.max(s, axis=-1, keepdims=True)
            e = jnp.exp(s - top)
            mass = jnp.sum(e, axis=-1, keepdims=True)
            lses.append(top + jnp.log(mass))
            p = (e * (1.0 / mass)).astype(BF)
            m = nn(p, v_win)
            mix[part * heads_per + h] = m
            af[:, cols] = m.astype(BF)
    inputs = x[0]
    upstream = up[0]
    attn_sum = nn(af_o[...], wo_o[...]) + nn(af_x[...], wo_x[...])
    hat_attn, inv_attn = rms_stats(attn_sum)
    middle = inputs + hat_attn * g_ao[...]
    hat_mid, inv_mid = rms_stats(middle)
    mid_b = (hat_mid * g_fi[...]).astype(BF)
    mid_out[...] = mid_b
    ff_sum = None
    for part, (wg, wu, wd, act) in enumerate(((wg_o, wu_o, wd_o, act_o), (wg_x, wu_x, wd_x, act_x))):
        gate = nn(mid_b, wg[...])
        upp = nn(mid_b, wu[...])
        sq = gate * gate
        th = jnp.tanh(gate * (GELU_C + (GELU_C * GELU_A) * sq))
        onep = 0.5 + 0.5 * th
        gelu = gate * onep
        deriv = onep + gate * (1.0 - th * th) * (0.5 * GELU_C + (1.5 * GELU_C * GELU_A) * sq)
        gate_s[part] = gelu
        up_s[part] = upp * deriv
        a = (gelu * upp).astype(BF)
        act[...] = a
        f = nn(a, wd[...])
        ff_sum = f if ff_sum is None else ff_sum + f
    hat_ff, inv_ff = rms_stats(ff_sum)
    out[...] = middle + hat_ff * g_fo[...]
    gff = rms_back(hat_ff, inv_ff, g_fo[...], upstream).astype(BF)
    gff_out[...] = gff
    gmn = None
    for part, (wg, wu, wd, gg_out, gu_out) in enumerate(
        ((wg_o, wu_o, wd_o, gg_o, gu_o), (wg_x, wu_x, wd_x, gg_x, gu_x))
    ):
        gact = nt(gff, wd[...])
        gg = (gact * up_s[part]).astype(BF)
        gu = (gact * gate_s[part]).astype(BF)
        gg_out[...] = gg
        gu_out[...] = gu
        t = nt(gg, wg[...]) + nt(gu, wu[...])
        gmn = t if gmn is None else gmn + t
    gmid = upstream + rms_back(hat_mid, inv_mid, g_fi[...], gmn)
    gmid_out[...] = gmid
    gas = rms_back(hat_attn, inv_attn, g_ao[...], gmid).astype(BF)
    gas_out[...] = gas
    deltas = []
    for part, (wo, ga) in enumerate(((wo_o, ga_o), (wo_x, ga_x))):
        g = nt(gas, wo[...]).astype(BF)
        ga[...] = g
        for h in range(heads_per):
            gh = g[:, h * HEAD_WIDTH : (h + 1) * HEAD_WIDTH].astype(F32)
            deltas.append(jnp.sum(gh * mix[part * heads_per + h], axis=-1, keepdims=True))
    lane = lax.broadcasted_iota(jnp.int32, (rows, LANES), 1)
    lse_all = jnp.zeros((rows, LANES), F32)
    delta_all = jnp.zeros((rows, LANES), F32)
    for n, (a, b) in enumerate(zip(lses, deltas)):
        lse_all = jnp.where(lane == n, a, lse_all)
        delta_all = jnp.where(lane == n, b, delta_all)
    lse_out[...] = jnp.transpose(lse_all)[:8]
    delta_out[...] = jnp.transpose(delta_all)[:8]

    @pl.when(i == 0)
    def _():
        gains[...] = jnp.zeros_like(gains)

    gains[0:1, :] += jnp.sum(upstream * hat_ff, axis=0, keepdims=True)
    gains[1:2, :] += jnp.sum(gmn * hat_mid, axis=0, keepdims=True)
    gains[2:3, :] += jnp.sum(gmid * hat_attn, axis=0, keepdims=True)


def attn_rows(i, seg, buf, lse, delta, gq, qr_o, qr_x, dk, dv, gain):
    rows = QB
    base = pl.multiple_of(i * rows, rows)
    mine = pl.ds(base, rows)
    k_win = buf["k"][pl.ds(base, WIN), :]
    v_win = buf["v"][pl.ds(base, WIN), :]
    seg_k = column_of(seg[:, pl.ds(base, WIN)])[:, :1]
    seg_q = seg[:, pl.ds(base + BLOCK, rows)]
    lane = lax.broadcasted_iota(jnp.int32, (WIN, rows), 1)
    sub = lax.broadcasted_iota(jnp.int32, (WIN, rows), 0)
    mask = (seg_q == seg_k) & (sub <= lane + (WIN - rows))
    cos = buf["cos"][mine, :]
    sin = buf["sin"][mine, :]
    dk_sum = None
    dv_sum = None
    g_sum = None
    heads = qr_o.shape[1] // HEAD_WIDTH
    for n in range(2 * heads):
        side = "ox"[n // heads]
        qraw = (qr_o, qr_x)[n // heads]
        h = n % heads
        cols = slice(h * HEAD_WIDTH, (h + 1) * HEAD_WIDTH)
        qh = buf["q_" + side][mine, cols]
        gh = buf["ga_" + side][mine, cols]
        s = jnp.where(mask, nt(k_win, qh), -jnp.inf)
        p = jnp.exp(s - lse[n : n + 1, mine])
        ds = (p * (nt(v_win, gh) - delta[n : n + 1, mine])).astype(BF)
        dq = tn(ds, k_win) * SCORE_SCALE
        a = nn(ds, qh)
        b = nn(p.astype(BF), gh)
        dk_sum = a if dk_sum is None else dk_sum + a
        dv_sum = b if dv_sum is None else dv_sum + b
        dqn = rotate(dq, cos, sin, -1)
        hat, inv = rms_stats(buf["ql_" + side][mine, cols])
        g = jnp.sum(dqn * hat, axis=0, keepdims=True)
        g_sum = g if g_sum is None else g_sum + g
        qraw[mine, cols] = rms_back(hat, inv, gq, dqn).astype(BF)
    dk[pl.ds(base, WIN), :] += dk_sum
    dv[pl.ds(base, WIN), :] += dv_sum
    gain[...] += g_sum


def whole(shape):
    return pl.BlockSpec(shape, lambda *_: (0,) * len(shape), pipeline_mode=pl.Buffered(1))


def rows_of(n, width, shift=0):
    if shift:
        return pl.BlockSpec((n, width), lambda i, *_: (jnp.maximum(i - shift, 0), 0))
    return pl.BlockSpec((n, width), lambda i, *_: (i, 0))


def params():
    return pltpu.CompilerParams(dimension_semantics=("arbitrary",), vmem_limit_bytes=VMEM_LIMIT)


def cost(us):
    return pl.CostEstimate(flops=us * 10**9, bytes_accessed=us * 10**6, transcendentals=0)


def sds(shape, dtype):
    return jax.ShapeDtypeStruct(shape, dtype)


def project(first_row, own, x3, seg, table, gain_list, wq_o, wq_x, wk, wv):
    depth = x3.shape[2]
    ext = own + BLOCK
    part = wq_o.shape[1]
    n = BLOCK
    me_block = lambda i, me: (0, jnp.maximum(me[0] // n + i - 1, 0), 0)
    return pl.pallas_call(
        project_kernel,
        grid_spec=pltpu.PrefetchScalarGridSpec(
            num_scalar_prefetch=1,
            grid=(ext // n,),
            in_specs=[
                pl.BlockSpec((1, n, depth), me_block),
                whole(seg.shape),
                whole(table.shape),
                *[whole(g.shape) for g in gain_list],
                whole(wq_o.shape), whole(wq_x.shape), whole(wk.shape), whole(wv.shape),
            ],
            out_specs=[
                rows_of(n, part, 1), rows_of(n, part, 1), rows_of(n, part, 1), rows_of(n, part, 1),
                rows_of(n, HEAD_WIDTH), rows_of(n, HEAD_WIDTH), rows_of(n, HEAD_WIDTH, 1),
                rows_of(n, depth, 1), rows_of(n, LANES, 1), rows_of(n, LANES, 1),
                pl.BlockSpec((1, n), lambda i, *_: (0, i)), pl.BlockSpec((8, depth), lambda i, *_: (0, 0)),
            ],
        ),
        out_shape=[
            sds((own, part), BF), sds((own, part), BF), sds((own, part), F32), sds((own, part), F32),
            sds((ext, HEAD_WIDTH), BF), sds((ext, HEAD_WIDTH), BF), sds((own, HEAD_WIDTH), F32),
            sds((own, depth), BF), sds((own, LANES), F32), sds((own, LANES), F32),
            sds((1, ext), jnp.int32), sds((8, depth), F32),
        ],
        compiler_params=params(),
        cost_estimate=cost(6),
        name="project",
    )(first_row, x3, seg, table, *gain_list, wq_o, wq_x, wk, wv)


def block_pass(first_row, x3, up3, seg_ext, q_o, q_x, k, v, weights, rows8):
    depth = x3.shape[2]
    own, part = q_o.shape
    n = QB
    hidden = weights[2].shape[1]
    mine = pl.BlockSpec((1, n, depth), lambda i, me: (0, me[0] // n + i, 0))
    kern = lambda me, *refs: block_kernel(*refs)
    heads = 2 * part // HEAD_WIDTH
    return pl.pallas_call(
        kern,
        grid_spec=pltpu.PrefetchScalarGridSpec(
            num_scalar_prefetch=1,
            grid=(own // n,),
            in_specs=[mine, mine, whole(seg_ext.shape), rows_of(n, part), rows_of(n, part),
                      whole(k.shape), whole(v.shape)]
            + [whole(w.shape) for w in weights]
            + [whole(rows8.shape)],
            out_specs=[rows_of(n, depth)] * 2 + [rows_of(n, part)] * 4 + [pl.BlockSpec((8, n), lambda i, *_: (0, i))] * 2
            + [rows_of(n, depth)] * 3 + [rows_of(n, hidden)] * 6
            + [pl.BlockSpec((8, depth), lambda i, *_: (0, 0))],
            scratch_shapes=[
                pltpu.VMEM((heads, n, HEAD_WIDTH), F32),
                pltpu.VMEM((2, n, hidden), F32),
                pltpu.VMEM((2, n, hidden), F32),
            ],
        ),
        out_shape=[sds((own, depth), F32)] * 2 + [sds((own, part), BF)] * 4 + [sds((8, own), F32)] * 2
        + [sds((own, depth), BF)] * 3 + [sds((own, hidden), BF)] * 6 + [sds((8, depth), F32)],
        compiler_params=params(),
        cost_estimate=cost(40),
        name="block",
    )(first_row, x3, up3, seg_ext, q_o, q_x, k, v, *weights, rows8)


def swap(value, n_tensor):
    return lax.ppermute(value, "tensor", [(t, n_tensor - 1 - t) for t in range(n_tensor)])


def bit_of(index, b):
    return lax.rem(lax.div(index, 2**b), 2)


def bit_orders(n_bits):
    plain = tuple(range(n_bits))
    turned = plain[1:] + plain[:1]
    lead = (plain[2],) + plain[:2] + plain[3:] if n_bits > 2 else plain[::-1]
    return plain, turned, lead


def natural_index(me, j, fixed, free):
    index = 0
    for b, flip in fixed:
        mine = bit_of(me, b)
        index = index + (1 - mine if flip else mine) * 2**b
    for k, b in enumerate(free):
        index = index + lax.rem(lax.div(j, 2 ** (len(free) - 1 - k)), 2) * 2**b
    return index


NAMES = ("x", "gmid", "wq_o", "wq_x", "wk", "wv", "kl", "cos", "sin", "nb", "k", "v", "q_o", "q_x", "ga_o", "ga_x",
         "ql_o", "ql_x")


def finish_kernel(items, kv_groups, n_bits, *refs):
    n_items = len(items)
    kv_order = sum(kv_groups, ())
    refs = list(refs)
    take = lambda count: [refs.pop(0) for _ in range(count)]
    ins = [take(1) for _, early in items if early]
    seg, lse, delta, rows8, g_block = take(5)
    far = take(len(NAMES))
    outs = take(n_items)
    k_out, v_out, gain_out, gin_far = take(4)
    near = take(len(NAMES))
    local_sems = refs.pop(0)
    (front, front_got, dk_all, dv_all, qr_o, qr_x, kraw, vraw, kv_in, query_sent, query_got, query,
     g_in, g_k, g_q) = take(15)
    ins.append([query])
    recvs, curs = [], []
    for _ in items:
        recvs.append({s: refs.pop(0) for s in range(n_bits)})
        curs.append({s: refs.pop(0) for s in range(1, n_bits)})
    kv_core = refs.pop(0)
    kv_recv = take(len(kv_groups))
    kv_cur = take(len(kv_groups))
    kv_all = refs.pop(0)
    kv_wide = refs.pop(0)
    gain_own = take(len(kv_groups) + 1)
    gain_got = take(len(kv_groups) + 1)
    send_sems, recv_sems = take(2)

    me = lax.axis_index("dp")
    core = lax.axis_index("tensor")

    def flipped(bits):
        return me + sum((1 - 2 * bit_of(me, b)) * 2**b for b in bits)

    def subsets(group):
        return [tuple(b for k, b in enumerate(group) if m >> k & 1) for m in range(1, 2 ** len(group))]

    peers = {(b,) for b in range(n_bits)} | {tuple(sorted(m)) for g in kv_groups for m in subsets(g)}
    barrier = pltpu.get_barrier_semaphore()
    for bits in sorted(peers):
        pl.semaphore_signal(barrier, inc=1, device_id={"dp": flipped(bits)}, device_id_type=pl.DeviceIdType.MESH)
    pl.semaphore_signal(barrier, inc=1, device_id={"tensor": 1 - core}, device_id_type=pl.DeviceIdType.MESH)
    pl.semaphore_wait(barrier, len(peers) + 1)

    sent = []

    def send(src, dst, device):
        k = len(sent)
        copy = pltpu.make_async_remote_copy(
            src_ref=src, dst_ref=dst, send_sem=send_sems.at[k], recv_sem=recv_sems.at[k],
            device_id=device, device_id_type=pl.DeviceIdType.MESH)
        copy.start()
        sent.append(copy)
        return copy

    flying = {}

    def start(n, s):
        order, _ = items[n]
        half = 2 ** (n_bits - s - 1)
        device = {"dp": flipped((order[s],))}
        if s == 0:
            flying[n] = [
                send(ins[n][0].at[natural_index(me, j, ((order[0], True),), order[1:])], recvs[n][0].at[j], device)
                for j in range(half)
            ]
        else:
            away = (1 - bit_of(me, order[s])) * half
            flying[n] = [send(curs[n][s].at[pl.ds(away, half)], recvs[n][s], device)]

    def finish(n, s):
        order, _ = items[n]
        half = 2 ** (n_bits - s - 1)
        for copy in flying.pop(n):
            copy.wait_recv()
        got = recvs[n][s]
        held = curs[n][s] if s else ins[n][0]

        def total_at(j):
            if s:
                index = bit_of(me, order[s]) * half + j
            else:
                index = natural_index(me, j, ((order[0], False),), order[1:])
            return held[index].astype(F32) + got[j].astype(F32)

        if s == n_bits - 1:
            outs[n][...] = total_at(0)
            return

        def body(j, carry):
            curs[n][s + 1][j] = total_at(j).astype(BF)
            return carry

        lax.fori_loop(0, half, body, 0)
        start(n, s + 1)

    other_core = {"tensor": 1 - core}
    own, depth = near[0].shape
    sources = list(far)
    sources[0] = far[0].at[0, pl.ds(pl.multiple_of(core * own, own), own), :]
    buf = dict(zip(NAMES, near))
    fetch = {name: pltpu.make_async_copy(s, d, local_sems.at[k])
             for k, (name, s, d) in enumerate(zip(NAMES, sources, near))}
    first_use = ("k", "v", "q_o", "ga_o", "cos", "sin", "ql_o", "q_x", "ga_x", "ql_x")
    second_use = ("nb", "kl", "wk", "wv", "wq_o", "wq_x", "x", "gmid")
    for name in first_use:
        fetch[name].start()
    for n in range(n_items):
        if items[n][1]:
            start(n, 0)
    for name in second_use:
        fetch[name].start()
    dk_all[...] = jnp.zeros_like(dk_all)
    dv_all[...] = jnp.zeros_like(dv_all)
    g_q[...] = jnp.zeros_like(g_q)
    gq_row = rows8[4:5, :HEAD_WIDTH]
    for name in first_use:
        fetch[name].wait()

    def attn_body(i, carry):
        attn_rows(i, seg, buf, lse, delta, gq_row, qr_o, qr_x, dk_all, dv_all, g_q)
        return carry

    lax.fori_loop(0, own // QB, attn_body, 0)
    front[:, :HEAD_WIDTH] = dk_all[:BLOCK, :].astype(BF)
    front[:, HEAD_WIDTH:] = dv_all[:BLOCK, :].astype(BF)
    front_copy = send(front, front_got, other_core)
    fetch["nb"].wait()
    query_sent[...] = tn(qr_x[...], buf["nb"][...]).astype(BF)
    query_copy = send(query_sent, query_got, other_core)
    fetch["kl"].wait()
    front_copy.wait_recv()
    gk_row, gin_row = rows8[5:6, :HEAD_WIDTH], rows8[0:1, :]
    g_k[...] = jnp.zeros_like(g_k)
    g_in[...] = jnp.zeros_like(g_in)
    blocks = own // BLOCK

    def kv_rows(i, carry):
        at = pl.ds(pl.multiple_of(i * BLOCK, BLOCK), BLOCK)
        tail = ((i == blocks - 1) & (core == 0)).astype(F32)
        later = pl.ds(pl.multiple_of((i + 1) * BLOCK, BLOCK), BLOCK)
        dk = dk_all[later, :] + tail * front_got[:, :HEAD_WIDTH].astype(F32)
        dv = dv_all[later, :] + tail * front_got[:, HEAD_WIDTH:].astype(F32)
        dkn = rotate(dk, buf["cos"][at, :], buf["sin"][at, :], -1)
        k_hat, k_inv = rms_stats(buf["kl"][at, :])
        kraw[at, :] = rms_back(k_hat, k_inv, gk_row, dkn).astype(BF)
        vraw[at, :] = dv.astype(BF)
        g_k[...] += jnp.sum(dkn * k_hat, axis=0, keepdims=True)
        return carry

    lax.fori_loop(0, blocks, kv_rows, 0)
    n_chunk, rows_k = kv_in.shape[1:3]
    for t, raw in enumerate((kraw, vraw)):
        kv_in[t] = tn(raw[...], buf["nb"][...]).astype(BF).reshape(n_chunk, rows_k, depth)
    kv_copies = [send(kv_in.at[1 - core], kv_core, other_core)]
    query_copy.wait_recv()
    own_query = tn(qr_o[...], buf["nb"][...]) + query_got[...].astype(F32)
    query[...] = own_query.astype(BF).reshape(query.shape)
    start(n_items - 1, 0)
    kv_copies[0].wait_recv()

    def kv_first(j, carry):
        index = natural_index(me, j, (), kv_order)
        kv_cur[0][j] = (kv_in[core, index].astype(F32) + kv_core[index].astype(F32)).astype(BF)
        return carry

    lax.fori_loop(0, 2**n_bits, kv_first, 0)

    def rest_of(g):
        return 2 ** (n_bits - sum(len(x) for x in kv_groups[: g + 1]))

    def block_index(group, bits):
        index = 0
        for k, b in enumerate(group):
            mine = bit_of(me, b)
            index = index + (1 - mine if b in bits else mine) * 2 ** (len(group) - 1 - k)
        return index

    def kv_start(g):
        rest = rest_of(g)
        return [send(kv_cur[g].at[pl.ds(block_index(kv_groups[g], m) * rest, rest)], kv_recv[g].at[c],
                     {"dp": flipped(m)}) for c, m in enumerate(subsets(kv_groups[g]))]

    spot = 0
    for k, b in enumerate(kv_order):
        spot = spot + bit_of(me, b) * 2 ** (n_bits - 1 - k)
    kv_copies = kv_start(0)
    for n in range(n_items):
        if items[n][1]:
            finish(n, 0)
    for name in ("wk", "wv", "wq_o", "wq_x", "x", "gmid"):
        fetch[name].wait()

    def input_rows(i, carry):
        at = pl.ds(pl.multiple_of(i * QB, QB), QB)
        gn = nt(kraw[at, :], buf["wk"][...]) + nt(vraw[at, :], buf["wv"][...])
        gn = gn + nt(qr_o[at, :], buf["wq_o"][...]) + nt(qr_x[at, :], buf["wq_x"][...])
        hat, inv = rms_stats(buf["x"][at, :])
        buf["x"][at, :] = buf["gmid"][at, :] + rms_back(hat, inv, gin_row, gn)
        g_in[...] += jnp.sum(gn * hat, axis=0, keepdims=True)
        return carry

    gain_copies = []

    def gain_start(s):
        if s == 0:
            gain_copies.append([send(gain_own[0], gain_got[0].at[0], other_core)])
        else:
            gain_copies.append([send(gain_own[s], gain_got[s].at[c], {"dp": flipped(m)})
                                for c, m in enumerate(subsets(kv_groups[s - 1]))])

    def gain_step():
        s = len(gain_copies) - 1
        total = gain_own[s][...]
        for c, copy in enumerate(gain_copies[s]):
            copy.wait_recv()
            total = total + gain_got[s][c]
        if s == len(kv_groups):
            gain_out[...] = total
            return True
        gain_own[s + 1][...] = total
        gain_start(s + 1)
        return False

    half_rows = own // QB // 2

    def fill_first():
        lax.fori_loop(0, half_rows, input_rows, 0)

    def fill_second():
        lax.fori_loop(half_rows, own // QB, input_rows, 0)
        gain_own[0][...] = jnp.zeros_like(gain_own[0])
        gain_own[0][0:3, :] = g_block[0:3, :]
        gain_own[0][3:4, :] = g_in[...]
        gain_own[0][4:5, :HEAD_WIDTH] = g_q[...]
        gain_own[0][5:6, :HEAD_WIDTH] = g_k[...]
        gain_start(0)

    gin_copy = pltpu.make_async_copy(buf["x"], gin_far, local_sems.at[len(NAMES)])
    fills = [fill_first, fill_second, gin_copy.start]
    rank = lambda e: e[1] - (1 if items[e[0]][1] else 0)
    todo = [(n, s) for s in range(n_bits) for n in range(n_items) if s or not items[n][1]]
    todo.sort(key=rank)

    def advance():
        now = rank(todo[0]) if todo else 0
        while todo and rank(todo[0]) == now:
            finish(*todo.pop(0))

    for g in range(len(kv_groups)):
        rest = rest_of(g)
        for copy in kv_copies:
            copy.wait_recv()
        base = block_index(kv_groups[g], ()) * rest

        def kv_total(j, g=g, base=base):
            total = kv_cur[g][base + j].astype(F32)
            for c in range(2 ** len(kv_groups[g]) - 1):
                total = total + kv_recv[g][c, j].astype(F32)
            return total.astype(BF)

        if g < len(kv_groups) - 1:

            def kv_body(j, carry, g=g, kv_total=kv_total):
                kv_cur[g + 1][j] = kv_total(j)
                return carry

            lax.fori_loop(0, rest, kv_body, 0)
            kv_copies = kv_start(g + 1)
            if len(fills) > 2:
                fills.pop(0)()
            advance()
        else:
            kv_all[core, spot] = kv_total(0)
    gains_done = False
    for g in reversed(range(len(kv_groups))):
        size = rest_of(g)
        begin = 0
        for k, b in enumerate(sum(kv_groups[: g + 1], ())):
            begin = begin + bit_of(me, b) * 2 ** (n_bits - 1 - k)
        region = kv_all.at[core, pl.ds(begin, size)]
        copies = [send(region, region, {"dp": flipped(m)}) for m in subsets(kv_groups[g])]
        while len(fills) > 1:
            fills.pop(0)()
        if fills:
            fills.pop(0)()
        elif not gains_done:
            gains_done = gain_step()
        advance()
        for copy in copies:
            copy.wait_recv()
    copy = send(kv_all.at[core], kv_all.at[core], other_core)
    while todo:
        advance()
    while not gains_done:
        gains_done = gain_step()
    copy.wait_recv()

    def unpack(j, carry):
        index = natural_index(me, j, (), kv_order)
        for t in range(2):
            kv_wide[t, index] = kv_all[t, j].astype(F32)
        return carry

    lax.fori_loop(0, 2**n_bits, unpack, 0)
    for t, out in enumerate((k_out, v_out)):
        out[...] = jnp.transpose(kv_wide[t].reshape(HEAD_WIDTH, depth))
    gin_copy.wait()
    for copy in sent:
        copy.wait_send()


def finish_all(n_dp, items, order, kv_order, small, far):
    n_bits = len(kv_order)
    own, part = far[12].shape
    ext = far[10].shape[0]
    depth = far[1].shape[1]
    groups = tuple(tuple(kv_order[k : k + 2]) for k in range(0, n_bits, 2))
    spec, operands, outs, comm = [], [], [], []
    copies = 3
    shapes = [value.shape for value, _ in items] + [(n_dp, part // n_dp, depth)]
    for k, (n, c, width) in enumerate(shapes):
        early = k < len(items)
        spec.append((tuple(items[k][1] if early else order), early))
        if early:
            operands.append(items[k][0])
        outs.append(sds((c, width), F32))
        comm += [pltpu.VMEM((2 ** (n_bits - s - 1), c, width), BF) for s in range(n_bits)]
        comm += [pltpu.VMEM((2 ** (n_bits - s), c, width), BF) for s in range(1, n_bits)]
        copies += n_bits - 1 + n // 2
    n, c, width = n_dp, HEAD_WIDTH // n_dp, depth
    comm += [pltpu.VMEM((n, c, width), BF)]
    sizes = [2 ** (n_bits - sum(len(x) for x in groups[:g])) for g in range(len(groups) + 1)]
    comm += [pltpu.VMEM((2 ** len(groups[g]) - 1, sizes[g + 1], c, width), BF) for g in range(len(groups))]
    comm += [pltpu.VMEM((sizes[g], c, width), BF) for g in range(len(groups))]
    comm += [pltpu.VMEM((2, n, c, width), BF)]
    comm += [pltpu.VMEM((2, n, c, width), F32)]
    comm += [pltpu.VMEM((8, width), F32) for _ in range(len(groups) + 1)]
    comm += [pltpu.VMEM((1, 8, width), F32)] + [pltpu.VMEM((2 ** len(g) - 1, 8, width), F32) for g in groups]
    copies += 3 + 3 * sum(2 ** len(g) - 1 for g in groups)
    comm += [pltpu.SemaphoreType.DMA((copies,)), pltpu.SemaphoreType.DMA((copies,))]
    outs += [sds((width, HEAD_WIDTH), F32), sds((width, HEAD_WIDTH), F32), sds((8, width), F32), sds((own, depth), F32)]
    near = [pltpu.VMEM((own, depth), F32)] + [pltpu.VMEM(a.shape, a.dtype) for a in far[1:]]
    scratch = near + [
        pltpu.SemaphoreType.DMA((len(far) + 1,)),
        pltpu.VMEM((BLOCK, 2 * HEAD_WIDTH), BF), pltpu.VMEM((BLOCK, 2 * HEAD_WIDTH), BF),
        pltpu.VMEM((ext, HEAD_WIDTH), F32), pltpu.VMEM((ext, HEAD_WIDTH), F32),
        pltpu.VMEM((own, part), BF), pltpu.VMEM((own, part), BF),
        pltpu.VMEM((own, HEAD_WIDTH), BF), pltpu.VMEM((own, HEAD_WIDTH), BF),
        pltpu.VMEM((2, n, c, width), BF), pltpu.VMEM((part, depth), BF), pltpu.VMEM((part, depth), BF),
        pltpu.VMEM((n_dp, part // n_dp, depth), BF), pltpu.VMEM((1, depth), F32),
        pltpu.VMEM((1, HEAD_WIDTH), F32), pltpu.VMEM((1, HEAD_WIDTH), F32),
    ] + comm
    vmem = pl.BlockSpec(memory_space=pltpu.VMEM)
    anywhere = pl.BlockSpec(memory_space=pl.ANY)
    operands += list(small)
    return pl.pallas_call(
        functools.partial(finish_kernel, tuple(spec), groups, n_bits),
        out_shape=outs,
        in_specs=[vmem] * len(operands) + [anywhere] * len(far),
        out_specs=[vmem] * (len(outs) - 1) + [anywhere],
        scratch_shapes=scratch,
        compiler_params=pltpu.CompilerParams(collective_id=0, has_side_effects=True, vmem_limit_bytes=VMEM_LIMIT),
        name="finish_all",
    )(*operands, *far)


def after(value, *others):
    return lax.optimization_barrier((value,) + others)[0]


def on_device(n_dp, n_tensor, residual_in, cotangent, segment_ids, gain_attn_in, w_query, w_key, w_value,
              gain_query, gain_key, w_out, gain_attn_out, gain_ff_in, w_gate, w_up, w_down, gain_ff_out):
    tokens, depth = residual_in.shape[1:]
    own = tokens // n_tensor
    me = lax.axis_index("tensor")
    first_row = (me * own).astype(jnp.int32).reshape(1)
    wq_x, wo_x, wg_x, wu_x, wd_x = (swap(w, n_tensor) for w in (w_query, w_out, w_gate, w_up, w_down))
    table = jnp.asarray(rope_table())
    gain_list = (gain_attn_in, gain_attn_out, gain_ff_in, gain_ff_out, gain_query, gain_key)
    q_o, q_x, ql_o, ql_x, k, v, kl, nb, cos, sin, seg_ext, rows8 = project(
        first_row, own, residual_in, segment_ids, table, gain_list, w_query, wq_x, w_key, w_value)
    weights = (w_out, wo_x, w_gate, wg_x, w_up, wu_x, w_down, wd_x)
    (output, gmid, ga_o, ga_x, af_o, af_x, lse, delta, mid_b, gff, gas,
     act_o, act_x, gg_o, gg_x, gu_o, gu_x, gains) = block_pass(
        first_row, residual_in, cotangent, seg_ext, q_o, q_x, k, v, weights, rows8)

    n_bits = n_dp.bit_length() - 1
    plain, turned, lead = bit_orders(n_bits)
    chunks = lambda value: value.reshape(n_dp, value.shape[0] // n_dp, value.shape[1])

    pairs = [(gff, act_x, act_o, plain), (mid_b, gg_x, gg_o, turned), (mid_b, gu_x, gu_o, lead), (gas, af_x, af_o, plain)]
    grad = lambda left, units: tn(left, units) if left is not mid_b else tn(units, left)
    gots = []
    last = ()
    for left, units, _, _ in pairs:
        sent = grad(left, after(units, *last)).astype(BF)
        last = (sent,)
        gots.append(swap(sent, n_tensor))
    items = []
    for (left, _, units, order), got in zip(pairs, gots):
        items.append((chunks((grad(left, after(units, *last)) + got.astype(F32)).astype(BF)), order))
    far = (residual_in, gmid, w_query, wq_x, w_key, w_value, kl, cos, sin, nb, k, v, q_o, q_x, ga_o, ga_x, ql_o, ql_x)
    *shares, k_sum, v_sum, gain_sum, grad_input = finish_all(
        n_dp, items, plain, plain, (seg_ext, lse, delta, rows8, gains), far)
    s_down, s_gate, s_up, s_out, s_query = shares
    return (
        output[None], grad_input[None], gain_sum[3], s_query.T, k_sum, v_sum,
        gain_sum[4, :HEAD_WIDTH], gain_sum[5, :HEAD_WIDTH],
        s_out.T, gain_sum[2], gain_sum[1], s_gate.T, s_up.T, s_down.T, gain_sum[0],
    )


def solution(mesh):
    n_dp, n_tensor = mesh.shape["dp"], mesh.shape["tensor"]
    return jax.shard_map(
        functools.partial(on_device, n_dp, n_tensor),
        mesh=mesh,
        in_specs=(
            P("dp", None, None), P("dp", None, None), P("dp", None), P(), P(None, "tensor"), P(), P(), P(), P(),
            P("tensor", None), P(), P(), P(None, "tensor"), P(None, "tensor"), P("tensor", None), P(),
        ),
        out_specs=(
            P("dp", "tensor", None), P("dp", "tensor", None), P(), P(None, ("tensor", "dp")), P(), P(), P(), P(),
            P("tensor", "dp"), P(), P(), P(None, ("tensor", "dp")), P(None, ("tensor", "dp")), P("tensor", "dp"),
            P(),
        ),
        check_vma=False,
    )
```

```python
import functools
import jax
import jax.numpy as jnp
import numpy as np
from jax import lax
from jax.experimental import pallas as pl
from jax.experimental.pallas import tpu as pltpu
from jax.sharding import PartitionSpec as P

HEAD_WIDTH = 256
BLOCK = 512
EPS = 1e-06
THETA = 1000000.0
SCORE_SCALE = 0.0625
GELU_C = 0.7978845608028654
GELU_A = 0.044715
HALF = HEAD_WIDTH // 2
QB = 256
WIN = BLOCK + QB
LANES = 128
BF = jnp.bfloat16
F32 = jnp.float32
VMEM_LIMIT = 60 << 20


def nn(a, b):
    return lax.dot_general(a, b, (((1,), (0,)), ((), ())), preferred_element_type=F32)


def nt(a, b):
    return lax.dot_general(a, b, (((1,), (1,)), ((), ())), preferred_element_type=F32)


def tn(a, b):
    return lax.dot_general(a, b, (((0,), (0,)), ((), ())), preferred_element_type=F32)


def rms_stats(v):
    inv = lax.rsqrt(jnp.mean(v * v, axis=-1, keepdims=True) + EPS)
    return v * inv, inv


def rms_back(hat, inv, gain, up):
    scaled = up * gain
    return inv * (scaled - hat * jnp.mean(scaled * hat, axis=-1, keepdims=True))


def rotate(v, cos, sin, direction):
    a, b = v[:, :HALF], v[:, HALF:]
    if direction > 0:
        return jnp.concatenate([a * cos - b * sin, b * cos + a * sin], axis=-1)
    return jnp.concatenate([a * cos + b * sin, b * cos - a * sin], axis=-1)


def column_of(row):
    n = row.shape[1]
    return jnp.transpose(jnp.broadcast_to(row, (LANES, n)))


def rope_table():
    freq = np.arange(HALF, dtype=np.float32)
    inv_freq = np.exp(freq * np.float32(-2.0 * np.log(THETA) / HEAD_WIDTH)).astype(np.float32)
    angles = np.arange(BLOCK, dtype=np.float32)[:, None] * inv_freq[None, :]
    parts = []
    for tab in (np.cos(angles.astype(np.float64)), np.sin(angles.astype(np.float64))):
        tab = tab.astype(np.float32)
        hi = tab.astype(BF)
        lo = (tab - hi.astype(np.float32)).astype(BF)
        parts += [hi, lo]
    return np.concatenate(parts, axis=1)


def project_kernel(me, x, seg, table, g1, g2, g3, g4, g5, g6, wq_o, wq_x, wk, wv,
                   q_o, q_x, ql_o, ql_x, k_out, v_out, kl_out, nb_out, cos_out, sin_out, seg_out, rows8):
    i = pl.program_id(0)
    rows = x.shape[1]

    @pl.when(i == 0)
    def _():
        rows8[...] = jnp.zeros_like(rows8)
        for r, g in enumerate((g1, g2, g3, g4, g5, g6)):
            rows8[r : r + 1, : g.shape[0]] = g[...].reshape(1, g.shape[0])

    g_in, gq, gk = gain_refs(rows8, 0, 4, 5)
    hat, _ = rms_stats(x[0])
    nb = (hat * g_in[...]).astype(BF)
    nb_out[...] = nb
    base = me[0] + (i - 1) * rows
    seg_row = seg[:, pl.ds(pl.multiple_of(jnp.maximum(base, 0), rows), rows)]
    seg_row = jnp.where(base < 0, -1, seg_row)
    seg_out[...] = seg_row
    before = (seg[...] < column_of(seg_row)[:, :1]).astype(F32)
    start = jnp.sum(before, axis=1, keepdims=True)
    pos = lax.broadcasted_iota(jnp.int32, (rows, 1), 0) + base - start.astype(jnp.int32)
    hot = (lax.broadcasted_iota(jnp.int32, (rows, BLOCK), 1) == pos).astype(F32).astype(BF)
    cs = nn(hot, table[...])
    cos = cs[:, :LANES] + cs[:, LANES : 2 * LANES]
    sin = cs[:, 2 * LANES : 3 * LANES] + cs[:, 3 * LANES :]
    cos_out[...] = cos
    sin_out[...] = sin
    k_lin = nn(nb, wk[...])
    kl_out[...] = k_lin
    k_hat, _ = rms_stats(k_lin)
    k_out[...] = rotate(k_hat * gk[...], cos, sin, 1).astype(BF)
    v_out[...] = nn(nb, wv[...]).astype(BF)

    @pl.when(i > 0)
    def _():
        for w, lin_out, out in ((wq_o, ql_o, q_o), (wq_x, ql_x, q_x)):
            lin = nn(nb, w[...])
            lin_out[...] = lin
            for h in range(lin.shape[1] // HEAD_WIDTH):
                cols = slice(h * HEAD_WIDTH, (h + 1) * HEAD_WIDTH)
                q_hat, _ = rms_stats(lin[:, cols])
                out[:, cols] = (rotate(q_hat * gq[...], cos, sin, 1) * SCORE_SCALE).astype(BF)


def gain_refs(rows8, *which):
    width = rows8.shape[1]
    return [rows8.at[r : r + 1, : (width if r < 4 else HEAD_WIDTH)] for r in which]


def score_mask(seg_q, seg_k, rows, width):
    lane = lax.broadcasted_iota(jnp.int32, (rows, width), 1)
    sub = lax.broadcasted_iota(jnp.int32, (rows, width), 0)
    return (seg_q == seg_k) & (lane <= sub + (width - rows))


def block_kernel(x, up, seg, q_o, q_x, k, v, wo_o, wo_x, wg_o, wg_x, wu_o, wu_x, wd_o, wd_x,
                 rows8,
                 out, gmid_out, ga_o, ga_x, af_o, af_x, lse_out, delta_out, mid_out, gff_out, gas_out,
                 act_o, act_x, gg_o, gg_x, gu_o, gu_x, gains,
                 mix, gate_s, up_s):
    g_ao, g_fi, g_fo = gain_refs(rows8, 1, 2, 3)
    i = pl.program_id(0)
    rows = x.shape[1]
    base = pl.multiple_of(i * rows, rows)
    k_win = k[pl.ds(base, WIN), :]
    v_win = v[pl.ds(base, WIN), :]
    seg_k = seg[:, pl.ds(base, WIN)]
    seg_q = column_of(seg[:, pl.ds(base + BLOCK, rows)])[:, :1]
    mask = score_mask(seg_q, seg_k, rows, WIN)
    heads_per = q_o.shape[1] // HEAD_WIDTH
    lses = []
    for part, (q, af) in enumerate(((q_o, af_o), (q_x, af_x))):
        for h in range(heads_per):
            cols = slice(h * HEAD_WIDTH, (h + 1) * HEAD_WIDTH)
            s = jnp.where(mask, nt(q[:, cols], k_win), -jnp.inf)
            top = jnp.max(s, axis=-1, keepdims=True)
            e = jnp.exp(s - top)
            mass = jnp.sum(e, axis=-1, keepdims=True)
            lses.append(top + jnp.log(mass))
            p = (e * (1.0 / mass)).astype(BF)
            m = nn(p, v_win)
            mix[part * heads_per + h] = m
            af[:, cols] = m.astype(BF)
    inputs = x[0]
    upstream = up[0]
    attn_sum = nn(af_o[...], wo_o[...]) + nn(af_x[...], wo_x[...])
    hat_attn, inv_attn = rms_stats(attn_sum)
    middle = inputs + hat_attn * g_ao[...]
    hat_mid, inv_mid = rms_stats(middle)
    mid_b = (hat_mid * g_fi[...]).astype(BF)
    mid_out[...] = mid_b
    ff_sum = None
    for part, (wg, wu, wd, act) in enumerate(((wg_o, wu_o, wd_o, act_o), (wg_x, wu_x, wd_x, act_x))):
        gate = nn(mid_b, wg[...])
        upp = nn(mid_b, wu[...])
        sq = gate * gate
        th = jnp.tanh(gate * (GELU_C + (GELU_C * GELU_A) * sq))
        onep = 0.5 + 0.5 * th
        gelu = gate * onep
        deriv = onep + gate * (1.0 - th * th) * (0.5 * GELU_C + (1.5 * GELU_C * GELU_A) * sq)
        gate_s[part] = gelu
        up_s[part] = upp * deriv
        a = (gelu * upp).astype(BF)
        act[...] = a
        f = nn(a, wd[...])
        ff_sum = f if ff_sum is None else ff_sum + f
    hat_ff, inv_ff = rms_stats(ff_sum)
    out[...] = middle + hat_ff * g_fo[...]
    gff = rms_back(hat_ff, inv_ff, g_fo[...], upstream).astype(BF)
    gff_out[...] = gff
    gmn = None
    for part, (wg, wu, wd, gg_out, gu_out) in enumerate(
        ((wg_o, wu_o, wd_o, gg_o, gu_o), (wg_x, wu_x, wd_x, gg_x, gu_x))
    ):
        gact = nt(gff, wd[...])
        gg = (gact * up_s[part]).astype(BF)
        gu = (gact * gate_s[part]).astype(BF)
        gg_out[...] = gg
        gu_out[...] = gu
        t = nt(gg, wg[...]) + nt(gu, wu[...])
        gmn = t if gmn is None else gmn + t
    gmid = upstream + rms_back(hat_mid, inv_mid, g_fi[...], gmn)
    gmid_out[...] = gmid
    gas = rms_back(hat_attn, inv_attn, g_ao[...], gmid).astype(BF)
    gas_out[...] = gas
    deltas = []
    for part, (wo, ga) in enumerate(((wo_o, ga_o), (wo_x, ga_x))):
        g = nt(gas, wo[...]).astype(BF)
        ga[...] = g
        for h in range(heads_per):
            gh = g[:, h * HEAD_WIDTH : (h + 1) * HEAD_WIDTH].astype(F32)
            deltas.append(jnp.sum(gh * mix[part * heads_per + h], axis=-1, keepdims=True))
    lane = lax.broadcasted_iota(jnp.int32, (rows, LANES), 1)
    lse_all = jnp.zeros((rows, LANES), F32)
    delta_all = jnp.zeros((rows, LANES), F32)
    for n, (a, b) in enumerate(zip(lses, deltas)):
        lse_all = jnp.where(lane == n, a, lse_all)
        delta_all = jnp.where(lane == n, b, delta_all)
    lse_out[...] = jnp.transpose(lse_all)[:8]
    delta_out[...] = jnp.transpose(delta_all)[:8]

    @pl.when(i == 0)
    def _():
        gains[...] = jnp.zeros_like(gains)

    gains[0:1, :] += jnp.sum(upstream * hat_ff, axis=0, keepdims=True)
    gains[1:2, :] += jnp.sum(gmn * hat_mid, axis=0, keepdims=True)
    gains[2:3, :] += jnp.sum(gmid * hat_attn, axis=0, keepdims=True)


def attn_rows(i, seg, buf, lse, delta, gq, qr_o, qr_x, dk, dv, gain):
    rows = QB
    base = pl.multiple_of(i * rows, rows)
    mine = pl.ds(base, rows)
    k_win = buf["k"][pl.ds(base, WIN), :]
    v_win = buf["v"][pl.ds(base, WIN), :]
    seg_k = column_of(seg[:, pl.ds(base, WIN)])[:, :1]
    seg_q = seg[:, pl.ds(base + BLOCK, rows)]
    lane = lax.broadcasted_iota(jnp.int32, (WIN, rows), 1)
    sub = lax.broadcasted_iota(jnp.int32, (WIN, rows), 0)
    mask = (seg_q == seg_k) & (sub <= lane + (WIN - rows))
    cos = buf["cos"][mine, :]
    sin = buf["sin"][mine, :]
    dk_sum = None
    dv_sum = None
    g_sum = None
    heads = qr_o.shape[1] // HEAD_WIDTH
    for n in range(2 * heads):
        side = "ox"[n // heads]
        qraw = (qr_o, qr_x)[n // heads]
        h = n % heads
        cols = slice(h * HEAD_WIDTH, (h + 1) * HEAD_WIDTH)
        qh = buf["q_" + side][mine, cols]
        gh = buf["ga_" + side][mine, cols]
        s = jnp.where(mask, nt(k_win, qh), -jnp.inf)
        p = jnp.exp(s - lse[n : n + 1, mine])
        ds = (p * (nt(v_win, gh) - delta[n : n + 1, mine])).astype(BF)
        dq = tn(ds, k_win) * SCORE_SCALE
        a = nn(ds, qh)
        b = nn(p.astype(BF), gh)
        dk_sum = a if dk_sum is None else dk_sum + a
        dv_sum = b if dv_sum is None else dv_sum + b
        dqn = rotate(dq, cos, sin, -1)
        hat, inv = rms_stats(buf["ql_" + side][mine, cols])
        g = jnp.sum(dqn * hat, axis=0, keepdims=True)
        g_sum = g if g_sum is None else g_sum + g
        qraw[mine, cols] = rms_back(hat, inv, gq, dqn).astype(BF)
    dk[pl.ds(base, WIN), :] += dk_sum
    dv[pl.ds(base, WIN), :] += dv_sum
    gain[...] += g_sum


def whole(shape):
    return pl.BlockSpec(shape, lambda *_: (0,) * len(shape), pipeline_mode=pl.Buffered(1))


def rows_of(n, width, shift=0):
    if shift:
        return pl.BlockSpec((n, width), lambda i, *_: (jnp.maximum(i - shift, 0), 0))
    return pl.BlockSpec((n, width), lambda i, *_: (i, 0))


def params():
    return pltpu.CompilerParams(dimension_semantics=("arbitrary",), vmem_limit_bytes=VMEM_LIMIT)


def cost(us):
    return pl.CostEstimate(flops=us * 10**9, bytes_accessed=us * 10**6, transcendentals=0)


def sds(shape, dtype):
    return jax.ShapeDtypeStruct(shape, dtype)


def project(first_row, own, x3, seg, table, gain_list, wq_o, wq_x, wk, wv):
    depth = x3.shape[2]
    ext = own + BLOCK
    part = wq_o.shape[1]
    n = BLOCK
    me_block = lambda i, me: (0, jnp.maximum(me[0] // n + i - 1, 0), 0)
    return pl.pallas_call(
        project_kernel,
        grid_spec=pltpu.PrefetchScalarGridSpec(
            num_scalar_prefetch=1,
            grid=(ext // n,),
            in_specs=[
                pl.BlockSpec((1, n, depth), me_block),
                whole(seg.shape),
                whole(table.shape),
                *[whole(g.shape) for g in gain_list],
                whole(wq_o.shape), whole(wq_x.shape), whole(wk.shape), whole(wv.shape),
            ],
            out_specs=[
                rows_of(n, part, 1), rows_of(n, part, 1), rows_of(n, part, 1), rows_of(n, part, 1),
                rows_of(n, HEAD_WIDTH), rows_of(n, HEAD_WIDTH), rows_of(n, HEAD_WIDTH, 1),
                rows_of(n, depth, 1), rows_of(n, LANES, 1), rows_of(n, LANES, 1),
                pl.BlockSpec((1, n), lambda i, *_: (0, i)), pl.BlockSpec((8, depth), lambda i, *_: (0, 0)),
            ],
        ),
        out_shape=[
            sds((own, part), BF), sds((own, part), BF), sds((own, part), F32), sds((own, part), F32),
            sds((ext, HEAD_WIDTH), BF), sds((ext, HEAD_WIDTH), BF), sds((own, HEAD_WIDTH), F32),
            sds((own, depth), BF), sds((own, LANES), F32), sds((own, LANES), F32),
            sds((1, ext), jnp.int32), sds((8, depth), F32),
        ],
        compiler_params=params(),
        cost_estimate=cost(6),
        name="project",
    )(first_row, x3, seg, table, *gain_list, wq_o, wq_x, wk, wv)


def block_pass(first_row, x3, up3, seg_ext, q_o, q_x, k, v, weights, rows8):
    depth = x3.shape[2]
    own, part = q_o.shape
    n = QB
    hidden = weights[2].shape[1]
    mine = pl.BlockSpec((1, n, depth), lambda i, me: (0, me[0] // n + i, 0))
    kern = lambda me, *refs: block_kernel(*refs)
    heads = 2 * part // HEAD_WIDTH
    return pl.pallas_call(
        kern,
        grid_spec=pltpu.PrefetchScalarGridSpec(
            num_scalar_prefetch=1,
            grid=(own // n,),
            in_specs=[mine, mine, whole(seg_ext.shape), rows_of(n, part), rows_of(n, part),
                      whole(k.shape), whole(v.shape)]
            + [whole(w.shape) for w in weights]
            + [whole(rows8.shape)],
            out_specs=[rows_of(n, depth)] * 2 + [rows_of(n, part)] * 4 + [pl.BlockSpec((8, n), lambda i, *_: (0, i))] * 2
            + [rows_of(n, depth)] * 3 + [rows_of(n, hidden)] * 6
            + [pl.BlockSpec((8, depth), lambda i, *_: (0, 0))],
            scratch_shapes=[
                pltpu.VMEM((heads, n, HEAD_WIDTH), F32),
                pltpu.VMEM((2, n, hidden), F32),
                pltpu.VMEM((2, n, hidden), F32),
            ],
        ),
        out_shape=[sds((own, depth), F32)] * 2 + [sds((own, part), BF)] * 4 + [sds((8, own), F32)] * 2
        + [sds((own, depth), BF)] * 3 + [sds((own, hidden), BF)] * 6 + [sds((8, depth), F32)],
        compiler_params=params(),
        cost_estimate=cost(40),
        name="block",
    )(first_row, x3, up3, seg_ext, q_o, q_x, k, v, *weights, rows8)


def swap(value, n_tensor):
    return lax.ppermute(value, "tensor", [(t, n_tensor - 1 - t) for t in range(n_tensor)])


def bit_of(index, b):
    return lax.rem(lax.div(index, 2**b), 2)


def bit_orders(n_bits):
    plain = tuple(range(n_bits))
    turned = plain[1:] + plain[:1]
    lead = (plain[2],) + plain[:2] + plain[3:] if n_bits > 2 else plain[::-1]
    return plain, turned, lead


def natural_index(me, j, fixed, free):
    index = 0
    for b, flip in fixed:
        mine = bit_of(me, b)
        index = index + (1 - mine if flip else mine) * 2**b
    for k, b in enumerate(free):
        index = index + lax.rem(lax.div(j, 2 ** (len(free) - 1 - k)), 2) * 2**b
    return index


NAMES = ("x", "gmid", "wq_o", "wq_x", "wk", "wv", "kl", "cos", "sin", "nb", "k", "v", "q_o", "q_x", "ga_o", "ga_x",
         "ql_o", "ql_x")


def finish_kernel(items, kv_groups, n_bits, *refs):
    n_items = len(items)
    kv_order = sum(kv_groups, ())
    refs = list(refs)
    take = lambda count: [refs.pop(0) for _ in range(count)]
    ins = [take(1) for _, early in items if early]
    seg, lse, delta, rows8, g_block = take(5)
    far = take(len(NAMES))
    outs = take(n_items)
    k_out, v_out, gain_out, gin_far = take(4)
    near = take(len(NAMES))
    local_sems, part_sems = take(2)
    (front, front_got, dk_all, dv_all, qr_o, qr_x, kraw, vraw, kv_in, query_sent, query_got, query,
     g_in, g_k, g_q) = take(15)
    ins.append([query])
    recvs, curs = [], []
    for _ in items:
        recvs.append({s: refs.pop(0) for s in range(n_bits)})
        curs.append({s: refs.pop(0) for s in range(1, n_bits)})
    kv_core = refs.pop(0)
    kv_recv = take(len(kv_groups))
    kv_cur = take(len(kv_groups))
    kv_all = refs.pop(0)
    kv_wide = refs.pop(0)
    gain_own = take(len(kv_groups) + 1)
    gain_got = take(len(kv_groups) + 1)
    send_sems, recv_sems = take(2)

    me = lax.axis_index("dp")
    core = lax.axis_index("tensor")

    def flipped(bits):
        return me + sum((1 - 2 * bit_of(me, b)) * 2**b for b in bits)

    def subsets(group):
        return [tuple(b for k, b in enumerate(group) if m >> k & 1) for m in range(1, 2 ** len(group))]

    peers = {(b,) for b in range(n_bits)} | {tuple(sorted(m)) for g in kv_groups for m in subsets(g)}
    barrier = pltpu.get_barrier_semaphore()
    for bits in sorted(peers):
        pl.semaphore_signal(barrier, inc=1, device_id={"dp": flipped(bits)}, device_id_type=pl.DeviceIdType.MESH)
    pl.semaphore_signal(barrier, inc=1, device_id={"tensor": 1 - core}, device_id_type=pl.DeviceIdType.MESH)
    pl.semaphore_wait(barrier, len(peers) + 1)

    sent = []

    def send(src, dst, device):
        k = len(sent)
        copy = pltpu.make_async_remote_copy(
            src_ref=src, dst_ref=dst, send_sem=send_sems.at[k], recv_sem=recv_sems.at[k],
            device_id=device, device_id_type=pl.DeviceIdType.MESH)
        copy.start()
        sent.append(copy)
        return copy

    flying = {}

    def start(n, s):
        order, _ = items[n]
        half = 2 ** (n_bits - s - 1)
        device = {"dp": flipped((order[s],))}
        if s == 0:
            flying[n] = [
                send(ins[n][0].at[natural_index(me, j, ((order[0], True),), order[1:])], recvs[n][0].at[j], device)
                for j in range(half)
            ]
        else:
            away = (1 - bit_of(me, order[s])) * half
            flying[n] = [send(curs[n][s].at[pl.ds(away, half)], recvs[n][s], device)]

    def finish(n, s):
        order, _ = items[n]
        half = 2 ** (n_bits - s - 1)
        for copy in flying.pop(n):
            copy.wait_recv()
        got = recvs[n][s]
        held = curs[n][s] if s else ins[n][0]

        def total_at(j):
            if s:
                index = bit_of(me, order[s]) * half + j
            else:
                index = natural_index(me, j, ((order[0], False),), order[1:])
            return held[index].astype(F32) + got[j].astype(F32)

        if s == n_bits - 1:
            outs[n][...] = total_at(0)
            return

        def body(j, carry):
            curs[n][s + 1][j] = total_at(j).astype(BF)
            return carry

        lax.fori_loop(0, half, body, 0)
        start(n, s + 1)

    other_core = {"tensor": 1 - core}
    own, depth = near[0].shape
    sources = list(far)
    sources[0] = far[0].at[0, pl.ds(pl.multiple_of(core * own, own), own), :]
    buf = dict(zip(NAMES, near))
    fetch = {name: pltpu.make_async_copy(s, d, local_sems.at[k])
             for k, (name, s, d) in enumerate(zip(NAMES, sources, near))}
    first_use = ("k", "v")
    by_rows = ("q_o", "ga_o", "cos", "sin", "ql_o", "q_x", "ga_x", "ql_x")

    def fetch_rows(name, i):
        k = NAMES.index(name)
        at = pl.ds(pl.multiple_of(i * QB, QB), QB)
        return pltpu.make_async_copy(far[k].at[at, :], near[k].at[at, :], part_sems.at[by_rows.index(name), i])

    second_use = ("nb", "kl", "wk", "wv", "wq_o", "wq_x", "x", "gmid")
    for name in first_use:
        fetch[name].start()
    for i in range(own // QB):
        for name in by_rows:
            fetch_rows(name, i).start()
    for n in range(n_items):
        if items[n][1]:
            start(n, 0)
    for name in second_use:
        fetch[name].start()
    dk_all[...] = jnp.zeros_like(dk_all)
    dv_all[...] = jnp.zeros_like(dv_all)
    g_q[...] = jnp.zeros_like(g_q)
    gq_row = rows8[4:5, :HEAD_WIDTH]
    for name in first_use:
        fetch[name].wait()

    def attn_body(i, carry):
        for name in by_rows:
            fetch_rows(name, i).wait()
        attn_rows(i, seg, buf, lse, delta, gq_row, qr_o, qr_x, dk_all, dv_all, g_q)
        return carry

    lax.fori_loop(0, own // QB, attn_body, 0)
    front[:, :HEAD_WIDTH] = dk_all[:BLOCK, :].astype(BF)
    front[:, HEAD_WIDTH:] = dv_all[:BLOCK, :].astype(BF)
    front_copy = send(front, front_got, other_core)
    fetch["nb"].wait()
    query_sent[...] = tn(qr_x[...], buf["nb"][...]).astype(BF)
    query_copy = send(query_sent, query_got, other_core)
    fetch["kl"].wait()
    front_copy.wait_recv()
    gk_row, gin_row = rows8[5:6, :HEAD_WIDTH], rows8[0:1, :]
    g_k[...] = jnp.zeros_like(g_k)
    g_in[...] = jnp.zeros_like(g_in)
    blocks = own // BLOCK

    def kv_rows(i, carry):
        at = pl.ds(pl.multiple_of(i * BLOCK, BLOCK), BLOCK)
        tail = ((i == blocks - 1) & (core == 0)).astype(F32)
        later = pl.ds(pl.multiple_of((i + 1) * BLOCK, BLOCK), BLOCK)
        dk = dk_all[later, :] + tail * front_got[:, :HEAD_WIDTH].astype(F32)
        dv = dv_all[later, :] + tail * front_got[:, HEAD_WIDTH:].astype(F32)
        dkn = rotate(dk, buf["cos"][at, :], buf["sin"][at, :], -1)
        k_hat, k_inv = rms_stats(buf["kl"][at, :])
        kraw[at, :] = rms_back(k_hat, k_inv, gk_row, dkn).astype(BF)
        vraw[at, :] = dv.astype(BF)
        g_k[...] += jnp.sum(dkn * k_hat, axis=0, keepdims=True)
        return carry

    lax.fori_loop(0, blocks, kv_rows, 0)
    n_chunk, rows_k = kv_in.shape[1:3]
    for t, raw in enumerate((kraw, vraw)):
        kv_in[t] = tn(raw[...], buf["nb"][...]).astype(BF).reshape(n_chunk, rows_k, depth)
    kv_copies = [send(kv_in.at[1 - core], kv_core, other_core)]
    query_copy.wait_recv()
    own_query = tn(qr_o[...], buf["nb"][...]) + query_got[...].astype(F32)
    query[...] = own_query.astype(BF).reshape(query.shape)
    start(n_items - 1, 0)
    kv_copies[0].wait_recv()

    def kv_first(j, carry):
        index = natural_index(me, j, (), kv_order)
        kv_cur[0][j] = (kv_in[core, index].astype(F32) + kv_core[index].astype(F32)).astype(BF)
        return carry

    lax.fori_loop(0, 2**n_bits, kv_first, 0)

    def rest_of(g):
        return 2 ** (n_bits - sum(len(x) for x in kv_groups[: g + 1]))

    def block_index(group, bits):
        index = 0
        for k, b in enumerate(group):
            mine = bit_of(me, b)
            index = index + (1 - mine if b in bits else mine) * 2 ** (len(group) - 1 - k)
        return index

    def kv_start(g):
        rest = rest_of(g)
        return [send(kv_cur[g].at[pl.ds(block_index(kv_groups[g], m) * rest, rest)], kv_recv[g].at[c],
                     {"dp": flipped(m)}) for c, m in enumerate(subsets(kv_groups[g]))]

    spot = 0
    for k, b in enumerate(kv_order):
        spot = spot + bit_of(me, b) * 2 ** (n_bits - 1 - k)
    kv_copies = kv_start(0)
    for n in range(n_items):
        if items[n][1]:
            finish(n, 0)
    for name in ("wk", "wv", "wq_o", "wq_x", "x", "gmid"):
        fetch[name].wait()

    def input_rows(i, carry):
        at = pl.ds(pl.multiple_of(i * QB, QB), QB)
        gn = nt(kraw[at, :], buf["wk"][...]) + nt(vraw[at, :], buf["wv"][...])
        gn = gn + nt(qr_o[at, :], buf["wq_o"][...]) + nt(qr_x[at, :], buf["wq_x"][...])
        hat, inv = rms_stats(buf["x"][at, :])
        buf["x"][at, :] = buf["gmid"][at, :] + rms_back(hat, inv, gin_row, gn)
        g_in[...] += jnp.sum(gn * hat, axis=0, keepdims=True)
        return carry

    gain_copies = []

    def gain_start(s):
        if s == 0:
            gain_copies.append([send(gain_own[0], gain_got[0].at[0], other_core)])
        else:
            gain_copies.append([send(gain_own[s], gain_got[s].at[c], {"dp": flipped(m)})
                                for c, m in enumerate(subsets(kv_groups[s - 1]))])

    def gain_step():
        s = len(gain_copies) - 1
        total = gain_own[s][...]
        for c, copy in enumerate(gain_copies[s]):
            copy.wait_recv()
            total = total + gain_got[s][c]
        if s == len(kv_groups):
            gain_out[...] = total
            return True
        gain_own[s + 1][...] = total
        gain_start(s + 1)
        return False

    half_rows = own // QB // 2

    def fill_first():
        lax.fori_loop(0, half_rows, input_rows, 0)

    def fill_second():
        lax.fori_loop(half_rows, own // QB, input_rows, 0)
        gain_own[0][...] = jnp.zeros_like(gain_own[0])
        gain_own[0][0:3, :] = g_block[0:3, :]
        gain_own[0][3:4, :] = g_in[...]
        gain_own[0][4:5, :HEAD_WIDTH] = g_q[...]
        gain_own[0][5:6, :HEAD_WIDTH] = g_k[...]
        gain_start(0)

    gin_copy = pltpu.make_async_copy(buf["x"], gin_far, local_sems.at[len(NAMES)])
    fills = [fill_first, fill_second, gin_copy.start]
    rank = lambda e: e[1] - (1 if items[e[0]][1] else 0)
    todo = [(n, s) for s in range(n_bits) for n in range(n_items) if s or not items[n][1]]
    todo.sort(key=rank)

    def advance():
        now = rank(todo[0]) if todo else 0
        while todo and rank(todo[0]) == now:
            finish(*todo.pop(0))

    for g in range(len(kv_groups)):
        rest = rest_of(g)
        for copy in kv_copies:
            copy.wait_recv()
        base = block_index(kv_groups[g], ()) * rest

        def kv_total(j, g=g, base=base):
            total = kv_cur[g][base + j].astype(F32)
            for c in range(2 ** len(kv_groups[g]) - 1):
                total = total + kv_recv[g][c, j].astype(F32)
            return total.astype(BF)

        if g < len(kv_groups) - 1:

            def kv_body(j, carry, g=g, kv_total=kv_total):
                kv_cur[g + 1][j] = kv_total(j)
                return carry

            lax.fori_loop(0, rest, kv_body, 0)
            kv_copies = kv_start(g + 1)
            if len(fills) > 2:
                fills.pop(0)()
            advance()
        else:
            kv_all[core, spot] = kv_total(0)
    gains_done = False
    for g in reversed(range(len(kv_groups))):
        size = rest_of(g)
        begin = 0
        for k, b in enumerate(sum(kv_groups[: g + 1], ())):
            begin = begin + bit_of(me, b) * 2 ** (n_bits - 1 - k)
        region = kv_all.at[core, pl.ds(begin, size)]
        copies = [send(region, region, {"dp": flipped(m)}) for m in subsets(kv_groups[g])]
        while len(fills) > 1:
            fills.pop(0)()
        if fills:
            fills.pop(0)()
        elif not gains_done:
            gains_done = gain_step()
        advance()
        for copy in copies:
            copy.wait_recv()
    copy = send(kv_all.at[core], kv_all.at[core], other_core)
    while todo:
        advance()
    while not gains_done:
        gains_done = gain_step()
    copy.wait_recv()

    def unpack(j, carry):
        index = natural_index(me, j, (), kv_order)
        for t in range(2):
            kv_wide[t, index] = kv_all[t, j].astype(F32)
        return carry

    lax.fori_loop(0, 2**n_bits, unpack, 0)
    for t, out in enumerate((k_out, v_out)):
        out[...] = jnp.transpose(kv_wide[t].reshape(HEAD_WIDTH, depth))
    gin_copy.wait()
    for copy in sent:
        copy.wait_send()


def finish_all(n_dp, items, order, kv_order, small, far):
    n_bits = len(kv_order)
    own, part = far[12].shape
    ext = far[10].shape[0]
    depth = far[1].shape[1]
    groups = tuple(tuple(kv_order[k : k + 2]) for k in range(0, n_bits, 2))
    spec, operands, outs, comm = [], [], [], []
    copies = 3
    shapes = [value.shape for value, _ in items] + [(n_dp, part // n_dp, depth)]
    for k, (n, c, width) in enumerate(shapes):
        early = k < len(items)
        spec.append((tuple(items[k][1] if early else order), early))
        if early:
            operands.append(items[k][0])
        outs.append(sds((c, width), F32))
        comm += [pltpu.VMEM((2 ** (n_bits - s - 1), c, width), BF) for s in range(n_bits)]
        comm += [pltpu.VMEM((2 ** (n_bits - s), c, width), BF) for s in range(1, n_bits)]
        copies += n_bits - 1 + n // 2
    n, c, width = n_dp, HEAD_WIDTH // n_dp, depth
    comm += [pltpu.VMEM((n, c, width), BF)]
    sizes = [2 ** (n_bits - sum(len(x) for x in groups[:g])) for g in range(len(groups) + 1)]
    comm += [pltpu.VMEM((2 ** len(groups[g]) - 1, sizes[g + 1], c, width), BF) for g in range(len(groups))]
    comm += [pltpu.VMEM((sizes[g], c, width), BF) for g in range(len(groups))]
    comm += [pltpu.VMEM((2, n, c, width), BF)]
    comm += [pltpu.VMEM((2, n, c, width), F32)]
    comm += [pltpu.VMEM((8, width), F32) for _ in range(len(groups) + 1)]
    comm += [pltpu.VMEM((1, 8, width), F32)] + [pltpu.VMEM((2 ** len(g) - 1, 8, width), F32) for g in groups]
    copies += 3 + 3 * sum(2 ** len(g) - 1 for g in groups)
    comm += [pltpu.SemaphoreType.DMA((copies,)), pltpu.SemaphoreType.DMA((copies,))]
    outs += [sds((width, HEAD_WIDTH), F32), sds((width, HEAD_WIDTH), F32), sds((8, width), F32), sds((own, depth), F32)]
    near = [pltpu.VMEM((own, depth), F32)] + [pltpu.VMEM(a.shape, a.dtype) for a in far[1:]]
    scratch = near + [
        pltpu.SemaphoreType.DMA((len(far) + 1,)), pltpu.SemaphoreType.DMA((8, own // QB)),
        pltpu.VMEM((BLOCK, 2 * HEAD_WIDTH), BF), pltpu.VMEM((BLOCK, 2 * HEAD_WIDTH), BF),
        pltpu.VMEM((ext, HEAD_WIDTH), F32), pltpu.VMEM((ext, HEAD_WIDTH), F32),
        pltpu.VMEM((own, part), BF), pltpu.VMEM((own, part), BF),
        pltpu.VMEM((own, HEAD_WIDTH), BF), pltpu.VMEM((own, HEAD_WIDTH), BF),
        pltpu.VMEM((2, n, c, width), BF), pltpu.VMEM((part, depth), BF), pltpu.VMEM((part, depth), BF),
        pltpu.VMEM((n_dp, part // n_dp, depth), BF), pltpu.VMEM((1, depth), F32),
        pltpu.VMEM((1, HEAD_WIDTH), F32), pltpu.VMEM((1, HEAD_WIDTH), F32),
    ] + comm
    vmem = pl.BlockSpec(memory_space=pltpu.VMEM)
    anywhere = pl.BlockSpec(memory_space=pl.ANY)
    operands += list(small)
    return pl.pallas_call(
        functools.partial(finish_kernel, tuple(spec), groups, n_bits),
        out_shape=outs,
        in_specs=[vmem] * len(operands) + [anywhere] * len(far),
        out_specs=[vmem] * (len(outs) - 1) + [anywhere],
        scratch_shapes=scratch,
        compiler_params=pltpu.CompilerParams(collective_id=0, has_side_effects=True, vmem_limit_bytes=VMEM_LIMIT),
        name="finish_all",
    )(*operands, *far)


def after(value, *others):
    return lax.optimization_barrier((value,) + others)[0]


def on_device(n_dp, n_tensor, residual_in, cotangent, segment_ids, gain_attn_in, w_query, w_key, w_value,
              gain_query, gain_key, w_out, gain_attn_out, gain_ff_in, w_gate, w_up, w_down, gain_ff_out):
    tokens, depth = residual_in.shape[1:]
    own = tokens // n_tensor
    me = lax.axis_index("tensor")
    first_row = (me * own).astype(jnp.int32).reshape(1)
    wq_x = swap(w_query, n_tensor)
    *later, wq_x = lax.optimization_barrier((w_out, w_gate, w_up, w_down, wq_x))
    wo_x, wg_x, wu_x, wd_x = (swap(w, n_tensor) for w in later)
    table = jnp.asarray(rope_table())
    gain_list = (gain_attn_in, gain_attn_out, gain_ff_in, gain_ff_out, gain_query, gain_key)
    q_o, q_x, ql_o, ql_x, k, v, kl, nb, cos, sin, seg_ext, rows8 = project(
        first_row, own, residual_in, segment_ids, table, gain_list, w_query, wq_x, w_key, w_value)
    weights = (w_out, wo_x, w_gate, wg_x, w_up, wu_x, w_down, wd_x)
    (output, gmid, ga_o, ga_x, af_o, af_x, lse, delta, mid_b, gff, gas,
     act_o, act_x, gg_o, gg_x, gu_o, gu_x, gains) = block_pass(
        first_row, residual_in, cotangent, seg_ext, q_o, q_x, k, v, weights, rows8)

    n_bits = n_dp.bit_length() - 1
    plain, turned, lead = bit_orders(n_bits)
    chunks = lambda value: value.reshape(n_dp, value.shape[0] // n_dp, value.shape[1])

    pairs = [(gff, act_x, act_o, plain), (mid_b, gg_x, gg_o, turned), (mid_b, gu_x, gu_o, lead), (gas, af_x, af_o, plain)]
    grad = lambda left, units: tn(left, units) if left is not mid_b else tn(units, left)
    gots = []
    last = ()
    for left, units, _, _ in pairs:
        sent = grad(left, after(units, *last)).astype(BF)
        last = (sent,)
        gots.append(swap(sent, n_tensor))
    items = []
    for (left, _, units, order), got in zip(pairs, gots):
        value = chunks((grad(left, after(units, *last)) + got.astype(F32)).astype(BF))
        last = (value,)
        items.append((value, order))
    far = (residual_in, gmid, w_query, wq_x, w_key, w_value, kl, cos, sin, nb, k, v, q_o, q_x, ga_o, ga_x, ql_o, ql_x)
    *shares, k_sum, v_sum, gain_sum, grad_input = finish_all(
        n_dp, items, plain, plain, (seg_ext, lse, delta, rows8, gains), far)
    s_down, s_gate, s_up, s_out, s_query = shares
    return (
        output[None], grad_input[None], gain_sum[3], s_query.T, k_sum, v_sum,
        gain_sum[4, :HEAD_WIDTH], gain_sum[5, :HEAD_WIDTH],
        s_out.T, gain_sum[2], gain_sum[1], s_gate.T, s_up.T, s_down.T, gain_sum[0],
    )


def solution(mesh):
    n_dp, n_tensor = mesh.shape["dp"], mesh.shape["tensor"]
    return jax.shard_map(
        functools.partial(on_device, n_dp, n_tensor),
        mesh=mesh,
        in_specs=(
            P("dp", None, None), P("dp", None, None), P("dp", None), P(), P(None, "tensor"), P(), P(), P(), P(),
            P("tensor", None), P(), P(), P(None, "tensor"), P(None, "tensor"), P("tensor", None), P(),
        ),
        out_specs=(
            P("dp", "tensor", None), P("dp", "tensor", None), P(), P(None, ("tensor", "dp")), P(), P(), P(), P(),
            P("tensor", "dp"), P(), P(), P(None, ("tensor", "dp")), P(None, ("tensor", "dp")), P("tensor", "dp"),
            P(),
        ),
        check_vma=False,
    )
```

```python
import functools
import jax
import jax.numpy as jnp
import numpy as np
from jax import lax
from jax.experimental import pallas as pl
from jax.experimental.pallas import tpu as pltpu
from jax.sharding import PartitionSpec as P

HEAD_WIDTH = 256
BLOCK = 512
EPS = 1e-06
THETA = 1000000.0
SCORE_SCALE = 0.0625
GELU_C = 0.7978845608028654
GELU_A = 0.044715
HALF = HEAD_WIDTH // 2
QB = 256
WIN = BLOCK + QB
LANES = 128
BF = jnp.bfloat16
F32 = jnp.float32
VMEM_LIMIT = 60 << 20


def nn(a, b):
    return lax.dot_general(a, b, (((1,), (0,)), ((), ())), preferred_element_type=F32)


def nt(a, b):
    return lax.dot_general(a, b, (((1,), (1,)), ((), ())), preferred_element_type=F32)


def tn(a, b):
    return lax.dot_general(a, b, (((0,), (0,)), ((), ())), preferred_element_type=F32)


def rms_stats(v):
    inv = lax.rsqrt(jnp.mean(v * v, axis=-1, keepdims=True) + EPS)
    return v * inv, inv


def rms_back(hat, inv, gain, up):
    scaled = up * gain
    return inv * (scaled - hat * jnp.mean(scaled * hat, axis=-1, keepdims=True))


def rotate(v, cos, sin, direction):
    a, b = v[:, :HALF], v[:, HALF:]
    if direction > 0:
        return jnp.concatenate([a * cos - b * sin, b * cos + a * sin], axis=-1)
    return jnp.concatenate([a * cos + b * sin, b * cos - a * sin], axis=-1)


def column_of(row):
    n = row.shape[1]
    return jnp.transpose(jnp.broadcast_to(row, (LANES, n)))


def rope_table():
    freq = np.arange(HALF, dtype=np.float32)
    inv_freq = np.exp(freq * np.float32(-2.0 * np.log(THETA) / HEAD_WIDTH)).astype(np.float32)
    angles = np.arange(BLOCK, dtype=np.float32)[:, None] * inv_freq[None, :]
    parts = []
    for tab in (np.cos(angles.astype(np.float64)), np.sin(angles.astype(np.float64))):
        tab = tab.astype(np.float32)
        hi = tab.astype(BF)
        lo = (tab - hi.astype(np.float32)).astype(BF)
        parts += [hi, lo]
    return np.concatenate(parts, axis=1)


def project_kernel(me, x, seg, table, g1, g2, g3, g4, g5, g6, wq_o, wq_x, wk, wv,
                   q_o, q_x, ql_o, ql_x, k_out, v_out, kl_out, nb_out, cos_out, sin_out, seg_out, rows8):
    i = pl.program_id(0)
    rows = x.shape[1]

    @pl.when(i == 0)
    def _():
        rows8[...] = jnp.zeros_like(rows8)
        for r, g in enumerate((g1, g2, g3, g4, g5, g6)):
            rows8[r : r + 1, : g.shape[0]] = g[...].reshape(1, g.shape[0])

    g_in, gq, gk = gain_refs(rows8, 0, 4, 5)
    hat, _ = rms_stats(x[0])
    nb = (hat * g_in[...]).astype(BF)
    nb_out[...] = nb
    base = me[0] + (i - 1) * rows
    seg_row = seg[:, pl.ds(pl.multiple_of(jnp.maximum(base, 0), rows), rows)]
    seg_row = jnp.where(base < 0, -1, seg_row)
    seg_out[...] = seg_row
    before = (seg[...] < column_of(seg_row)[:, :1]).astype(F32)
    start = jnp.sum(before, axis=1, keepdims=True)
    pos = lax.broadcasted_iota(jnp.int32, (rows, 1), 0) + base - start.astype(jnp.int32)
    hot = (lax.broadcasted_iota(jnp.int32, (rows, BLOCK), 1) == pos).astype(F32).astype(BF)
    cs = nn(hot, table[...])
    cos = cs[:, :LANES] + cs[:, LANES : 2 * LANES]
    sin = cs[:, 2 * LANES : 3 * LANES] + cs[:, 3 * LANES :]
    cos_out[...] = cos
    sin_out[...] = sin
    k_lin = nn(nb, wk[...])
    kl_out[...] = k_lin
    k_hat, _ = rms_stats(k_lin)
    k_out[...] = rotate(k_hat * gk[...], cos, sin, 1).astype(BF)
    v_out[...] = nn(nb, wv[...]).astype(BF)

    @pl.when(i > 0)
    def _():
        for w, lin_out, out in ((wq_o, ql_o, q_o), (wq_x, ql_x, q_x)):
            lin = nn(nb, w[...])
            lin_out[...] = lin
            for h in range(lin.shape[1] // HEAD_WIDTH):
                cols = slice(h * HEAD_WIDTH, (h + 1) * HEAD_WIDTH)
                q_hat, _ = rms_stats(lin[:, cols])
                out[:, cols] = (rotate(q_hat * gq[...], cos, sin, 1) * SCORE_SCALE).astype(BF)


def gain_refs(rows8, *which):
    width = rows8.shape[1]
    return [rows8.at[r : r + 1, : (width if r < 4 else HEAD_WIDTH)] for r in which]


def score_mask(seg_q, seg_k, rows, width):
    lane = lax.broadcasted_iota(jnp.int32, (rows, width), 1)
    sub = lax.broadcasted_iota(jnp.int32, (rows, width), 0)
    return (seg_q == seg_k) & (lane <= sub + (width - rows))


def block_kernel(x, up, seg, q_o, q_x, k, v, wo_o, wo_x, wg_o, wg_x, wu_o, wu_x, wd_o, wd_x,
                 rows8,
                 out, gmid_out, ga_o, ga_x, af_o, af_x, lse_out, delta_out, mid_out, gff_out, gas_out,
                 act_o, act_x, gg_o, gg_x, gu_o, gu_x, gains,
                 mix, gate_s, up_s):
    g_ao, g_fi, g_fo = gain_refs(rows8, 1, 2, 3)
    i = pl.program_id(0)
    rows = x.shape[1]
    base = pl.multiple_of(i * rows, rows)
    k_win = k[pl.ds(base, WIN), :]
    v_win = v[pl.ds(base, WIN), :]
    seg_k = seg[:, pl.ds(base, WIN)]
    seg_q = column_of(seg[:, pl.ds(base + BLOCK, rows)])[:, :1]
    mask = score_mask(seg_q, seg_k, rows, WIN)
    heads_per = q_o.shape[1] // HEAD_WIDTH
    lses = []
    for part, (q, af) in enumerate(((q_o, af_o), (q_x, af_x))):
        for h in range(heads_per):
            cols = slice(h * HEAD_WIDTH, (h + 1) * HEAD_WIDTH)
            s = jnp.where(mask, nt(q[:, cols], k_win), -jnp.inf)
            top = jnp.max(s, axis=-1, keepdims=True)
            e = jnp.exp(s - top)
            mass = jnp.sum(e, axis=-1, keepdims=True)
            lses.append(top + jnp.log(mass))
            p = (e * (1.0 / mass)).astype(BF)
            m = nn(p, v_win)
            mix[part * heads_per + h] = m
            af[:, cols] = m.astype(BF)
    inputs = x[0]
    upstream = up[0]
    attn_sum = nn(af_o[...], wo_o[...]) + nn(af_x[...], wo_x[...])
    hat_attn, inv_attn = rms_stats(attn_sum)
    middle = inputs + hat_attn * g_ao[...]
    hat_mid, inv_mid = rms_stats(middle)
    mid_b = (hat_mid * g_fi[...]).astype(BF)
    mid_out[...] = mid_b
    ff_sum = None
    for part, (wg, wu, wd, act) in enumerate(((wg_o, wu_o, wd_o, act_o), (wg_x, wu_x, wd_x, act_x))):
        gate = nn(mid_b, wg[...])
        upp = nn(mid_b, wu[...])
        sq = gate * gate
        th = jnp.tanh(gate * (GELU_C + (GELU_C * GELU_A) * sq))
        onep = 0.5 + 0.5 * th
        gelu = gate * onep
        deriv = onep + gate * (1.0 - th * th) * (0.5 * GELU_C + (1.5 * GELU_C * GELU_A) * sq)
        gate_s[part] = gelu
        up_s[part] = upp * deriv
        a = (gelu * upp).astype(BF)
        act[...] = a
        f = nn(a, wd[...])
        ff_sum = f if ff_sum is None else ff_sum + f
    hat_ff, inv_ff = rms_stats(ff_sum)
    out[...] = middle + hat_ff * g_fo[...]
    gff = rms_back(hat_ff, inv_ff, g_fo[...], upstream).astype(BF)
    gff_out[...] = gff
    gmn = None
    for part, (wg, wu, wd, gg_out, gu_out) in enumerate(
        ((wg_o, wu_o, wd_o, gg_o, gu_o), (wg_x, wu_x, wd_x, gg_x, gu_x))
    ):
        gact = nt(gff, wd[...])
        gg = (gact * up_s[part]).astype(BF)
        gu = (gact * gate_s[part]).astype(BF)
        gg_out[...] = gg
        gu_out[...] = gu
        t = nt(gg, wg[...]) + nt(gu, wu[...])
        gmn = t if gmn is None else gmn + t
    gmid = upstream + rms_back(hat_mid, inv_mid, g_fi[...], gmn)
    gmid_out[...] = gmid
    gas = rms_back(hat_attn, inv_attn, g_ao[...], gmid).astype(BF)
    gas_out[...] = gas
    deltas = []
    for part, (wo, ga) in enumerate(((wo_o, ga_o), (wo_x, ga_x))):
        g = nt(gas, wo[...]).astype(BF)
        ga[...] = g
        for h in range(heads_per):
            gh = g[:, h * HEAD_WIDTH : (h + 1) * HEAD_WIDTH].astype(F32)
            deltas.append(jnp.sum(gh * mix[part * heads_per + h], axis=-1, keepdims=True))
    lane = lax.broadcasted_iota(jnp.int32, (rows, LANES), 1)
    lse_all = jnp.zeros((rows, LANES), F32)
    delta_all = jnp.zeros((rows, LANES), F32)
    for n, (a, b) in enumerate(zip(lses, deltas)):
        lse_all = jnp.where(lane == n, a, lse_all)
        delta_all = jnp.where(lane == n, b, delta_all)
    lse_out[...] = jnp.transpose(lse_all)[:8]
    delta_out[...] = jnp.transpose(delta_all)[:8]

    @pl.when(i == 0)
    def _():
        gains[...] = jnp.zeros_like(gains)

    gains[0:1, :] += jnp.sum(upstream * hat_ff, axis=0, keepdims=True)
    gains[1:2, :] += jnp.sum(gmn * hat_mid, axis=0, keepdims=True)
    gains[2:3, :] += jnp.sum(gmid * hat_attn, axis=0, keepdims=True)


def attn_rows(i, seg, buf, lse, delta, gq, qr_o, qr_x, dk, dv, gain):
    rows = QB
    base = pl.multiple_of(i * rows, rows)
    mine = pl.ds(base, rows)
    k_win = buf["k"][pl.ds(base, WIN), :]
    v_win = buf["v"][pl.ds(base, WIN), :]
    seg_k = column_of(seg[:, pl.ds(base, WIN)])[:, :1]
    seg_q = seg[:, pl.ds(base + BLOCK, rows)]
    lane = lax.broadcasted_iota(jnp.int32, (WIN, rows), 1)
    sub = lax.broadcasted_iota(jnp.int32, (WIN, rows), 0)
    mask = (seg_q == seg_k) & (sub <= lane + (WIN - rows))
    cos = buf["cos"][mine, :]
    sin = buf["sin"][mine, :]
    dk_sum = None
    dv_sum = None
    g_sum = None
    heads = qr_o.shape[1] // HEAD_WIDTH
    for n in range(2 * heads):
        side = "ox"[n // heads]
        qraw = (qr_o, qr_x)[n // heads]
        h = n % heads
        cols = slice(h * HEAD_WIDTH, (h + 1) * HEAD_WIDTH)
        qh = buf["q_" + side][mine, cols]
        gh = buf["ga_" + side][mine, cols]
        s = jnp.where(mask, nt(k_win, qh), -jnp.inf)
        p = jnp.exp(s - lse[n : n + 1, mine])
        ds = (p * (nt(v_win, gh) - delta[n : n + 1, mine])).astype(BF)
        dq = tn(ds, k_win) * SCORE_SCALE
        a = nn(ds, qh)
        b = nn(p.astype(BF), gh)
        dk_sum = a if dk_sum is None else dk_sum + a
        dv_sum = b if dv_sum is None else dv_sum + b
        dqn = rotate(dq, cos, sin, -1)
        hat, inv = rms_stats(buf["ql_" + side][mine, cols])
        g = jnp.sum(dqn * hat, axis=0, keepdims=True)
        g_sum = g if g_sum is None else g_sum + g
        qraw[mine, cols] = rms_back(hat, inv, gq, dqn).astype(BF)
    dk[pl.ds(base, WIN), :] += dk_sum
    dv[pl.ds(base, WIN), :] += dv_sum
    gain[...] += g_sum


def whole(shape):
    return pl.BlockSpec(shape, lambda *_: (0,) * len(shape), pipeline_mode=pl.Buffered(1))


def rows_of(n, width, shift=0):
    if shift:
        return pl.BlockSpec((n, width), lambda i, *_: (jnp.maximum(i - shift, 0), 0))
    return pl.BlockSpec((n, width), lambda i, *_: (i, 0))


def params():
    return pltpu.CompilerParams(dimension_semantics=("arbitrary",), vmem_limit_bytes=VMEM_LIMIT)


def cost(us):
    return pl.CostEstimate(flops=us * 10**9, bytes_accessed=us * 10**6, transcendentals=0)


def sds(shape, dtype):
    return jax.ShapeDtypeStruct(shape, dtype)


def project(first_row, own, x3, seg, table, gain_list, wq_o, wq_x, wk, wv):
    depth = x3.shape[2]
    ext = own + BLOCK
    part = wq_o.shape[1]
    n = BLOCK
    me_block = lambda i, me: (0, jnp.maximum(me[0] // n + i - 1, 0), 0)
    return pl.pallas_call(
        project_kernel,
        grid_spec=pltpu.PrefetchScalarGridSpec(
            num_scalar_prefetch=1,
            grid=(ext // n,),
            in_specs=[
                pl.BlockSpec((1, n, depth), me_block),
                whole(seg.shape),
                whole(table.shape),
                *[whole(g.shape) for g in gain_list],
                whole(wq_o.shape), whole(wq_x.shape), whole(wk.shape), whole(wv.shape),
            ],
            out_specs=[
                rows_of(n, part, 1), rows_of(n, part, 1), rows_of(n, part, 1), rows_of(n, part, 1),
                rows_of(n, HEAD_WIDTH), rows_of(n, HEAD_WIDTH), rows_of(n, HEAD_WIDTH, 1),
                rows_of(n, depth, 1), rows_of(n, LANES, 1), rows_of(n, LANES, 1),
                pl.BlockSpec((1, n), lambda i, *_: (0, i)), pl.BlockSpec((8, depth), lambda i, *_: (0, 0)),
            ],
        ),
        out_shape=[
            sds((own, part), BF), sds((own, part), BF), sds((own, part), F32), sds((own, part), F32),
            sds((ext, HEAD_WIDTH), BF), sds((ext, HEAD_WIDTH), BF), sds((own, HEAD_WIDTH), F32),
            sds((own, depth), BF), sds((own, LANES), F32), sds((own, LANES), F32),
            sds((1, ext), jnp.int32), sds((8, depth), F32),
        ],
        compiler_params=params(),
        cost_estimate=cost(6),
        name="project",
    )(first_row, x3, seg, table, *gain_list, wq_o, wq_x, wk, wv)


def block_pass(first_row, x3, up3, seg_ext, q_o, q_x, k, v, weights, rows8):
    depth = x3.shape[2]
    own, part = q_o.shape
    n = QB
    hidden = weights[2].shape[1]
    mine = pl.BlockSpec((1, n, depth), lambda i, me: (0, me[0] // n + i, 0))
    kern = lambda me, *refs: block_kernel(*refs)
    heads = 2 * part // HEAD_WIDTH
    return pl.pallas_call(
        kern,
        grid_spec=pltpu.PrefetchScalarGridSpec(
            num_scalar_prefetch=1,
            grid=(own // n,),
            in_specs=[mine, mine, whole(seg_ext.shape), rows_of(n, part), rows_of(n, part),
                      whole(k.shape), whole(v.shape)]
            + [whole(w.shape) for w in weights]
            + [whole(rows8.shape)],
            out_specs=[rows_of(n, depth)] * 2 + [rows_of(n, part)] * 4 + [pl.BlockSpec((8, n), lambda i, *_: (0, i))] * 2
            + [rows_of(n, depth)] * 3 + [rows_of(n, hidden)] * 6
            + [pl.BlockSpec((8, depth), lambda i, *_: (0, 0))],
            scratch_shapes=[
                pltpu.VMEM((heads, n, HEAD_WIDTH), F32),
                pltpu.VMEM((2, n, hidden), F32),
                pltpu.VMEM((2, n, hidden), F32),
            ],
        ),
        out_shape=[sds((own, depth), F32)] * 2 + [sds((own, part), BF)] * 4 + [sds((8, own), F32)] * 2
        + [sds((own, depth), BF)] * 3 + [sds((own, hidden), BF)] * 6 + [sds((8, depth), F32)],
        compiler_params=pltpu.CompilerParams(
            dimension_semantics=("arbitrary",), vmem_limit_bytes=VMEM_LIMIT),
        cost_estimate=cost(40),
        name="block",
    )(first_row, x3, up3, seg_ext, q_o, q_x, k, v, *weights, rows8)


def swap(value, n_tensor):
    return lax.ppermute(value, "tensor", [(t, n_tensor - 1 - t) for t in range(n_tensor)])


def bit_of(index, b):
    return lax.rem(lax.div(index, 2**b), 2)


def bit_orders(n_bits):
    plain = tuple(range(n_bits))
    turned = plain[1:] + plain[:1]
    lead = (plain[2],) + plain[:2] + plain[3:] if n_bits > 2 else plain[::-1]
    return plain, turned, lead


def natural_index(me, j, fixed, free):
    index = 0
    for b, flip in fixed:
        mine = bit_of(me, b)
        index = index + (1 - mine if flip else mine) * 2**b
    for k, b in enumerate(free):
        index = index + lax.rem(lax.div(j, 2 ** (len(free) - 1 - k)), 2) * 2**b
    return index


NAMES = ("x", "gmid", "wq_o", "wq_x", "wk", "wv", "kl", "cos", "sin", "nb", "k", "v", "q_o", "q_x", "ga_o", "ga_x",
         "ql_o", "ql_x")


def finish_kernel(items, kv_groups, n_bits, *refs):
    n_items = len(items)
    kv_order = sum(kv_groups, ())
    refs = list(refs)
    take = lambda count: [refs.pop(0) for _ in range(count)]
    ins = [take(1) for _, early in items if early]
    seg, lse, delta, rows8, g_block = take(5)
    far = take(len(NAMES))
    outs = take(n_items)
    k_out, v_out, gain_out, gin_far = take(4)
    near = take(len(NAMES))
    local_sems, part_sems = take(2)
    (front, front_got, dk_all, dv_all, qr_o, qr_x, kraw, vraw, kv_in, query_sent, query_got, query,
     g_in, g_k, g_q) = take(15)
    ins.append([query])
    recvs, curs = [], []
    for _ in items:
        recvs.append({s: refs.pop(0) for s in range(n_bits)})
        curs.append({s: refs.pop(0) for s in range(1, n_bits)})
    kv_core = refs.pop(0)
    kv_recv = take(len(kv_groups))
    kv_cur = take(len(kv_groups))
    kv_all = refs.pop(0)
    kv_wide = refs.pop(0)
    gain_own = take(len(kv_groups) + 1)
    gain_got = take(len(kv_groups) + 1)
    send_sems, recv_sems = take(2)

    me = lax.axis_index("dp")
    core = lax.axis_index("tensor")

    def flipped(bits):
        return me + sum((1 - 2 * bit_of(me, b)) * 2**b for b in bits)

    def subsets(group):
        return [tuple(b for k, b in enumerate(group) if m >> k & 1) for m in range(1, 2 ** len(group))]

    peers = {(b,) for b in range(n_bits)} | {tuple(sorted(m)) for g in kv_groups for m in subsets(g)}
    barrier = pltpu.get_barrier_semaphore()
    for bits in sorted(peers):
        pl.semaphore_signal(barrier, inc=1, device_id={"dp": flipped(bits)}, device_id_type=pl.DeviceIdType.MESH)
    pl.semaphore_signal(barrier, inc=1, device_id={"tensor": 1 - core}, device_id_type=pl.DeviceIdType.MESH)
    pl.semaphore_wait(barrier, len(peers) + 1)

    sent = []

    def send(src, dst, device):
        k = len(sent)
        copy = pltpu.make_async_remote_copy(
            src_ref=src, dst_ref=dst, send_sem=send_sems.at[k], recv_sem=recv_sems.at[k],
            device_id=device, device_id_type=pl.DeviceIdType.MESH)
        copy.start()
        sent.append(copy)
        return copy

    flying = {}

    def start(n, s):
        order, _ = items[n]
        half = 2 ** (n_bits - s - 1)
        device = {"dp": flipped((order[s],))}
        if s == 0:
            flying[n] = [
                send(ins[n][0].at[natural_index(me, j, ((order[0], True),), order[1:])], recvs[n][0].at[j], device)
                for j in range(half)
            ]
        else:
            away = (1 - bit_of(me, order[s])) * half
            flying[n] = [send(curs[n][s].at[pl.ds(away, half)], recvs[n][s], device)]

    def finish(n, s):
        order, _ = items[n]
        half = 2 ** (n_bits - s - 1)
        for copy in flying.pop(n):
            copy.wait_recv()
        got = recvs[n][s]
        held = curs[n][s] if s else ins[n][0]

        def total_at(j):
            if s:
                index = bit_of(me, order[s]) * half + j
            else:
                index = natural_index(me, j, ((order[0], False),), order[1:])
            return held[index].astype(F32) + got[j].astype(F32)

        if s == n_bits - 1:
            outs[n][...] = total_at(0)
            return

        def body(j, carry):
            curs[n][s + 1][j] = total_at(j).astype(BF)
            return carry

        lax.fori_loop(0, half, body, 0)
        start(n, s + 1)

    other_core = {"tensor": 1 - core}
    own, depth = near[0].shape
    sources = list(far)
    sources[0] = far[0].at[0, pl.ds(pl.multiple_of(core * own, own), own), :]
    buf = dict(zip(NAMES, near))
    fetch = {name: pltpu.make_async_copy(s, d, local_sems.at[k])
             for k, (name, s, d) in enumerate(zip(NAMES, sources, near))}
    first_use = ("k", "v")
    by_rows = ("q_o", "ga_o", "cos", "sin", "ql_o", "q_x", "ga_x", "ql_x")

    def fetch_rows(name, i):
        k = NAMES.index(name)
        at = pl.ds(pl.multiple_of(i * QB, QB), QB)
        return pltpu.make_async_copy(far[k].at[at, :], near[k].at[at, :], part_sems.at[by_rows.index(name), i])

    second_use = ("nb", "kl", "wk", "wv", "wq_o", "wq_x", "x", "gmid")
    for name in first_use:
        fetch[name].start()
    for i in range(own // QB):
        for name in by_rows:
            fetch_rows(name, i).start()
    for n in range(n_items):
        if items[n][1]:
            start(n, 0)
    for name in second_use:
        fetch[name].start()
    dk_all[...] = jnp.zeros_like(dk_all)
    dv_all[...] = jnp.zeros_like(dv_all)
    g_q[...] = jnp.zeros_like(g_q)
    gq_row = rows8[4:5, :HEAD_WIDTH]
    for name in first_use:
        fetch[name].wait()

    def attn_body(i, carry):
        for name in by_rows:
            fetch_rows(name, i).wait()
        attn_rows(i, seg, buf, lse, delta, gq_row, qr_o, qr_x, dk_all, dv_all, g_q)
        return carry

    lax.fori_loop(0, own // QB, attn_body, 0)
    front[:, :HEAD_WIDTH] = dk_all[:BLOCK, :].astype(BF)
    front[:, HEAD_WIDTH:] = dv_all[:BLOCK, :].astype(BF)
    front_copy = send(front, front_got, other_core)
    fetch["nb"].wait()
    query_sent[...] = tn(qr_x[...], buf["nb"][...]).astype(BF)
    query_copy = send(query_sent, query_got, other_core)
    fetch["kl"].wait()
    front_copy.wait_recv()
    gk_row, gin_row = rows8[5:6, :HEAD_WIDTH], rows8[0:1, :]
    g_k[...] = jnp.zeros_like(g_k)
    g_in[...] = jnp.zeros_like(g_in)
    blocks = own // BLOCK

    def kv_rows(i, carry):
        at = pl.ds(pl.multiple_of(i * BLOCK, BLOCK), BLOCK)
        tail = ((i == blocks - 1) & (core == 0)).astype(F32)
        later = pl.ds(pl.multiple_of((i + 1) * BLOCK, BLOCK), BLOCK)
        dk = dk_all[later, :] + tail * front_got[:, :HEAD_WIDTH].astype(F32)
        dv = dv_all[later, :] + tail * front_got[:, HEAD_WIDTH:].astype(F32)
        dkn = rotate(dk, buf["cos"][at, :], buf["sin"][at, :], -1)
        k_hat, k_inv = rms_stats(buf["kl"][at, :])
        kraw[at, :] = rms_back(k_hat, k_inv, gk_row, dkn).astype(BF)
        vraw[at, :] = dv.astype(BF)
        g_k[...] += jnp.sum(dkn * k_hat, axis=0, keepdims=True)
        return carry

    lax.fori_loop(0, blocks, kv_rows, 0)
    n_chunk, rows_k = kv_in.shape[1:3]
    for t, raw in enumerate((kraw, vraw)):
        kv_in[t] = tn(raw[...], buf["nb"][...]).astype(BF).reshape(n_chunk, rows_k, depth)
    kv_copies = [send(kv_in.at[1 - core], kv_core, other_core)]
    query_copy.wait_recv()
    own_query = tn(qr_o[...], buf["nb"][...]) + query_got[...].astype(F32)
    query[...] = own_query.astype(BF).reshape(query.shape)
    start(n_items - 1, 0)
    kv_copies[0].wait_recv()

    def kv_first(j, carry):
        index = natural_index(me, j, (), kv_order)
        kv_cur[0][j] = (kv_in[core, index].astype(F32) + kv_core[index].astype(F32)).astype(BF)
        return carry

    lax.fori_loop(0, 2**n_bits, kv_first, 0)

    def rest_of(g):
        return 2 ** (n_bits - sum(len(x) for x in kv_groups[: g + 1]))

    def block_index(group, bits):
        index = 0
        for k, b in enumerate(group):
            mine = bit_of(me, b)
            index = index + (1 - mine if b in bits else mine) * 2 ** (len(group) - 1 - k)
        return index

    def kv_start(g):
        rest = rest_of(g)
        return [send(kv_cur[g].at[pl.ds(block_index(kv_groups[g], m) * rest, rest)], kv_recv[g].at[c],
                     {"dp": flipped(m)}) for c, m in enumerate(subsets(kv_groups[g]))]

    spot = 0
    for k, b in enumerate(kv_order):
        spot = spot + bit_of(me, b) * 2 ** (n_bits - 1 - k)
    kv_copies = kv_start(0)
    for n in range(n_items):
        if items[n][1]:
            finish(n, 0)
    for name in ("wk", "wv", "wq_o", "wq_x", "x", "gmid"):
        fetch[name].wait()

    def input_rows(i, carry):
        at = pl.ds(pl.multiple_of(i * QB, QB), QB)
        gn = nt(kraw[at, :], buf["wk"][...]) + nt(vraw[at, :], buf["wv"][...])
        gn = gn + nt(qr_o[at, :], buf["wq_o"][...]) + nt(qr_x[at, :], buf["wq_x"][...])
        hat, inv = rms_stats(buf["x"][at, :])
        buf["x"][at, :] = buf["gmid"][at, :] + rms_back(hat, inv, gin_row, gn)
        g_in[...] += jnp.sum(gn * hat, axis=0, keepdims=True)
        return carry

    gain_copies = []

    def gain_start(s):
        if s == 0:
            gain_copies.append([send(gain_own[0], gain_got[0].at[0], other_core)])
        else:
            gain_copies.append([send(gain_own[s], gain_got[s].at[c], {"dp": flipped(m)})
                                for c, m in enumerate(subsets(kv_groups[s - 1]))])

    def gain_step():
        s = len(gain_copies) - 1
        total = gain_own[s][...]
        for c, copy in enumerate(gain_copies[s]):
            copy.wait_recv()
            total = total + gain_got[s][c]
        if s == len(kv_groups):
            gain_out[...] = total
            return True
        gain_own[s + 1][...] = total
        gain_start(s + 1)
        return False

    half_rows = own // QB // 2

    def fill_first():
        lax.fori_loop(0, half_rows, input_rows, 0)

    def fill_second():
        lax.fori_loop(half_rows, own // QB, input_rows, 0)
        gain_own[0][...] = jnp.zeros_like(gain_own[0])
        gain_own[0][0:3, :] = g_block[0:3, :]
        gain_own[0][3:4, :] = g_in[...]
        gain_own[0][4:5, :HEAD_WIDTH] = g_q[...]
        gain_own[0][5:6, :HEAD_WIDTH] = g_k[...]
        gain_start(0)

    gin_copy = pltpu.make_async_copy(buf["x"], gin_far, local_sems.at[len(NAMES)])
    fills = [fill_first, fill_second, gin_copy.start]
    rank = lambda e: e[1] - (1 if items[e[0]][1] else 0)
    todo = [(n, s) for s in range(n_bits) for n in range(n_items) if s or not items[n][1]]
    todo.sort(key=rank)

    def advance():
        now = rank(todo[0]) if todo else 0
        while todo and rank(todo[0]) == now:
            finish(*todo.pop(0))

    for g in range(len(kv_groups)):
        rest = rest_of(g)
        for copy in kv_copies:
            copy.wait_recv()
        base = block_index(kv_groups[g], ()) * rest

        def kv_total(j, g=g, base=base):
            total = kv_cur[g][base + j].astype(F32)
            for c in range(2 ** len(kv_groups[g]) - 1):
                total = total + kv_recv[g][c, j].astype(F32)
            return total.astype(BF)

        if g < len(kv_groups) - 1:

            def kv_body(j, carry, g=g, kv_total=kv_total):
                kv_cur[g + 1][j] = kv_total(j)
                return carry

            lax.fori_loop(0, rest, kv_body, 0)
            kv_copies = kv_start(g + 1)
            if len(fills) > 2:
                fills.pop(0)()
            advance()
        else:
            kv_all[core, spot] = kv_total(0)
    gains_done = False
    for g in reversed(range(len(kv_groups))):
        size = rest_of(g)
        begin = 0
        for k, b in enumerate(sum(kv_groups[: g + 1], ())):
            begin = begin + bit_of(me, b) * 2 ** (n_bits - 1 - k)
        region = kv_all.at[core, pl.ds(begin, size)]
        copies = [send(region, region, {"dp": flipped(m)}) for m in subsets(kv_groups[g])]
        while len(fills) > 1:
            fills.pop(0)()
        if fills:
            fills.pop(0)()
        elif not gains_done:
            gains_done = gain_step()
        advance()
        for copy in copies:
            copy.wait_recv()
    copy = send(kv_all.at[core], kv_all.at[core], other_core)
    while todo:
        advance()
    while not gains_done:
        gains_done = gain_step()
    copy.wait_recv()

    def unpack(j, carry):
        index = natural_index(me, j, (), kv_order)
        for t in range(2):
            kv_wide[t, index] = kv_all[t, j].astype(F32)
        return carry

    lax.fori_loop(0, 2**n_bits, unpack, 0)
    for t, out in enumerate((k_out, v_out)):
        out[...] = jnp.transpose(kv_wide[t].reshape(HEAD_WIDTH, depth))
    gin_copy.wait()
    for copy in sent:
        copy.wait_send()


def finish_all(n_dp, items, order, kv_order, small, far):
    n_bits = len(kv_order)
    own, part = far[12].shape
    ext = far[10].shape[0]
    depth = far[1].shape[1]
    groups = tuple(tuple(kv_order[k : k + 2]) for k in range(0, n_bits, 2))
    spec, operands, outs, comm = [], [], [], []
    copies = 3
    shapes = [value.shape for value, _ in items] + [(n_dp, part // n_dp, depth)]
    for k, (n, c, width) in enumerate(shapes):
        early = k < len(items)
        spec.append((tuple(items[k][1] if early else order), early))
        if early:
            operands.append(items[k][0])
        outs.append(sds((c, width), F32))
        comm += [pltpu.VMEM((2 ** (n_bits - s - 1), c, width), BF) for s in range(n_bits)]
        comm += [pltpu.VMEM((2 ** (n_bits - s), c, width), BF) for s in range(1, n_bits)]
        copies += n_bits - 1 + n // 2
    n, c, width = n_dp, HEAD_WIDTH // n_dp, depth
    comm += [pltpu.VMEM((n, c, width), BF)]
    sizes = [2 ** (n_bits - sum(len(x) for x in groups[:g])) for g in range(len(groups) + 1)]
    comm += [pltpu.VMEM((2 ** len(groups[g]) - 1, sizes[g + 1], c, width), BF) for g in range(len(groups))]
    comm += [pltpu.VMEM((sizes[g], c, width), BF) for g in range(len(groups))]
    comm += [pltpu.VMEM((2, n, c, width), BF)]
    comm += [pltpu.VMEM((2, n, c, width), F32)]
    comm += [pltpu.VMEM((8, width), F32) for _ in range(len(groups) + 1)]
    comm += [pltpu.VMEM((1, 8, width), F32)] + [pltpu.VMEM((2 ** len(g) - 1, 8, width), F32) for g in groups]
    copies += 3 + 3 * sum(2 ** len(g) - 1 for g in groups)
    comm += [pltpu.SemaphoreType.DMA((copies,)), pltpu.SemaphoreType.DMA((copies,))]
    outs += [sds((width, HEAD_WIDTH), F32), sds((width, HEAD_WIDTH), F32), sds((8, width), F32), sds((own, depth), F32)]
    near = [pltpu.VMEM((own, depth), F32)] + [pltpu.VMEM(a.shape, a.dtype) for a in far[1:]]
    scratch = near + [
        pltpu.SemaphoreType.DMA((len(far) + 1,)), pltpu.SemaphoreType.DMA((8, own // QB)),
        pltpu.VMEM((BLOCK, 2 * HEAD_WIDTH), BF), pltpu.VMEM((BLOCK, 2 * HEAD_WIDTH), BF),
        pltpu.VMEM((ext, HEAD_WIDTH), F32), pltpu.VMEM((ext, HEAD_WIDTH), F32),
        pltpu.VMEM((own, part), BF), pltpu.VMEM((own, part), BF),
        pltpu.VMEM((own, HEAD_WIDTH), BF), pltpu.VMEM((own, HEAD_WIDTH), BF),
        pltpu.VMEM((2, n, c, width), BF), pltpu.VMEM((part, depth), BF), pltpu.VMEM((part, depth), BF),
        pltpu.VMEM((n_dp, part // n_dp, depth), BF), pltpu.VMEM((1, depth), F32),
        pltpu.VMEM((1, HEAD_WIDTH), F32), pltpu.VMEM((1, HEAD_WIDTH), F32),
    ] + comm
    vmem = pl.BlockSpec(memory_space=pltpu.VMEM)
    anywhere = pl.BlockSpec(memory_space=pl.ANY)
    operands += list(small)
    return pl.pallas_call(
        functools.partial(finish_kernel, tuple(spec), groups, n_bits),
        out_shape=outs,
        in_specs=[vmem] * len(operands) + [anywhere] * len(far),
        out_specs=[vmem] * (len(outs) - 1) + [anywhere],
        scratch_shapes=scratch,
        compiler_params=pltpu.CompilerParams(
            collective_id=0, has_side_effects=True, vmem_limit_bytes=VMEM_LIMIT),
        name="finish_all",
    )(*operands, *far)


def after(value, *others):
    return lax.optimization_barrier((value,) + others)[0]


def on_device(n_dp, n_tensor, residual_in, cotangent, segment_ids, gain_attn_in, w_query, w_key, w_value,
              gain_query, gain_key, w_out, gain_attn_out, gain_ff_in, w_gate, w_up, w_down, gain_ff_out):
    tokens, depth = residual_in.shape[1:]
    own = tokens // n_tensor
    me = lax.axis_index("tensor")
    first_row = (me * own).astype(jnp.int32).reshape(1)
    wq_x = swap(w_query, n_tensor)
    *later, wq_x = lax.optimization_barrier((w_out, w_gate, w_up, w_down, wq_x))
    wo_x, wg_x, wu_x, wd_x = (swap(w, n_tensor) for w in later)
    table = jnp.asarray(rope_table())
    gain_list = (gain_attn_in, gain_attn_out, gain_ff_in, gain_ff_out, gain_query, gain_key)
    q_o, q_x, ql_o, ql_x, k, v, kl, nb, cos, sin, seg_ext, rows8 = project(
        first_row, own, residual_in, segment_ids, table, gain_list, w_query, wq_x, w_key, w_value)
    weights = (w_out, wo_x, w_gate, wg_x, w_up, wu_x, w_down, wd_x)
    (output, gmid, ga_o, ga_x, af_o, af_x, lse, delta, mid_b, gff, gas,
     act_o, act_x, gg_o, gg_x, gu_o, gu_x, gains) = block_pass(
        first_row, residual_in, cotangent, seg_ext, q_o, q_x, k, v, weights, rows8)

    n_bits = n_dp.bit_length() - 1
    plain, turned, lead = bit_orders(n_bits)
    chunks = lambda value: value.reshape(n_dp, value.shape[0] // n_dp, value.shape[1])

    pairs = [(gff, act_x, act_o, plain), (mid_b, gg_x, gg_o, turned), (mid_b, gu_x, gu_o, lead), (gas, af_x, af_o, plain)]
    grad = lambda left, units: tn(left, units) if left is not mid_b else tn(units, left)
    gots = []
    last = ()
    for left, units, _, _ in pairs:
        sent = grad(left, after(units, *last)).astype(BF)
        last = (sent,)
        gots.append(swap(sent, n_tensor))
    items = []
    for (left, _, units, order), got in zip(pairs, gots):
        value = chunks((grad(left, after(units, *last)) + got.astype(F32)).astype(BF))
        last = (value,)
        items.append((value, order))
    far = (residual_in, gmid, w_query, wq_x, w_key, w_value, kl, cos, sin, nb, k, v, q_o, q_x, ga_o, ga_x, ql_o, ql_x)
    *shares, k_sum, v_sum, gain_sum, grad_input = finish_all(
        n_dp, items, plain, plain, (seg_ext, lse, delta, rows8, gains), far)
    s_down, s_gate, s_up, s_out, s_query = shares
    return (
        output[None], grad_input[None], gain_sum[3], s_query.T, k_sum, v_sum,
        gain_sum[4, :HEAD_WIDTH], gain_sum[5, :HEAD_WIDTH],
        s_out.T, gain_sum[2], gain_sum[1], s_gate.T, s_up.T, s_down.T, gain_sum[0],
    )


def solution(mesh):
    n_dp, n_tensor = mesh.shape["dp"], mesh.shape["tensor"]
    return jax.shard_map(
        functools.partial(on_device, n_dp, n_tensor),
        mesh=mesh,
        in_specs=(
            P("dp", None, None), P("dp", None, None), P("dp", None), P(), P(None, "tensor"), P(), P(), P(), P(),
            P("tensor", None), P(), P(), P(None, "tensor"), P(None, "tensor"), P("tensor", None), P(),
        ),
        out_specs=(
            P("dp", "tensor", None), P("dp", "tensor", None), P(), P(None, ("tensor", "dp")), P(), P(), P(), P(),
            P("tensor", "dp"), P(), P(), P(None, ("tensor", "dp")), P(None, ("tensor", "dp")), P("tensor", "dp"),
            P(),
        ),
        check_vma=False,
    )
```
